32 devices in a mesh: dom: 8 (over z, y), sub: 4 (over x, core).
Axes of the slice: x: 2, y: 2, z: 4, core: 2. Of those that a mesh axis runs over, the one named last changes fastest.
Arguments:
- nodal_values: float32 [512, 8192], P(None, ('dom', 'sub')), may hold values from -6 to 6
- kappa: float32 [512, 8192], P(None, ('dom', 'sub')), may hold values from 0.25 to 4
- levels: int32 [8192], P(('dom', 'sub')), may hold values from 0 to 3
- local_faces: int32 [2, 2048], P(None, ('dom', 'sub')), may hold values from 0 to 511, as said below
- sub_faces: int32 [2, 1024], P(None, ('dom', 'sub')), may hold values from 0 to 511, as said below
- near_faces: int32 [2, 1024], P(None, ('dom', 'sub')), may hold values from 512 to 1023, as said below
- far_faces: int32 [2, 384], P(None, ('dom', 'sub')), may hold values from 1024 to 1535, as said below
- child_faces: int32 [4, 96], P(None, ('dom', 'sub')), may hold values from 1024 to 1279, as said below
- child_peer: int32 [96], P(('dom', 'sub')), may hold values from 0 to 7, as said below
- coarse_faces: int32 [256], P(('dom', 'sub')), may hold values from -1 to 1535, as said below
Outputs:
- applied: float32 [512, 8192], P(None, ('dom', 'sub'))
The draws below stay inside these ranges and needn't reach their ends.
Inputs may be any that keep to these rules, and one draw needn't show every extreme that they name: `local_faces`: row 0 holds faces f = 1 and row 1 faces f = 0 of distinct elements of the same device; column k of both rows is one shared face. `sub_faces`: row 0 holds faces f = 0, row 1 faces f = 1, of distinct elements; entries toward a missing neighbour are boundary faces. `near_faces`: row 0 holds faces f = 2, row 1 faces f = 3, of distinct elements; entries toward a missing neighbour are boundary faces. `far_faces`: row 0 holds faces f = 4, row 1 faces f = 5, of distinct elements; entries toward a missing partner are boundary faces. `child_faces`: faces f = 4 of distinct elements, distinct from all far faces; row m is the child at subface position (m // 2, m % 2). `child_peer`: A device's 3 groups name distinct dom indices other than its own; in every draw one device per sub index is named by every other dom index. `coarse_faces`: slot p is the face f = 5 that takes the group which the device of dom index p (same sub index) sends here, -1 where it sends none; faces are of distinct elements, distinct from all far faces.
All inputs are finite; a program needn't handle non-finite values.
Results may differ from the reference program's by a relative error of at most 0.0003.
Values sent between devices are 32-bit elements; how exact they have to be, the bound alone decides.
A program may use at most 64 MiB of HBM per device.

```python
import math
import jax
import jax.numpy as jnp
import numpy as np
from jax import lax

NPTS = 8
E_DEV = 256
S_FACES = 32
NEAR = 32
L_PAIRS = 64
FAR = 4
SHIFTS = 3
NODES = 512
ELEMS = 8192
N_DOM = 8
N_SUB = 4


def element_orders(key):
    devices = N_DOM * N_SUB
    keys = jax.random.split(jax.random.fold_in(key, 11), 3 * devices)
    orders = jax.vmap(lambda item: jax.random.permutation(item, E_DEV))(keys)
    return orders.reshape(3, devices, E_DEV).astype(jnp.int32)


def mortar_plan(key):
    count = 3 * N_DOM // 8
    hub = jax.random.randint(jax.random.fold_in(key, 31), (N_SUB,), 0, N_DOM)
    keys = jax.random.split(jax.random.fold_in(key, 37), N_DOM * N_SUB)
    ranks = jax.vmap(lambda item: jax.random.permutation(item, N_DOM))(keys).astype(jnp.int32)
    ranks = ranks.reshape(N_DOM, N_SUB, N_DOM)
    lanes = lax.iota(jnp.int32, N_DOM)
    scores = jnp.where(lanes[None, None, :] == hub[None, :, None], -1, ranks)
    scores = jnp.where(lanes[None, None, :] == lanes[:, None, None], N_DOM + 1, scores)
    chosen = jnp.argsort(scores, axis=-1, stable=True)[:, :, :count].astype(jnp.int32)
    shuffle_keys = jax.random.split(jax.random.fold_in(key, 41), N_DOM * N_SUB)
    shuffle = jax.vmap(lambda item: jax.random.permutation(item, count))(shuffle_keys).astype(jnp.int32)
    return jnp.take_along_axis(chosen, shuffle.reshape(N_DOM, N_SUB, count), axis=-1)


def draw_local_faces(key, part):
    orders = element_orders(key)[0]
    first = E_DEV + orders[:, 2 * S_FACES:2 * S_FACES + L_PAIRS]
    second = orders[:, 2 * S_FACES + L_PAIRS:2 * S_FACES + 2 * L_PAIRS]
    return jnp.stack([first.reshape(-1), second.reshape(-1)]).astype(jnp.int32)


def draw_sub_faces(key, part):
    orders = element_orders(key)[0]
    lower = orders[:, :S_FACES]
    upper = E_DEV + orders[:, S_FACES:2 * S_FACES]
    return jnp.stack([lower.reshape(-1), upper.reshape(-1)]).astype(jnp.int32)


def draw_near_faces(key, part):
    orders = element_orders(key)[1]
    lower = 2 * E_DEV + orders[:, :NEAR]
    upper = 3 * E_DEV + orders[:, NEAR:2 * NEAR]
    return jnp.stack([lower.reshape(-1), upper.reshape(-1)]).astype(jnp.int32)


def draw_far_faces(key, part):
    span = SHIFTS * FAR
    orders = element_orders(key)[2]
    lower = 4 * E_DEV + orders[:, :span]
    upper = 5 * E_DEV + orders[:, span:2 * span]
    return jnp.stack([lower.reshape(-1), upper.reshape(-1)]).astype(jnp.int32)


def draw_child_faces(key, part):
    count = 3 * N_DOM // 8
    base = 2 * SHIFTS * FAR
    orders = element_orders(key)[2].reshape(N_DOM, N_SUB, E_DEV)
    elements = orders[:, :, base:base + 4 * count].reshape(N_DOM, N_SUB, count, 4)
    faces = 4 * E_DEV + elements
    return faces.transpose(3, 0, 1, 2).reshape(4, -1).astype(jnp.int32)


def draw_child_peer(key, part):
    return mortar_plan(key).reshape(-1).astype(jnp.int32)


def draw_coarse_faces(key, part):
    base = 2 * SHIFTS * FAR
    plan = mortar_plan(key)
    lanes = lax.iota(jnp.int32, N_DOM)
    sends = (plan[:, :, :, None] == lanes[None, None, None, :]).any(axis=2)
    receive = sends.transpose(2, 1, 0)
    rank = jnp.cumsum(receive.astype(jnp.int32), axis=2) - 1
    orders = element_orders(key)[2].reshape(N_DOM, N_SUB, E_DEV)
    elements = jnp.take_along_axis(orders, base + jnp.maximum(rank, 0), axis=2)
    faces = jnp.where(receive, 5 * E_DEV + elements, -1)
    return faces.reshape(-1).astype(jnp.int32)


def with_ends(drawn, stream_key, least, top_value):
    longest = drawn.shape.index(max(drawn.shape))
    spots = []
    for shift in (0, 1):
        where = [jax.random.randint(jax.random.fold_in(stream_key, axis), (), 0, length) for axis, length in enumerate(drawn.shape)]
        where[longest] = (where[longest] + shift) % drawn.shape[longest]
        spots.append(tuple(where))
    return drawn.at[spots[0]].set(least).at[spots[1]].set(top_value)


def level_of(key, dims, cuts, least, largest):
    def one(dim, blocks):
        draws = jax.random.uniform(jax.random.fold_in(jax.random.fold_in(key, 6), dim), (blocks,), jnp.float32, least / len(cuts), largest / len(cuts))
        return jnp.repeat(jnp.exp(draws), dims[dim] // blocks).reshape((-1,) + (1,) * (len(dims) - dim - 1))

    level = one(*cuts[0])
    for cut in cuts[1:]:
        level = level * one(*cut)
    return level


def centred(own_key, shape, scale, reach, cuts=(), kind=jnp.bfloat16):
    loudness = level_of(own_key, shape, cuts, -0.22, 0.18) if cuts else 1.0
    values = jax.random.normal(own_key, shape, jnp.float32) * scale * loudness
    return jnp.minimum(jnp.maximum(values, -reach), reach).astype(kind)


def setup_inputs(seed: int = 0) -> dict:
    key_list = jax.random.split(jax.random.key(seed), 11)
    nodal_values = centred(key_list[0], (NODES, ELEMS), 1.0, 6.0, ((1, 32),), jnp.float32)
    kappa = jnp.clip(jnp.exp(math.log(4.0) - 2.7725887 * jax.random.uniform(key_list[1], (NODES, ELEMS), jnp.float32) ** level_of(key_list[1], (NODES, ELEMS), ((1, 32),), -0.2, 0.2)), 0.25, 4.0)
    levels = with_ends(jax.random.randint(key_list[2], (ELEMS,), 0, 4), jax.random.fold_in(key_list[2], 1), 0, 3).astype(jnp.int32)
    local_faces = draw_local_faces(jax.random.fold_in(key_list[10], 71), 0)
    sub_faces = draw_sub_faces(jax.random.fold_in(key_list[10], 71), 0)
    near_faces = draw_near_faces(jax.random.fold_in(key_list[10], 71), 0)
    far_faces = draw_far_faces(jax.random.fold_in(key_list[10], 71), 0)
    child_faces = draw_child_faces(jax.random.fold_in(key_list[10], 71), 0)
    child_peer = draw_child_peer(jax.random.fold_in(key_list[10], 71), 0)
    coarse_faces = draw_coarse_faces(jax.random.fold_in(key_list[10], 71), 0)
    return {"nodal_values": nodal_values, "kappa": kappa, "levels": levels, "local_faces": local_faces, "sub_faces": sub_faces, "near_faces": near_faces, "far_faces": far_faces, "child_faces": child_faces, "child_peer": child_peer, "coarse_faces": coarse_faces}


HIGHEST = lax.Precision.HIGHEST


def legendre_table(points, degree):
    table = [np.ones(points.shape), points.copy()]
    for order in range(2, degree + 1):
        table.append(((2 * order - 1) * points * table[order - 1] - (order - 1) * table[order - 2]) / order)
    return table


def lobatto_points(degree):
    points = np.cos(np.pi * np.arange(degree + 1) / degree)
    for sweep in range(100):
        table = legendre_table(points, degree)
        points = points - (points * table[degree] - table[degree - 1]) / ((degree + 1) * table[degree])
    points = np.sort(points)
    return points, legendre_table(points, degree)[degree]


def node_tables(count):
    degree = count - 1
    points, legendre = lobatto_points(degree)
    weights = 2.0 / (degree * (degree + 1) * legendre ** 2)
    spread = points[:, None] - points[None, :] + np.eye(count)
    derivative = legendre[:, None] / (legendre[None, :] * spread) * (1.0 - np.eye(count))
    derivative[0, 0] = -degree * (degree + 1) / 4.0
    derivative[degree, degree] = degree * (degree + 1) / 4.0
    halves = []
    for side in range(2):
        target = (points + 2.0 * side - 1.0) / 2.0
        matrix = np.ones((count, count))
        for column in range(count):
            for other in range(count):
                if other != column:
                    matrix[:, column] = matrix[:, column] * (target - points[other]) / (points[column] - points[other])
        halves.append(matrix)
    return points, weights, derivative, np.stack(halves)


def stiffness(values, coeffs, level):
    points, weights, derivative, halves = node_tables(NPTS)
    deriv = jnp.asarray(derivative, jnp.float32)
    elems = values.shape[1]
    cube = values.reshape(NPTS, NPTS, NPTS, elems)
    weight_cube = jnp.asarray(weights[:, None, None] * weights[None, :, None] * weights[None, None, :], jnp.float32)
    scale = jnp.power(jnp.float32(0.5), level.astype(jnp.float32))
    geometry = coeffs.reshape(NPTS, NPTS, NPTS, elems) * weight_cube[:, :, :, None] * scale[None, None, None, :]
    first = jnp.einsum("ai,ijkn->ajkn", deriv, cube, precision=HIGHEST)
    first = jnp.einsum("ai,ajkn->ijkn", deriv, geometry * first, precision=HIGHEST)
    second = jnp.einsum("bj,ijkn->ibkn", deriv, cube, precision=HIGHEST)
    second = jnp.einsum("bj,ibkn->ijkn", deriv, geometry * second, precision=HIGHEST)
    third = jnp.einsum("ck,ijkn->ijcn", deriv, cube, precision=HIGHEST)
    third = jnp.einsum("ck,ijcn->ijkn", deriv, geometry * third, precision=HIGHEST)
    return (first + second + third).reshape(NPTS ** 3, elems)


def extract_faces(local):
    elems = local.shape[1]
    cube = local.reshape(NPTS, NPTS, NPTS, elems)
    sides = jnp.stack([cube[0], cube[NPTS - 1], cube[:, 0], cube[:, NPTS - 1], cube[:, :, 0], cube[:, :, NPTS - 1]])
    return sides.reshape(6, NPTS * NPTS, elems).transpose(1, 0, 2).reshape(NPTS * NPTS, 6 * elems)


def add_back(local, total):
    elems = local.shape[1]
    boxes = total.reshape(NPTS * NPTS, 6, elems).transpose(1, 0, 2).reshape(6, NPTS, NPTS, elems)
    cube = local.reshape(NPTS, NPTS, NPTS, elems)
    cube = cube.at[0].add(boxes[0]).at[NPTS - 1].add(boxes[1])
    cube = cube.at[:, 0].add(boxes[2]).at[:, NPTS - 1].add(boxes[3])
    cube = cube.at[:, :, 0].add(boxes[4]).at[:, :, NPTS - 1].add(boxes[5])
    return cube.reshape(NPTS ** 3, elems)


def pick_faces(faces, index_list):
    safe = jnp.maximum(index_list, 0)
    taken = jnp.take(faces, safe, axis=1)
    return taken * (index_list >= 0).astype(faces.dtype)[None, :]


def put_faces(total, index_list, values):
    safe = jnp.where(index_list >= 0, index_list, total.shape[1])
    return total.at[:, safe].add(values, mode="drop")


def restrict(face, part, halves):
    shape = face.shape
    grid = face.reshape(shape[:-2] + (NPTS, NPTS, shape[-1]))
    result = jnp.einsum("ai,bj,...abn->...ijn", halves[part // 2], halves[part % 2], grid, precision=HIGHEST)
    return result.reshape(shape)


def prolong(face, part, halves):
    shape = face.shape
    grid = face.reshape(shape[:-2] + (NPTS, NPTS, shape[-1]))
    result = jnp.einsum("ai,bj,...ijn->...abn", halves[part // 2], halves[part % 2], grid, precision=HIGHEST)
    return result.reshape(shape)


def reference(nodal_values, kappa, levels, local_faces, sub_faces, near_faces, far_faces, child_faces, child_peer, coarse_faces):
    halves = jnp.asarray(node_tables(NPTS)[3], jnp.float32)
    devs = N_DOM * N_SUB
    elems = nodal_values.shape[1] // devs
    square = NPTS * NPTS

    def per_device(array):
        return array.reshape(array.shape[0], devs, elems).transpose(1, 0, 2)

    def tables(array):
        return array.reshape(array.shape[0], devs, array.shape[1] // devs).transpose(1, 0, 2)

    values = per_device(nodal_values)
    coeffs = per_device(kappa)
    level = levels.reshape(devs, elems)
    local = lax.map(lambda items: stiffness(items[0], items[1], items[2]), (values, coeffs, level))
    faces = jax.vmap(extract_faces)(local)
    total = jnp.zeros_like(faces)
    pick_all = jax.vmap(pick_faces)
    put_all = jax.vmap(put_faces)

    pairs = tables(local_faces)
    total = put_all(total, pairs[:, 0], pick_all(faces, pairs[:, 1]))
    total = put_all(total, pairs[:, 1], pick_all(faces, pairs[:, 0]))

    rims = tables(sub_faces)
    width = rims.shape[2]
    down = pick_all(faces, rims[:, 0]).reshape(N_DOM, N_SUB, square, width)
    above = pick_all(faces, rims[:, 1]).reshape(N_DOM, N_SUB, square, width)
    blank = jnp.zeros((N_DOM, 1, square, width), jnp.float32)
    from_lower = jnp.concatenate([blank, above[:, :-1]], axis=1).reshape(devs, square, width)
    from_upper = jnp.concatenate([down[:, 1:], blank], axis=1).reshape(devs, square, width)
    total = put_all(total, rims[:, 0], from_lower)
    total = put_all(total, rims[:, 1], from_upper)

    near = tables(near_faces)
    width = near.shape[2]
    down = pick_all(faces, near[:, 0]).reshape(N_DOM, N_SUB, square, width)
    above = pick_all(faces, near[:, 1]).reshape(N_DOM, N_SUB, square, width)
    blank = jnp.zeros((1, N_SUB, square, width), jnp.float32)
    from_lower = jnp.concatenate([blank, above[:-1]], axis=0).reshape(devs, square, width)
    from_upper = jnp.concatenate([down[1:], blank], axis=0).reshape(devs, square, width)
    total = put_all(total, near[:, 0], from_lower)
    total = put_all(total, near[:, 1], from_upper)

    far = tables(far_faces)
    far_low = pick_all(faces, far[:, 0]).reshape(N_DOM, N_SUB, square, SHIFTS, FAR)
    far_high = pick_all(faces, far[:, 1]).reshape(N_DOM, N_SUB, square, SHIFTS, FAR)
    lower_parts = []
    upper_parts = []
    for step in range(SHIFTS):
        offset = step + 2
        blank = jnp.zeros((offset, N_SUB, square, FAR), jnp.float32)
        lower_parts.append(jnp.concatenate([blank, far_high[:-offset, :, :, step]], axis=0))
        upper_parts.append(jnp.concatenate([far_low[offset:, :, :, step], blank], axis=0))
    from_lower = jnp.stack(lower_parts, axis=3).reshape(devs, square, SHIFTS * FAR)
    from_upper = jnp.stack(upper_parts, axis=3).reshape(devs, square, SHIFTS * FAR)
    total = put_all(total, far[:, 0], from_lower)
    total = put_all(total, far[:, 1], from_upper)

    groups = tables(child_faces)
    count = groups.shape[2]
    peer = child_peer.reshape(N_DOM, N_SUB, count)
    coarse_table = coarse_faces.reshape(devs, N_DOM)
    children = jnp.stack([pick_all(faces, groups[:, part]) for part in range(4)], axis=1)
    projected = sum(restrict(children[:, part], part, halves) for part in range(4))
    projected = projected.reshape(N_DOM, N_SUB, square, count).transpose(0, 1, 3, 2)
    sub_index = lax.iota(jnp.int32, N_SUB)[None, :, None]
    dom_index = lax.iota(jnp.int32, N_DOM)[:, None, None]
    received = jnp.zeros((N_DOM, N_SUB, N_DOM, square), jnp.float32)
    received = received.at[peer, sub_index, dom_index].add(projected)
    received = received.transpose(0, 1, 3, 2).reshape(devs, square, N_DOM)
    coarse = pick_all(faces, coarse_table)
    summed = coarse + received
    total = put_all(total, coarse_table, received)
    spread = summed.reshape(N_DOM, N_SUB, square, N_DOM).transpose(0, 1, 3, 2)
    returned = spread[peer, sub_index, dom_index].transpose(0, 1, 3, 2).reshape(devs, square, count)
    for part in range(4):
        total = put_all(total, groups[:, part], prolong(returned, part, halves) - children[:, part])

    applied = jax.vmap(add_back)(local, total)
    return applied.transpose(1, 0, 2).reshape(NPTS ** 3, devs * elems)
```

```python
import functools

import jax
import jax.numpy as jnp
import numpy as np
from jax import lax
from jax.experimental import pallas as pl
from jax.experimental.pallas import tpu as pltpu
from jax.sharding import PartitionSpec as P

NPTS = 8
FAR = 4
MESH = pl.DeviceIdType.MESH
F32, BF16, I32 = jnp.float32, jnp.bfloat16, jnp.int32


def legendre_table(points, degree):
    table = [np.ones(points.shape), points.copy()]
    for order in range(2, degree + 1):
        table.append(
            ((2 * order - 1) * points * table[order - 1] - (order - 1) * table[order - 2]) / order
        )
    return table


def lobatto_points(degree):
    points = np.cos(np.pi * np.arange(degree + 1) / degree)
    for sweep in range(100):
        table = legendre_table(points, degree)
        points = points - (points * table[degree] - table[degree - 1]) / (
            (degree + 1) * table[degree]
        )
    points = np.sort(points)
    return (points, legendre_table(points, degree)[degree])


def node_tables(count):
    degree = count - 1
    points, legendre = lobatto_points(degree)
    weights = 2.0 / (degree * (degree + 1) * legendre**2)
    spread = points[:, None] - points[None, :] + np.eye(count)
    derivative = legendre[:, None] / (legendre[None, :] * spread) * (1.0 - np.eye(count))
    derivative[0, 0] = -degree * (degree + 1) / 4.0
    derivative[degree, degree] = degree * (degree + 1) / 4.0
    halves = []
    for side in range(2):
        target = (points + 2.0 * side - 1.0) / 2.0
        matrix = np.ones((count, count))
        for column in range(count):
            for other in range(count):
                if other != column:
                    matrix[:, column] = (
                        matrix[:, column]
                        * (target - points[other])
                        / (points[column] - points[other])
                    )
        halves.append(matrix)
    return (points, weights, derivative, np.stack(halves))


POINTS, WEIGHTS, DERIV, HALVES = node_tables(NPTS)


def up(count, unit=8):
    return -(-count // unit) * unit


def halves_of(values):
    high = values.astype(BF16)
    return high, (values - high.astype(F32)).astype(BF16)


def numpy_halves(matrix):
    matrix = np.asarray(matrix, np.float32)
    high = matrix.astype(jnp.bfloat16)
    low = (matrix - high.astype(np.float32)).astype(jnp.bfloat16)
    return high, low


def dot(a, b, dims=((1,), (0,))):
    return lax.dot_general(a, b, (dims, ((), ())), preferred_element_type=F32)


def select(hot, values):
    high, low = halves_of(values)
    return dot(hot, high) + dot(hot, low)


def take_rows(hot, face):
    high, low = halves_of(face)
    dims = ((1,), (1,))
    return dot(hot, high, dims) + dot(hot, low, dims)


def spread_rows(rows, hot):
    high, low = halves_of(rows.T)
    return dot(high, hot) + dot(low, hot)


def product(a, matrix):
    high, low = halves_of(a)
    mhigh, mlow = halves_of(matrix)
    return dot(high, mhigh) + dot(low, mhigh) + dot(high, mlow)


def column(row, padded):
    count = row.shape[1]
    r = lax.broadcasted_iota(I32, (padded, count), 0)
    c = lax.broadcasted_iota(I32, (padded, count), 1)
    spread = jnp.where(r == c, jnp.broadcast_to(row.astype(F32), (padded, count)), 0.0)
    col = jnp.sum(spread, axis=1, keepdims=True)
    inside = lax.broadcasted_iota(I32, (padded, 1), 0) < count
    return jnp.where(inside, col, -1.0)


def hot_rows(columns, base, elems, kind=BF16):
    col = columns[0] if len(columns) == 1 else jnp.concatenate(columns, axis=0)
    lane = lax.broadcasted_iota(I32, (col.shape[0], elems), 1).astype(F32)
    return jnp.where(lane == col - float(base), 1.0, 0.0).astype(kind)


def line(values, matrix):
    half = NPTS // 2
    even = [values[i] + values[NPTS - 1 - i] for i in range(half)]
    odd = [values[i] - values[NPTS - 1 - i] for i in range(half)]
    out = [None] * NPTS
    for a in range(half):
        p = q = None
        for i in range(half):
            s = float((matrix[a, i] + matrix[a, NPTS - 1 - i]) / 2)
            t = float((matrix[a, i] - matrix[a, NPTS - 1 - i]) / 2)
            p = even[i] * s if p is None else p + even[i] * s
            q = odd[i] * t if q is None else q + odd[i] * t
        out[a] = q + p
        out[NPTS - 1 - a] = q - p
    return out


def stencils():
    forth, back = np.kron(np.eye(16), DERIV), np.kron(np.eye(16), DERIV.T)
    pieces = [piece for table in (forth, back) for piece in numpy_halves(table)]
    return np.concatenate(pieces, axis=0)


def folds(krons):
    one = np.eye(NPTS)
    apply = np.concatenate(
        [np.kron(one, one), np.kron(DERIV.T, one), np.kron(one, DERIV.T)], axis=1
    )
    heads = [np.eye(NPTS * NPTS)] * 2 + [m.T for m in krons] + krons
    table = np.concatenate([(head @ apply).T for head in heads], axis=1)
    return np.concatenate(numpy_halves(table), axis=0)


def kernel(
    sizes,
    u_hbm,
    kappa_hbm,
    level_hbm,
    local_hbm,
    sub_hbm,
    near_hbm,
    far_hbm,
    child_hbm,
    coarse_hbm,
    fold_hbm,
    deriv_hbm,
    mortar_hbm,
    peer_hbm,
    out_ref,
    level_ref,
    local_ref,
    sub_ref,
    near_ref,
    far_ref,
    child_ref,
    coarse_ref,
    fold_ref,
    deriv_ref,
    mortar_ref,
    peer_ref,
    w_ref,
    u_ref,
    k_ref,
    g_ref,
    side_out,
    side_in,
    far_out,
    far_in,
    mort_out,
    mort_in,
    small_sem,
    load_sem,
    side_send,
    side_recv,
    far_send,
    far_recv,
    mort_send,
    mort_recv,
):
    n_dom, n_sub = sizes
    parts = u_ref.shape[0]
    elems = parts * 128
    square = NPTS * NPTS
    last = NPTS - 1
    me, sub = lax.axis_index("dom"), lax.axis_index("sub")

    urgent = [
        (far_hbm, far_ref),
        (child_hbm, child_ref),
        (coarse_hbm, coarse_ref),
        (level_hbm, level_ref),
        (peer_hbm, peer_ref),
    ]
    later = [
        (fold_hbm, fold_ref),
        (local_hbm, local_ref),
        (sub_hbm, sub_ref),
        (near_hbm, near_ref),
        (deriv_hbm, deriv_ref),
        (mortar_hbm, mortar_ref),
    ]
    small = [
        pltpu.make_async_copy(source, target, small_sem.at[slot])
        for slot, (source, target) in enumerate(urgent + later)
    ]
    block = 128
    blocks = NPTS**3 // block

    def load(n, part, source, target, slot):
        own = pl.ds(part * block, block)
        return pltpu.make_async_copy(
            source.at[own, pl.ds(n * 128, 128)], target.at[n, own], load_sem.at[slot, n, part]
        )

    for copy in small[:5]:
        copy.start()
    for part in range(blocks):
        for n in range(parts):
            load(n, part, u_hbm, u_ref, 0).start()
            load(n, part, kappa_hbm, k_ref, 1).start()
    for copy in small[5:]:
        copy.start()

    far_in[...] = jnp.zeros(far_in.shape, F32)
    mort_in[...] = jnp.zeros(mort_in.shape, F32)

    barrier = pltpu.get_barrier_semaphore()

    def greet(step, carry):
        other = lax.rem(me + step, n_dom)
        pl.semaphore_signal(barrier, inc=1, device_id=(other, sub), device_id_type=MESH)
        return carry

    lax.fori_loop(1, n_dom, greet, 0, unroll=n_dom <= 8)

    @pl.when(sub > 0)
    def _():
        pl.semaphore_signal(barrier, inc=1, device_id=(me, sub - 1), device_id_type=MESH)

    @pl.when(sub < n_sub - 1)
    def _():
        pl.semaphore_signal(barrier, inc=1, device_id=(me, sub + 1), device_id_type=MESH)

    def clear(missing, slot):
        @pl.when(missing)
        def _():
            side_in[slot] = jnp.zeros(side_in.shape[1:], F32)

    clear(sub == 0, 0)
    clear(sub == n_sub - 1, 1)
    clear(me == 0, 2)
    clear(me == n_dom - 1, 3)

    pairs, rim, near = local_ref.shape[1], sub_ref.shape[1], near_ref.shape[1]
    far, groups = far_ref.shape[1], child_ref.shape[1]
    shifts = far // FAR
    farp, groupp, coarsep = up(far), up(groups), up(n_dom)
    coarse_at = 2 * farp
    kids_at = coarse_at + coarsep
    used = kids_at + 4 * groupp
    sources = up(used, 128)
    lane = lax.broadcasted_iota(I32, (8, sources), 1)
    row8 = lax.broadcasted_iota(I32, (8, sources), 0)
    on_low = (lane < farp) | (lane >= kids_at)
    on_low_plane = jnp.concatenate([on_low] * NPTS, axis=0)
    reach = [
        jnp.where(on_low, float(WEIGHTS[c] * DERIV[c, 0]), float(WEIGHTS[c] * DERIV[c, last]))
        for c in range(NPTS)
    ]
    turn8 = []
    for r in range(NPTS):
        table = jnp.zeros((8, sources), F32)
        for b in range(NPTS):
            table = jnp.where(row8 == b, float(DERIV[b, (b + r) % NPTS]), table)
        turn8.append(table)
    quad8 = jnp.zeros((8, sources), F32)
    for k in range(NPTS):
        quad8 = jnp.where(row8 == k, float(WEIGHTS[k]), quad8)

    for copy in small[:5]:
        copy.wait()

    columns = [
        column(far_ref[0:1], farp) - float(4 * elems),
        column(far_ref[1:2], farp) - float(5 * elems),
        column(coarse_ref[...], coarsep) - float(5 * elems),
    ] + [column(child_ref[m : m + 1], groupp) - float(4 * elems) for m in range(4)]
    columns.append(jnp.full((sources - used, 1), -1.0, F32))
    hot_src = hot_rows(columns, 0, elems)

    scale = jnp.exp2(-level_ref[...].astype(F32))
    over = ((1,), (1,))
    chosen = dot(jnp.broadcast_to(scale, (16, elems)).astype(BF16), hot_src, over)[0:8]
    chosen = chosen * quad8

    for n in range(blocks * parts):
        load(n // blocks, n % blocks, u_hbm, u_ref, 0).wait()
        load(n // blocks, n % blocks, kappa_hbm, k_ref, 1).wait()

    def pick(ref, k):
        own = pl.ds(k, square, NPTS)
        high, low = halves_of(jnp.concatenate([ref[n, own, :] for n in range(parts)], axis=1))
        return dot(high, hot_src, over) + dot(low, hot_src, over)

    order = [0, last] + list(range(1, last))
    u_of, k_of = [None] * NPTS, [None] * NPTS
    for k in order:
        u_of[k], k_of[k] = pick(u_ref, k), pick(k_ref, k)
    u_plane = jnp.where(on_low_plane, u_of[0], u_of[last])
    k_plane = jnp.where(on_low_plane, k_of[0], k_of[last])

    def strip(plane, i):
        return plane[i * NPTS : (i + 1) * NPTS]

    edge = float(WEIGHTS[0])
    up_i = line([strip(u_plane, i) for i in range(NPTS)], DERIV)
    along_k, along_i, along_j = [], [], []
    for i in range(NPTS):
        here = chosen * float(WEIGHTS[i])
        g = strip(k_plane, i) * (here * edge)
        along_i.append(up_i[i] * g)
        flat = strip(u_plane, i)
        turned = turn8[0] * flat
        for r in range(1, NPTS):
            turned += turn8[r] * pltpu.roll(flat, NPTS - r, 0)
        along_j.append(turned * g)
        deep = line([strip(u_of[k], i) for k in range(NPTS)], DERIV)
        total = reach[0] * strip(k_of[0], i) * deep[0]
        for c in range(1, NPTS):
            total += reach[c] * strip(k_of[c], i) * deep[c]
        along_k.append(total * here)
    flux = jnp.concatenate(along_k + along_i + along_j, axis=0).T

    small[5].wait()
    fold = fold_ref.shape[0] // 2

    def folded(rows, first, width):
        high, low = halves_of(rows)
        cols = pl.ds(first, width)
        return (
            dot(high, fold_ref[0:fold, cols])
            + dot(low, fold_ref[0:fold, cols])
            + dot(high, fold_ref[fold:, cols])
        )

    own = folded(flux[0:up(used, 16)], 0, 128)
    kids = folded(flux[kids_at:used], 128, 256)
    raised = folded(flux[coarse_at:kids_at], 384, 256)

    half = lax.broadcasted_iota(I32, (8, 128), 1) < square
    for side in range(2):
        for first in range(0, farp, 8):
            faces = own[side * farp + first : side * farp + first + 8]
            far_out[side, first : first + 8] = jnp.where(half, faces, pltpu.roll(faces, 6, 0))
    half_g = lax.broadcasted_iota(I32, (groupp, 128), 1) < square
    kid = [kids[m * groupp : (m + 1) * groupp] for m in range(4)]
    projected = jnp.where(half_g, kid[0][:, 0:128], kid[1][:, 0:128]) + jnp.where(
        half_g, kid[2][:, 128:256], kid[3][:, 128:256]
    )
    peer_row = lax.broadcasted_iota(I32, (n_dom, 128), 0)
    routed = jnp.zeros((n_dom, 128), F32)
    for slot in range(groups):
        routed = jnp.where(peer_row == peer_ref[slot], projected[slot : slot + 1], routed)
    mort_out[pl.ds(0, n_dom, 8), :] = routed
    mort_out[pl.ds(1, n_dom, 8), :] = raised[0:n_dom, 0:128]
    mort_out[pl.ds(2, n_dom, 8), :] = raised[0:n_dom, 128:256]

    greeted = n_dom - 1 + (sub > 0).astype(I32) + (sub < n_sub - 1).astype(I32)

    def mail(step, landing):
        other = lax.rem(me + step, n_dom)
        return pltpu.make_async_remote_copy(
            src_ref=mort_out.at[pl.ds(pl.multiple_of(other * 8, 8), 3)],
            dst_ref=mort_in.at[
                pl.ds(pl.multiple_of((other if landing else me) * 8, 8), 3)
            ],
            send_sem=mort_send.at[other],
            recv_sem=mort_recv.at[other if landing else me],
            device_id=(other, sub),
            device_id_type=MESH,
        )

    def far_copy(side, s, landing):
        other = me - s - 2 if side == 0 else me + s + 2
        rows = pl.ds(s * FAR, FAR // 2)
        there = side if landing else 1 - side
        return pltpu.make_async_remote_copy(
            src_ref=far_out.at[side, rows],
            dst_ref=far_in.at[there, rows],
            send_sem=far_send.at[side, s],
            recv_sem=far_recv.at[there, s],
            device_id=(other, sub),
            device_id_type=MESH,
        )

    def far_there(side, s):
        return me >= s + 2 if side == 0 else me + s + 2 < n_dom

    def send_messages():
        pl.semaphore_wait(barrier, greeted)

        def start_all(step, carry):
            mail(step, False).start()
            return carry

        lax.fori_loop(1, n_dom, start_all, 0, unroll=n_dom <= 8)
        for side in range(2):
            for s in range(shifts):
                @pl.when(far_there(side, s))
                def _():
                    far_copy(side, s, False).start()

    @pl.when(me > 0)
    def _():
        send_messages()

    for copy in small[6:]:
        copy.wait()

    hot0l = hot_rows([column(local_ref[1:2], up(pairs))], 0, elems)
    hot1l = hot_rows([column(local_ref[0:1], up(pairs))], elems, elems)
    hot0s = hot_rows([column(sub_ref[0:1], up(rim))], 0, elems)
    hot1s = hot_rows([column(sub_ref[1:2], up(rim))], elems, elems)
    hot2 = hot_rows([column(near_ref[0:1], up(near))], 2 * elems, elems)
    hot3 = hot_rows([column(near_ref[1:2], up(near))], 3 * elems, elems)

    sub8 = lax.broadcasted_iota(I32, (8, elems), 0)
    weight = jnp.zeros((8, elems), F32)
    for k in range(NPTS):
        weight = jnp.where(sub8 == k, float(WEIGHTS[k]), weight)
    weight = weight * scale

    def slab(i, j):
        return pl.ds((i * NPTS + j) * NPTS, NPTS)

    def across(ref, own):
        return jnp.concatenate([ref[n, own, :] for n in range(parts)], axis=1)

    def add_across(own, values):
        for n in range(parts):
            w_ref[n, own, :] += values[:, n * 128 : (n + 1) * 128]

    turns = [deriv_ref[128 * n : 128 * n + 128, :] for n in range(4)]

    def along(pair, values):
        high, low = halves_of(values)
        both = jnp.concatenate([high, low], axis=0)
        return dot(jnp.concatenate([pair[0], pair[0]], axis=1), both) + dot(pair[1], high)

    for n in range(parts):
        here = weight[:, n * 128 : (n + 1) * 128]
        for i in range(NPTS):
            for j in range(NPTS):
                g_ref[n, slab(i, j), :] = k_ref[n, slab(i, j), :] * (
                    here * float(WEIGHTS[i] * WEIGHTS[j])
                )
    for part in range(blocks):
        own_rows = pl.ds(part * block, block)
        turn = along(turns[0:2], across(u_ref, own_rows)) * across(g_ref, own_rows)
        turn = along(turns[2:4], turn)
        for n in range(parts):
            w_ref[n, own_rows, :] = turn[:, n * 128 : (n + 1) * 128]
    for n in range(parts):
        for j in range(NPTS):
            turn = line([u_ref[n, slab(i, j), :] for i in range(NPTS)], DERIV)
            turn = [turn[i] * g_ref[n, slab(i, j), :] for i in range(NPTS)]
            turn = line(turn, DERIV.T)
            for i in range(NPTS):
                w_ref[n, slab(i, j), :] += turn[i]
        for i in range(NPTS):
            turn = line([u_ref[n, slab(i, j), :] for j in range(NPTS)], DERIV)
            turn = [turn[j] * g_ref[n, slab(i, j), :] for j in range(NPTS)]
            turn = line(turn, DERIV.T)
            for j in range(NPTS):
                w_ref[n, slab(i, j), :] += turn[j]

    low_i, high_i = pl.ds(0, square), pl.ds(last * square, square)
    low_k, high_k = pl.ds(0, square, NPTS), pl.ds(last, square, NPTS)
    face0 = across(w_ref, low_i)
    face1 = across(w_ref, high_i)
    face2 = jnp.concatenate([across(w_ref, slab(i, 0)) for i in range(NPTS)], axis=0)
    face3 = jnp.concatenate([across(w_ref, slab(i, last)) for i in range(NPTS)], axis=0)
    side_out[0, 0:rim, 0:square] = take_rows(hot0s, face0)[0:rim]
    side_out[1, 0:rim, 0:square] = take_rows(hot1s, face1)[0:rim]
    side_out[2, 0:near, 0:square] = take_rows(hot2, face2)[0:near]
    side_out[3, 0:near, 0:square] = take_rows(hot3, face3)[0:near]

    @pl.when(me == 0)
    def _():
        send_messages()

    sides = [
        (sub > 0, 0, 1, (me, sub - 1)),
        (sub < n_sub - 1, 1, 0, (me, sub + 1)),
        (me > 0, 2, 3, (me - 1, sub)),
        (me < n_dom - 1, 3, 2, (me + 1, sub)),
    ]

    def side_copy(mine, theirs, device):
        return pltpu.make_async_remote_copy(
            src_ref=side_out.at[mine],
            dst_ref=side_in.at[theirs],
            send_sem=side_send.at[mine],
            recv_sem=side_recv.at[theirs],
            device_id=device,
            device_id_type=MESH,
        )

    for there, mine, theirs, device in sides:
        @pl.when(there)
        def _():
            side_copy(mine, theirs, device).start()

    keyed = up(2 * farp + 8 * n_dom, 128)

    def landing_rows(keys):
        at = lax.broadcasted_iota(I32, (2 * keyed, sources), 0)
        hit = at == keys[0]
        for key in keys[1:]:
            hit = hit | (at == key)
        return dot(jnp.where(hit, 1.0, 0.0).astype(BF16), hot_src).astype(BF16)

    src = lax.broadcasted_iota(I32, (1, sources), 1)

    def far_key(first):
        f = src - first
        s, j = lax.shift_right_logical(f, 2), lax.bitwise_and(f, FAR - 1)
        key = lax.shift_right_logical(j, 1) * keyed + first + 4 * s + lax.bitwise_and(j, 1)
        return jnp.where((f >= 0) & (f < far), key, -1)

    key4 = far_key(0)
    for m in range(4):
        for slot in range(groups):
            key = (m & 1) * keyed + 2 * farp + peer_ref[slot] * 8 + 1 + (m >> 1)
            key4 = jnp.where(src == kids_at + m * groupp + slot, key, key4)
    key5 = far_key(farp)
    p = src - coarse_at
    holds = (p >= 0) & (p < n_dom)
    key5 = jnp.where(holds, 2 * farp + 8 * p, key5)
    land4 = landing_rows([key4])
    land5 = landing_rows([key5, jnp.where(holds, keyed + 2 * farp + 8 * p, -1)])

    joined = projected[:, 0:square] + projected[:, square:]
    lift = [mortar_ref[m * square : (m + 1) * square, :] for m in range(4)]
    share = []
    for m in range(4):
        first = kids_at + m * groupp
        share.append(product(joined, lift[m]) - own[first : first + groupp, 0:square])
    hot_kids = hot_src[kids_at:used]
    add_across(low_k, spread_rows(jnp.concatenate(share, axis=0), hot_kids))
    add_across(low_i, spread_rows(take_rows(hot1l, face1), hot0l))
    add_across(high_i, spread_rows(take_rows(hot0l, face0), hot1l))

    for there, mine, theirs, device in sides:
        @pl.when(there)
        def _():
            side_copy(mine, mine, device).wait()

    add_across(low_i, spread_rows(side_in[0, 0:rim, 0:square], hot0s))
    add_across(high_i, spread_rows(side_in[1, 0:rim, 0:square], hot1s))
    add2 = spread_rows(side_in[2, 0:near, 0:square], hot2)
    add3 = spread_rows(side_in[3, 0:near, 0:square], hot3)
    for i in range(NPTS):
        add_across(slab(i, 0), add2[i * NPTS : (i + 1) * NPTS])
        add_across(slab(i, last), add3[i * NPTS : (i + 1) * NPTS])

    def wait_all(step, carry):
        mail(step, True).wait()
        return carry

    lax.fori_loop(1, n_dom, wait_all, 0, unroll=n_dom <= 8)
    for side in range(2):
        for s in range(shifts):
            @pl.when(far_there(side, s))
            def _():
                far_copy(side, s, True).wait()

    received = [far_in[0], far_in[1], mort_in[...]]
    spare = keyed - 2 * farp - 8 * n_dom
    if spare:
        received.append(jnp.zeros((spare, 128), F32))
    received = jnp.concatenate(received, axis=0).T
    received = jnp.concatenate([received[0:square], received[square:]], axis=1)
    high, low = halves_of(received)
    add_across(low_k, dot(high, land4) + dot(low, land4))
    add_across(high_k, dot(high, land5) + dot(low, land5))
    for n in range(parts):
        out_ref[:, n * 128 : (n + 1) * 128] = w_ref[n]


def body(
    sizes,
    nodal_values,
    kappa,
    levels,
    local_faces,
    sub_faces,
    near_faces,
    far_faces,
    child_faces,
    child_peer,
    coarse_faces,
):
    n_dom, n_sub = sizes
    elems = nodal_values.shape[1]
    krons = [np.kron(HALVES[m // 2], HALVES[m % 2]) for m in range(4)]
    mortar = np.concatenate([m.T for m in krons], axis=0)
    far_rows = up(far_faces.shape[1])
    held = (elems // 128, NPTS**3, 128)
    side_rows = up(max(sub_faces.shape[1], near_faces.shape[1]))
    small = [
        levels.reshape(1, elems),
        local_faces,
        sub_faces,
        near_faces,
        far_faces,
        child_faces,
        coarse_faces.reshape(1, n_dom),
        jnp.asarray(folds(krons), BF16),
        jnp.asarray(stencils(), BF16),
        jnp.asarray(mortar, F32),
    ]
    hbm = pl.BlockSpec(memory_space=pltpu.HBM)
    vmem = pl.BlockSpec(memory_space=pltpu.VMEM)
    return pl.pallas_call(
        functools.partial(kernel, sizes),
        out_shape=pltpu.VMEM(nodal_values.shape, F32),
        in_specs=[hbm] * 13,
        out_specs=vmem,
        scratch_shapes=[pltpu.VMEM(item.shape, item.dtype) for item in small]
        + [
            pltpu.SMEM(child_peer.shape, I32),
            pltpu.VMEM(held, F32),
            pltpu.VMEM(held, F32),
            pltpu.VMEM(held, F32),
            pltpu.VMEM(held, F32),
            pltpu.VMEM((4, side_rows, 128), F32),
            pltpu.VMEM((4, side_rows, 128), F32),
            pltpu.VMEM((2, far_rows, 128), F32),
            pltpu.VMEM((2, far_rows, 128), F32),
            pltpu.VMEM((n_dom * 8, 128), F32),
            pltpu.VMEM((n_dom * 8, 128), F32),
            pltpu.SemaphoreType.DMA((len(small) + 1,)),
            pltpu.SemaphoreType.DMA((2, held[0], NPTS**3 // 128)),
            pltpu.SemaphoreType.DMA((4,)),
            pltpu.SemaphoreType.DMA((4,)),
            pltpu.SemaphoreType.DMA((2, far_faces.shape[1] // FAR)),
            pltpu.SemaphoreType.DMA((2, far_faces.shape[1] // FAR)),
            pltpu.SemaphoreType.DMA((n_dom,)),
            pltpu.SemaphoreType.DMA((n_dom,)),
        ],
        compiler_params=pltpu.CompilerParams(
            collective_id=0, has_side_effects=True, vmem_limit_bytes=60 * 1024 * 1024
        ),
    )(
        nodal_values,
        kappa,
        *small,
        child_peer,
    )


def solution(mesh):
    sizes = (mesh.shape["dom"], mesh.shape["sub"])
    wide = P(None, ("dom", "sub"))
    flat = P(("dom", "sub"))
    in_specs = (wide, wide, flat, wide, wide, wide, wide, wide, flat, flat)
    return jax.shard_map(
        functools.partial(body, sizes),
        mesh=mesh,
        in_specs=in_specs,
        out_specs=wide,
        check_vma=False,
    )
```

```python
import functools

import jax
import jax.numpy as jnp
import numpy as np
from jax import lax
from jax.experimental import pallas as pl
from jax.experimental.pallas import tpu as pltpu
from jax.sharding import PartitionSpec as P

NPTS = 8
FAR = 4
MESH = pl.DeviceIdType.MESH
F32, BF16, I32 = jnp.float32, jnp.bfloat16, jnp.int32


def legendre_table(points, degree):
    table = [np.ones(points.shape), points.copy()]
    for order in range(2, degree + 1):
        table.append(
            ((2 * order - 1) * points * table[order - 1] - (order - 1) * table[order - 2]) / order
        )
    return table


def lobatto_points(degree):
    points = np.cos(np.pi * np.arange(degree + 1) / degree)
    for sweep in range(100):
        table = legendre_table(points, degree)
        points = points - (points * table[degree] - table[degree - 1]) / (
            (degree + 1) * table[degree]
        )
    points = np.sort(points)
    return (points, legendre_table(points, degree)[degree])


def node_tables(count):
    degree = count - 1
    points, legendre = lobatto_points(degree)
    weights = 2.0 / (degree * (degree + 1) * legendre**2)
    spread = points[:, None] - points[None, :] + np.eye(count)
    derivative = legendre[:, None] / (legendre[None, :] * spread) * (1.0 - np.eye(count))
    derivative[0, 0] = -degree * (degree + 1) / 4.0
    derivative[degree, degree] = degree * (degree + 1) / 4.0
    halves = []
    for side in range(2):
        target = (points + 2.0 * side - 1.0) / 2.0
        matrix = np.ones((count, count))
        for column in range(count):
            for other in range(count):
                if other != column:
                    matrix[:, column] = (
                        matrix[:, column]
                        * (target - points[other])
                        / (points[column] - points[other])
                    )
        halves.append(matrix)
    return (points, weights, derivative, np.stack(halves))


POINTS, WEIGHTS, DERIV, HALVES = node_tables(NPTS)


def up(count, unit=8):
    return -(-count // unit) * unit


def halves_of(values):
    high = values.astype(BF16)
    return high, (values - high.astype(F32)).astype(BF16)


def numpy_halves(matrix):
    matrix = np.asarray(matrix, np.float32)
    high = matrix.astype(jnp.bfloat16)
    low = (matrix - high.astype(np.float32)).astype(jnp.bfloat16)
    return high, low


def dot(a, b, dims=((1,), (0,))):
    return lax.dot_general(a, b, (dims, ((), ())), preferred_element_type=F32)


def select(hot, values):
    high, low = halves_of(values)
    return dot(hot, high) + dot(hot, low)


def take_rows(hot, face):
    high, low = halves_of(face)
    dims = ((1,), (1,))
    return dot(hot, high, dims) + dot(hot, low, dims)


def spread_rows(rows, hot):
    high, low = halves_of(rows.T)
    return dot(high, hot) + dot(low, hot)


def product(a, matrix):
    high, low = halves_of(a)
    mhigh, mlow = halves_of(matrix)
    return dot(high, mhigh) + dot(low, mhigh) + dot(high, mlow)


def column(row, padded):
    count = row.shape[1]
    r = lax.broadcasted_iota(I32, (padded, count), 0)
    c = lax.broadcasted_iota(I32, (padded, count), 1)
    spread = jnp.where(r == c, jnp.broadcast_to(row.astype(F32), (padded, count)), 0.0)
    col = jnp.sum(spread, axis=1, keepdims=True)
    inside = lax.broadcasted_iota(I32, (padded, 1), 0) < count
    return jnp.where(inside, col, -1.0)


def hot_rows(columns, base, elems, kind=BF16):
    col = columns[0] if len(columns) == 1 else jnp.concatenate(columns, axis=0)
    lane = lax.broadcasted_iota(I32, (col.shape[0], elems), 1).astype(F32)
    return jnp.where(lane == col - float(base), 1.0, 0.0).astype(kind)


def line(values, matrix):
    half = NPTS // 2
    even = [values[i] + values[NPTS - 1 - i] for i in range(half)]
    odd = [values[i] - values[NPTS - 1 - i] for i in range(half)]
    out = [None] * NPTS
    for a in range(half):
        p = q = None
        for i in range(half):
            s = float((matrix[a, i] + matrix[a, NPTS - 1 - i]) / 2)
            t = float((matrix[a, i] - matrix[a, NPTS - 1 - i]) / 2)
            p = even[i] * s if p is None else p + even[i] * s
            q = odd[i] * t if q is None else q + odd[i] * t
        out[a] = q + p
        out[NPTS - 1 - a] = q - p
    return out


def stencils():
    forth, back = np.kron(np.eye(16), DERIV), np.kron(np.eye(16), DERIV.T)
    pieces = [piece for table in (forth, back) for piece in numpy_halves(table)]
    return np.concatenate(pieces, axis=0)


def folds():
    eye = np.eye(NPTS)
    heads = [(eye, eye)] * 2
    heads += [(HALVES[m // 2], HALVES[m % 2]) for m in range(4)]
    heads += [(HALVES[m // 2].T, HALVES[m % 2].T) for m in range(4)]
    rows, tiles = [], []
    for turn in (eye, DERIV):
        rows.append([np.repeat(turn @ first, NPTS, axis=1) for first, _ in heads])
        tiles.append([np.tile(turn @ second, (1, NPTS)) for _, second in heads])
    table = [np.concatenate(kind, axis=1) for kind in rows + tiles]
    return np.concatenate(table, axis=0).astype(np.float32)


def steps(
    sizes,
    u_hbm,
    kappa_hbm,
    level_hbm,
    local_hbm,
    sub_hbm,
    near_hbm,
    fold_hbm,
    deriv_hbm,
    mortar_hbm,
    far_hbm,
    child_hbm,
    peer_hbm,
    coarse_hbm,
    out_ref,
    level_ref,
    local_ref,
    sub_ref,
    near_ref,
    fold_ref,
    deriv_ref,
    mortar_ref,
    far_ref,
    child_ref,
    peer_ref,
    coarse_ref,
    w_ref,
    uk_ref,
    g_ref,
    side_out,
    side_in,
    far_out,
    far_in,
    mort_out,
    mort_in,
    side_recv,
    far_recv,
    mort_recv,
    small_sem,
    load_sem,
    side_send,
    far_send,
    mort_send,
):
    n_dom, n_sub = sizes
    u_ref, k_ref = uk_ref.at[0], uk_ref.at[1]
    parts = u_ref.shape[0]
    elems = parts * 128
    square = NPTS * NPTS
    last = NPTS - 1
    me, sub = lax.axis_index("dom"), lax.axis_index("sub")

    urgent = [
        (fold_hbm, fold_ref),
        (far_hbm, far_ref),
        (child_hbm, child_ref),
        (coarse_hbm, coarse_ref),
        (level_hbm, level_ref),
        (peer_hbm, peer_ref),
    ]
    later = [
        (local_hbm, local_ref),
        (sub_hbm, sub_ref),
        (near_hbm, near_ref),
        (deriv_hbm, deriv_ref),
        (mortar_hbm, mortar_ref),
    ]
    small = [
        pltpu.make_async_copy(source, target, small_sem.at[slot])
        for slot, (source, target) in enumerate(urgent + later)
    ]
    block = 128
    blocks = NPTS**3 // block

    def load(n, part, source, target):
        own = pl.ds(part * block, block)
        return pltpu.make_async_copy(
            source.at[own, pl.ds(n * 128, 128)], target.at[n, own], load_sem.at[part]
        )

    def loaded(part):
        whole = uk_ref.at[0, :, pl.ds(0, 2 * block)]
        pltpu.make_async_copy(whole, whole, load_sem.at[part]).wait()

    for copy in small[:6]:
        copy.start()
    for part in range(blocks):
        for n in range(parts):
            load(n, part, u_hbm, u_ref).start()
            load(n, part, kappa_hbm, k_ref).start()
    for copy in small[6:]:
        copy.start()

    far_in[...] = jnp.zeros(far_in.shape, F32)
    mort_in[...] = jnp.zeros(mort_in.shape, F32)

    barrier = pltpu.get_barrier_semaphore()

    def greet(step, carry):
        other = lax.rem(me + step, n_dom)
        pl.semaphore_signal(barrier, inc=1, device_id=(other, sub), device_id_type=MESH)
        return carry

    lax.fori_loop(1, n_dom, greet, 0, unroll=n_dom <= 8)

    @pl.when(sub > 0)
    def _():
        pl.semaphore_signal(barrier, inc=1, device_id=(me, sub - 1), device_id_type=MESH)

    @pl.when(sub < n_sub - 1)
    def _():
        pl.semaphore_signal(barrier, inc=1, device_id=(me, sub + 1), device_id_type=MESH)

    def clear(missing, slot):
        @pl.when(missing)
        def _():
            side_in[slot] = jnp.zeros(side_in.shape[1:], F32)

    clear(sub == 0, 0)
    clear(sub == n_sub - 1, 1)
    clear(me == 0, 2)
    clear(me == n_dom - 1, 3)

    pairs, rim, near = local_ref.shape[1], sub_ref.shape[1], near_ref.shape[1]
    far, groups = far_ref.shape[1], child_ref.shape[1]
    shifts = far // FAR
    farp, groupp, coarsep = up(far), up(groups), up(n_dom)
    coarse_at = 2 * farp
    kids_at = coarse_at + coarsep
    used = kids_at + 4 * groupp
    sources = up(used, 128)
    lane = lax.broadcasted_iota(I32, (8, sources), 1)
    row8 = lax.broadcasted_iota(I32, (8, sources), 0)
    on_low = (lane < farp) | (lane >= kids_at)
    reach = [
        jnp.where(on_low, float(WEIGHTS[c] * DERIV[c, 0]), float(WEIGHTS[c] * DERIV[c, last]))
        for c in range(NPTS)
    ]
    turn8 = []
    for r in range(NPTS):
        table = jnp.zeros((8, sources), F32)
        for b in range(NPTS):
            table = jnp.where(row8 == b, float(DERIV[b, (b + r) % NPTS]), table)
        turn8.append(table)
    quad8 = jnp.zeros((8, sources), F32)
    for k in range(NPTS):
        quad8 = jnp.where(row8 == k, float(WEIGHTS[k]), quad8)

    for copy in small[:6]:
        copy.wait()

    def held(first, ids, base):
        total = jnp.zeros((8, sources), I32)
        for slot, value in enumerate(ids):
            total = jnp.where(lane == first + slot, value + (1 - base * elems), total)
        return total

    ids = held(0, [far_ref[0, c] for c in range(far)], 4)
    ids += held(farp, [far_ref[1, c] for c in range(far)], 5)
    ids += held(coarse_at, [coarse_ref[c] for c in range(n_dom)], 5)
    for m in range(4):
        ids += held(kids_at + m * groupp, [child_ref[m, c] for c in range(groups)], 4)
    fold = []
    for rows_kind, tile_kind in ((0, 0), (1, 0), (0, 1)):
        tile = fold_ref[(2 + tile_kind) * NPTS : (3 + tile_kind) * NPTS, :]
        for i in range(NPTS):
            at = rows_kind * NPTS + i
            fold.append(fold_ref[at : at + 1, :] * tile)
    fold_high, fold_low = halves_of(jnp.concatenate(fold, axis=0))
    element = lax.broadcasted_iota(I32, (elems, sources), 0) + 1
    hot_src = jnp.where(element == ids[0:1], 1.0, 0.0).astype(BF16)
    scale = jnp.exp2(-level_ref[...].astype(F32))
    over = ((1,), (1,))

    def pick(ref, part):
        rows = []
        for k in range(NPTS):
            own = pl.ds(part * block + k, block // NPTS, NPTS)
            rows.append(jnp.concatenate([ref[n, own, :] for n in range(parts)], axis=1))
        high, low = halves_of(jnp.concatenate(rows, axis=0))
        both = dot(jnp.concatenate([high, low], axis=0), hot_src)
        return both[0:block] + both[block:]

    spot = jnp.bitwise_and(ids - 1, 127)
    piece = lax.shift_right_arithmetic(ids - 1, 7)
    lookup = lax.GatherDimensionNumbers(
        offset_dims=(),
        collapsed_slice_dims=(1,),
        start_index_map=(1,),
        operand_batching_dims=(0,),
        start_indices_batching_dims=(0,),
    )

    def fetch(ref, part):
        rows = []
        for k in range(NPTS):
            for at in range(0, block, NPTS * NPTS):
                own = pl.ds(part * block + at + k, NPTS, NPTS)
                tiles = []
                for first in range(0, sources, 128):
                    where = slice(first, first + 128)
                    found = jnp.zeros((8, 128), F32)
                    for n in range(parts):
                        taken = lax.gather(
                            ref[n, own, :],
                            spot[:, where][..., None],
                            lookup,
                            slice_sizes=(1, 1),
                            mode=lax.GatherScatterMode.PROMISE_IN_BOUNDS,
                        )
                        found = jnp.where(piece[:, where] == n, taken, found)
                    tiles.append(found)
                rows.append(tiles[0] if len(tiles) == 1 else jnp.concatenate(tiles, axis=1))
        return jnp.concatenate(rows, axis=0)

    edge = float(WEIGHTS[0])
    chosen = None
    along_k, along_j, plane_u, plane_g = [], [], [], []
    for part in range(blocks):
        loaded(part)
    for part in range(blocks):
        u_part, k_part = fetch(u_ref, part), pick(k_ref, part)
        if chosen is None:
            chosen = dot(jnp.broadcast_to(scale, (16, elems)).astype(BF16), hot_src)[0:8]
            chosen = chosen * quad8
        wide = block // NPTS
        for i in range(part * wide // NPTS, (part + 1) * wide // NPTS):
            at = i * NPTS - part * wide

            def strip(values, k):
                return values[k * wide + at : k * wide + at + NPTS]

            here = chosen * float(WEIGHTS[i])
            flat = jnp.where(on_low, strip(u_part, 0), strip(u_part, last))
            g = jnp.where(on_low, strip(k_part, 0), strip(k_part, last)) * (here * edge)
            plane_u.append(flat)
            plane_g.append(g)
            turned = turn8[0] * flat
            for r in range(1, NPTS):
                turned += turn8[r] * pltpu.roll(flat, NPTS - r, 0)
            along_j.append(turned * g)
            deep = line([strip(u_part, k) for k in range(NPTS)], DERIV)
            total = reach[0] * strip(k_part, 0) * deep[0]
            for c in range(1, NPTS):
                total += reach[c] * strip(k_part, c) * deep[c]
            along_k.append(total * here)
    across_i = line(plane_u, DERIV)
    along_i = [across_i[i] * plane_g[i] for i in range(NPTS)]
    flux = jnp.concatenate(along_k + along_i + along_j, axis=0)

    flux = flux.T

    def folded(rows, first, width):
        high, low = halves_of(rows)
        cols = slice(first, first + width)
        return (
            dot(high, fold_high[:, cols])
            + dot(low, fold_high[:, cols])
            + dot(high, fold_low[:, cols])
        )

    raised = folded(flux[coarse_at:kids_at], 384, 256)
    kids = folded(flux[kids_at:used], 128, 256)
    own = folded(flux[0 : up(used, 16)], 0, 128)

    half = lax.broadcasted_iota(I32, (8, 128), 1) < square
    for side in range(2):
        for first in range(0, farp, 8):
            faces = own[side * farp + first : side * farp + first + 8]
            far_out[side, first : first + 8] = jnp.where(half, faces, pltpu.roll(faces, 6, 0))
    half_g = lax.broadcasted_iota(I32, (groupp, 128), 1) < square
    kid = [kids[m * groupp : (m + 1) * groupp] for m in range(4)]
    projected = jnp.where(half_g, kid[0][:, 0:128], kid[1][:, 0:128]) + jnp.where(
        half_g, kid[2][:, 128:256], kid[3][:, 128:256]
    )
    peer_row = lax.broadcasted_iota(I32, (n_dom, 128), 0)
    routed = jnp.zeros((n_dom, 128), F32)
    for slot in range(groups):
        routed = jnp.where(peer_row == peer_ref[slot], projected[slot : slot + 1], routed)
    mort_out[pl.ds(0, n_dom, 8), :] = routed
    mort_out[pl.ds(1, n_dom, 8), :] = raised[0:n_dom, 0:128]
    mort_out[pl.ds(2, n_dom, 8), :] = raised[0:n_dom, 128:256]

    greeted = n_dom - 1 + (sub > 0).astype(I32) + (sub < n_sub - 1).astype(I32)

    def mail(step, landing):
        other = lax.rem(me + step, n_dom)
        return pltpu.make_async_remote_copy(
            src_ref=mort_out.at[pl.ds(pl.multiple_of(other * 8, 8), 3)],
            dst_ref=mort_in.at[
                pl.ds(pl.multiple_of((other if landing else me) * 8, 8), 3)
            ],
            send_sem=mort_send.at[other],
            recv_sem=mort_recv.at[other if landing else me],
            device_id=(other, sub),
            device_id_type=MESH,
        )

    def far_copy(side, s, landing):
        other = me - s - 2 if side == 0 else me + s + 2
        rows = pl.ds(s * FAR, FAR // 2)
        there = side if landing else 1 - side
        return pltpu.make_async_remote_copy(
            src_ref=far_out.at[side, rows],
            dst_ref=far_in.at[there, rows],
            send_sem=far_send.at[side, s],
            recv_sem=far_recv.at[there, s],
            device_id=(other, sub),
            device_id_type=MESH,
        )

    def far_there(side, s):
        return me >= s + 2 if side == 0 else me + s + 2 < n_dom

    def send_messages():
        pl.semaphore_wait(barrier, greeted)

        def start_all(step, carry):
            mail(step, False).start()
            return carry

        lax.fori_loop(1, n_dom, start_all, 0, unroll=n_dom <= 8)
        for side in range(2):
            for s in range(shifts):
                @pl.when(far_there(side, s))
                def _():
                    far_copy(side, s, False).start()

    @pl.when(me > 0)
    def _():
        send_messages()

    for copy in small[6:]:
        copy.wait()

    hot0l = hot_rows([column(local_ref[1:2], up(pairs))], 0, elems)
    hot1l = hot_rows([column(local_ref[0:1], up(pairs))], elems, elems)
    hot0s = hot_rows([column(sub_ref[0:1], up(rim))], 0, elems)
    hot1s = hot_rows([column(sub_ref[1:2], up(rim))], elems, elems)
    hot2 = hot_rows([column(near_ref[0:1], up(near))], 2 * elems, elems)
    hot3 = hot_rows([column(near_ref[1:2], up(near))], 3 * elems, elems)

    sub8 = lax.broadcasted_iota(I32, (8, elems), 0)
    weight = jnp.zeros((8, elems), F32)
    for k in range(NPTS):
        weight = jnp.where(sub8 == k, float(WEIGHTS[k]), weight)
    weight = weight * scale

    def slab(i, j):
        return pl.ds((i * NPTS + j) * NPTS, NPTS)

    def across(ref, own):
        return jnp.concatenate([ref[n, own, :] for n in range(parts)], axis=1)

    def add_across(own, values):
        for n in range(parts):
            w_ref[n, own, :] += values[:, n * 128 : (n + 1) * 128]

    turns = [deriv_ref[128 * n : 128 * n + 128, :] for n in range(4)]

    def along(pair, values):
        high, low = halves_of(values)
        both = jnp.concatenate([high, low], axis=0)
        return dot(jnp.concatenate([pair[0], pair[0]], axis=1), both) + dot(pair[1], high)

    for n in range(parts):
        here = weight[:, n * 128 : (n + 1) * 128]
        for i in range(NPTS):
            for j in range(NPTS):
                g_ref[n, slab(i, j), :] = k_ref[n, slab(i, j), :] * (
                    here * float(WEIGHTS[i] * WEIGHTS[j])
                )
    for part in range(blocks):
        own_rows = pl.ds(part * block, block)
        turn = along(turns[0:2], across(u_ref, own_rows)) * across(g_ref, own_rows)
        turn = along(turns[2:4], turn)
        for n in range(parts):
            w_ref[n, own_rows, :] = turn[:, n * 128 : (n + 1) * 128]
    for n in range(parts):
        for j in range(NPTS):
            turn = line([u_ref[n, slab(i, j), :] for i in range(NPTS)], DERIV)
            turn = [turn[i] * g_ref[n, slab(i, j), :] for i in range(NPTS)]
            turn = line(turn, DERIV.T)
            for i in range(NPTS):
                w_ref[n, slab(i, j), :] += turn[i]
        for i in range(NPTS):
            turn = line([u_ref[n, slab(i, j), :] for j in range(NPTS)], DERIV)
            turn = [turn[j] * g_ref[n, slab(i, j), :] for j in range(NPTS)]
            turn = line(turn, DERIV.T)
            for j in range(NPTS):
                w_ref[n, slab(i, j), :] += turn[j]

    low_i, high_i = pl.ds(0, square), pl.ds(last * square, square)
    low_k, high_k = pl.ds(0, square, NPTS), pl.ds(last, square, NPTS)
    face0 = across(w_ref, low_i)
    face1 = across(w_ref, high_i)
    face2 = jnp.concatenate([across(w_ref, slab(i, 0)) for i in range(NPTS)], axis=0)
    face3 = jnp.concatenate([across(w_ref, slab(i, last)) for i in range(NPTS)], axis=0)
    side_out[0, 0:rim, 0:square] = take_rows(hot0s, face0)[0:rim]
    side_out[1, 0:rim, 0:square] = take_rows(hot1s, face1)[0:rim]
    side_out[2, 0:near, 0:square] = take_rows(hot2, face2)[0:near]
    side_out[3, 0:near, 0:square] = take_rows(hot3, face3)[0:near]

    @pl.when(me == 0)
    def _():
        send_messages()

    sides = [
        (sub > 0, 0, 1, (me, sub - 1)),
        (sub < n_sub - 1, 1, 0, (me, sub + 1)),
        (me > 0, 2, 3, (me - 1, sub)),
        (me < n_dom - 1, 3, 2, (me + 1, sub)),
    ]

    def side_copy(mine, theirs, device):
        return pltpu.make_async_remote_copy(
            src_ref=side_out.at[mine],
            dst_ref=side_in.at[theirs],
            send_sem=side_send.at[mine],
            recv_sem=side_recv.at[theirs],
            device_id=device,
            device_id_type=MESH,
        )

    for there, mine, theirs, device in sides:
        @pl.when(there)
        def _():
            side_copy(mine, theirs, device).start()

    keyed = up(2 * farp + 8 * n_dom, 128)

    def landing_rows(keys):
        at = lax.broadcasted_iota(I32, (2 * keyed, sources), 0)
        hit = at == keys[0]
        for key in keys[1:]:
            hit = hit | (at == key)
        return dot(jnp.where(hit, 1.0, 0.0).astype(BF16), hot_src, over).astype(BF16)

    src = lax.broadcasted_iota(I32, (1, sources), 1)

    def far_key(first):
        f = src - first
        s, j = lax.shift_right_logical(f, 2), lax.bitwise_and(f, FAR - 1)
        key = lax.shift_right_logical(j, 1) * keyed + first + 4 * s + lax.bitwise_and(j, 1)
        return jnp.where((f >= 0) & (f < far), key, -1)

    key4 = far_key(0)
    for m in range(4):
        for slot in range(groups):
            key = (m & 1) * keyed + 2 * farp + peer_ref[slot] * 8 + 1 + (m >> 1)
            key4 = jnp.where(src == kids_at + m * groupp + slot, key, key4)
    key5 = far_key(farp)
    p = src - coarse_at
    holds = (p >= 0) & (p < n_dom)
    key5 = jnp.where(holds, 2 * farp + 8 * p, key5)
    land4 = landing_rows([key4])
    land5 = landing_rows([key5, jnp.where(holds, keyed + 2 * farp + 8 * p, -1)])

    joined = projected[:, 0:square] + projected[:, square:]
    lift = [mortar_ref[m * square : (m + 1) * square, :] for m in range(4)]
    share = []
    for m in range(4):
        first = kids_at + m * groupp
        share.append(product(joined, lift[m]) - own[first : first + groupp, 0:square])
    share = [jnp.zeros((kids_at, square), F32)] + share
    if sources > used:
        share.append(jnp.zeros((sources - used, square), F32))
    high, low = halves_of(jnp.concatenate(share, axis=0).T)
    add_across(low_k, dot(high, hot_src, over) + dot(low, hot_src, over))
    add_across(low_i, spread_rows(take_rows(hot1l, face1), hot0l))
    add_across(high_i, spread_rows(take_rows(hot0l, face0), hot1l))

    for there, mine, theirs, device in sides:
        @pl.when(there)
        def _():
            side_copy(mine, mine, device).wait()

    add_across(low_i, spread_rows(side_in[0, 0:rim, 0:square], hot0s))
    add_across(high_i, spread_rows(side_in[1, 0:rim, 0:square], hot1s))
    add2 = spread_rows(side_in[2, 0:near, 0:square], hot2)
    add3 = spread_rows(side_in[3, 0:near, 0:square], hot3)
    for i in range(NPTS):
        add_across(slab(i, 0), add2[i * NPTS : (i + 1) * NPTS])
        add_across(slab(i, last), add3[i * NPTS : (i + 1) * NPTS])

    def sent_all(step, carry):
        mail(step, True).wait_send()
        return carry

    lax.fori_loop(1, n_dom, sent_all, 0, unroll=n_dom <= 8)
    for side in range(2):
        for s in range(shifts):
            @pl.when(far_there(side, s))
            def _():
                far_copy(side, s, True).wait()

    def wait_all(step, carry):
        mail(step, True).wait_recv()
        return carry

    lax.fori_loop(1, n_dom, wait_all, 0, unroll=n_dom <= 8)

    received = [far_in[0], far_in[1], mort_in[...]]
    spare = keyed - 2 * farp - 8 * n_dom
    if spare:
        received.append(jnp.zeros((spare, 128), F32))
    received = jnp.concatenate(received, axis=0).T
    received = jnp.concatenate([received[0:square], received[square:]], axis=1)
    high, low = halves_of(received)
    add_across(low_k, dot(high, land4) + dot(low, land4))
    add_across(high_k, dot(high, land5) + dot(low, land5))
    for n in range(parts):
        out_ref[:, n * 128 : (n + 1) * 128] = w_ref[n]


def kernel(sizes, copies, *refs):
    n_dom, _ = sizes
    far_recv = refs[-2]
    pl.run_scoped(
        functools.partial(steps, sizes, *refs),
        pltpu.SemaphoreType.DMA((copies,)),
        pltpu.SemaphoreType.DMA((NPTS**3 // 128,)),
        pltpu.SemaphoreType.DMA((4,)),
        pltpu.SemaphoreType.DMA(far_recv.shape),
        pltpu.SemaphoreType.DMA((n_dom,)),
    )


def body(
    sizes,
    nodal_values,
    kappa,
    levels,
    local_faces,
    sub_faces,
    near_faces,
    far_faces,
    child_faces,
    child_peer,
    coarse_faces,
):
    n_dom, n_sub = sizes
    elems = nodal_values.shape[1]
    krons = [np.kron(HALVES[m // 2], HALVES[m % 2]) for m in range(4)]
    mortar = np.concatenate([m.T for m in krons], axis=0)
    far_rows = up(far_faces.shape[1])
    held = (elems // 128, NPTS**3, 128)
    side_rows = up(max(sub_faces.shape[1], near_faces.shape[1]))
    small = [
        levels.reshape(1, elems),
        local_faces,
        sub_faces,
        near_faces,
        jnp.asarray(folds(), F32),
        jnp.asarray(stencils(), BF16),
        jnp.asarray(mortar, F32),
    ]
    tables = [far_faces, child_faces, child_peer, coarse_faces]
    hbm = pl.BlockSpec(memory_space=pltpu.HBM)
    vmem = pl.BlockSpec(memory_space=pltpu.VMEM)
    return pl.pallas_call(
        functools.partial(kernel, sizes, len(small) + len(tables)),
        out_shape=pltpu.VMEM(nodal_values.shape, F32),
        in_specs=[hbm] * 13,
        out_specs=vmem,
        scratch_shapes=[pltpu.VMEM(item.shape, item.dtype) for item in small]
        + [pltpu.SMEM(item.shape, I32) for item in tables]
        + [
            pltpu.VMEM(held, F32),
            pltpu.VMEM((2, *held), F32),
            pltpu.VMEM(held, F32),
            pltpu.VMEM((4, side_rows, 128), F32),
            pltpu.VMEM((4, side_rows, 128), F32),
            pltpu.VMEM((2, far_rows, 128), F32),
            pltpu.VMEM((2, far_rows, 128), F32),
            pltpu.VMEM((n_dom * 8, 128), F32),
            pltpu.VMEM((n_dom * 8, 128), F32),
            pltpu.SemaphoreType.DMA((4,)),
            pltpu.SemaphoreType.DMA((2, far_faces.shape[1] // FAR)),
            pltpu.SemaphoreType.DMA((n_dom,)),
        ],
        compiler_params=pltpu.CompilerParams(
            collective_id=0, has_side_effects=True, vmem_limit_bytes=60 * 1024 * 1024
        ),
    )(
        nodal_values,
        kappa,
        *small,
        *tables,
    )


def solution(mesh):
    sizes = (mesh.shape["dom"], mesh.shape["sub"])
    wide = P(None, ("dom", "sub"))
    flat = P(("dom", "sub"))
    in_specs = (wide, wide, flat, wide, wide, wide, wide, wide, flat, flat)
    return jax.shard_map(
        functools.partial(body, sizes),
        mesh=mesh,
        in_specs=in_specs,
        out_specs=wide,
        check_vma=False,
    )
```

```python
import functools

import jax
import jax.numpy as jnp
import numpy as np
from jax import lax
from jax.experimental import pallas as pl
from jax.experimental.pallas import tpu as pltpu
from jax.sharding import PartitionSpec as P

NPTS = 8
FAR = 4
MESH = pl.DeviceIdType.MESH
F32, BF16, I32 = jnp.float32, jnp.bfloat16, jnp.int32


def legendre_table(points, degree):
    table = [np.ones(points.shape), points.copy()]
    for order in range(2, degree + 1):
        table.append(
            ((2 * order - 1) * points * table[order - 1] - (order - 1) * table[order - 2]) / order
        )
    return table


def lobatto_points(degree):
    points = np.cos(np.pi * np.arange(degree + 1) / degree)
    for sweep in range(100):
        table = legendre_table(points, degree)
        points = points - (points * table[degree] - table[degree - 1]) / (
            (degree + 1) * table[degree]
        )
    points = np.sort(points)
    return (points, legendre_table(points, degree)[degree])


def node_tables(count):
    degree = count - 1
    points, legendre = lobatto_points(degree)
    weights = 2.0 / (degree * (degree + 1) * legendre**2)
    spread = points[:, None] - points[None, :] + np.eye(count)
    derivative = legendre[:, None] / (legendre[None, :] * spread) * (1.0 - np.eye(count))
    derivative[0, 0] = -degree * (degree + 1) / 4.0
    derivative[degree, degree] = degree * (degree + 1) / 4.0
    halves = []
    for side in range(2):
        target = (points + 2.0 * side - 1.0) / 2.0
        matrix = np.ones((count, count))
        for column in range(count):
            for other in range(count):
                if other != column:
                    matrix[:, column] = (
                        matrix[:, column]
                        * (target - points[other])
                        / (points[column] - points[other])
                    )
        halves.append(matrix)
    return (points, weights, derivative, np.stack(halves))


POINTS, WEIGHTS, DERIV, HALVES = node_tables(NPTS)


def up(count, unit=8):
    return -(-count // unit) * unit


def halves_of(values):
    high = values.astype(BF16)
    return high, (values - high.astype(F32)).astype(BF16)


def numpy_halves(matrix):
    matrix = np.asarray(matrix, np.float32)
    high = matrix.astype(jnp.bfloat16)
    low = (matrix - high.astype(np.float32)).astype(jnp.bfloat16)
    return high, low


def dot(a, b, dims=((1,), (0,))):
    return lax.dot_general(a, b, (dims, ((), ())), preferred_element_type=F32)


def select(hot, values):
    high, low = halves_of(values)
    return dot(hot, high) + dot(hot, low)


def take_rows(hot, face):
    high, low = halves_of(face)
    dims = ((1,), (1,))
    return dot(hot, high, dims) + dot(hot, low, dims)


def spread_rows(rows, hot):
    high, low = halves_of(rows.T)
    return dot(high, hot) + dot(low, hot)


def product(a, matrix):
    high, low = halves_of(a)
    mhigh, mlow = halves_of(matrix)
    return dot(high, mhigh) + dot(low, mhigh) + dot(high, mlow)


def column(row, padded):
    count = row.shape[1]
    r = lax.broadcasted_iota(I32, (padded, count), 0)
    c = lax.broadcasted_iota(I32, (padded, count), 1)
    spread = jnp.where(r == c, jnp.broadcast_to(row.astype(F32), (padded, count)), 0.0)
    col = jnp.sum(spread, axis=1, keepdims=True)
    inside = lax.broadcasted_iota(I32, (padded, 1), 0) < count
    return jnp.where(inside, col, -1.0)


def hot_rows(columns, base, elems, kind=BF16):
    col = columns[0] if len(columns) == 1 else jnp.concatenate(columns, axis=0)
    lane = lax.broadcasted_iota(I32, (col.shape[0], elems), 1).astype(F32)
    return jnp.where(lane == col - float(base), 1.0, 0.0).astype(kind)


def line(values, matrix):
    half = NPTS // 2
    even = [values[i] + values[NPTS - 1 - i] for i in range(half)]
    odd = [values[i] - values[NPTS - 1 - i] for i in range(half)]
    out = [None] * NPTS
    for a in range(half):
        p = q = None
        for i in range(half):
            s = float((matrix[a, i] + matrix[a, NPTS - 1 - i]) / 2)
            t = float((matrix[a, i] - matrix[a, NPTS - 1 - i]) / 2)
            p = even[i] * s if p is None else p + even[i] * s
            q = odd[i] * t if q is None else q + odd[i] * t
        out[a] = q + p
        out[NPTS - 1 - a] = q - p
    return out


def stencils():
    forth, back = np.kron(np.eye(16), DERIV), np.kron(np.eye(16), DERIV.T)
    pieces = [piece for table in (forth, back) for piece in numpy_halves(table)]
    return np.concatenate(pieces, axis=0)


def folds():
    eye = np.eye(NPTS)
    heads = [(eye, eye)] * 2
    heads += [(HALVES[m // 2], HALVES[m % 2]) for m in range(4)]
    heads += [(HALVES[m // 2].T, HALVES[m % 2].T) for m in range(4)]
    rows, tiles = [], []
    for turn in (eye, DERIV):
        rows.append([np.repeat(turn @ first, NPTS, axis=1) for first, _ in heads])
        tiles.append([np.tile(turn @ second, (1, NPTS)) for _, second in heads])
    table = [np.concatenate(kind, axis=1) for kind in rows + tiles]
    return np.concatenate(table, axis=0).astype(np.float32)


def steps(
    sizes,
    u_hbm,
    kappa_hbm,
    level_hbm,
    local_hbm,
    sub_hbm,
    near_hbm,
    fold_hbm,
    deriv_hbm,
    mortar_hbm,
    far_hbm,
    child_hbm,
    peer_hbm,
    coarse_hbm,
    out_ref,
    level_ref,
    local_ref,
    sub_ref,
    near_ref,
    fold_ref,
    deriv_ref,
    mortar_ref,
    far_ref,
    child_ref,
    peer_ref,
    coarse_ref,
    w_ref,
    uk_ref,
    g_ref,
    side_out,
    side_in,
    far_out,
    far_in,
    mort_out,
    mort_in,
    side_recv,
    far_recv,
    mort_recv,
    small_sem,
    load_sem,
    side_send,
    far_send,
    mort_send,
):
    n_dom, n_sub = sizes
    u_ref, k_ref = uk_ref.at[0], uk_ref.at[1]
    parts = u_ref.shape[0]
    elems = parts * 128
    square = NPTS * NPTS
    last = NPTS - 1
    me, sub = lax.axis_index("dom"), lax.axis_index("sub")

    urgent = [
        (fold_hbm, fold_ref),
        (far_hbm, far_ref),
        (child_hbm, child_ref),
        (coarse_hbm, coarse_ref),
        (level_hbm, level_ref),
        (peer_hbm, peer_ref),
    ]
    later = [
        (local_hbm, local_ref),
        (sub_hbm, sub_ref),
        (near_hbm, near_ref),
        (deriv_hbm, deriv_ref),
        (mortar_hbm, mortar_ref),
    ]
    small = [
        pltpu.make_async_copy(source, target, small_sem.at[slot])
        for slot, (source, target) in enumerate(urgent + later)
    ]
    block = 128
    blocks = NPTS**3 // block

    def load(n, part, source, target):
        own = pl.ds(part * block, block)
        return pltpu.make_async_copy(
            source.at[own, pl.ds(n * 128, 128)], target.at[n, own], load_sem.at[part]
        )

    def loaded(part):
        whole = uk_ref.at[0, :, pl.ds(0, 2 * block)]
        pltpu.make_async_copy(whole, whole, load_sem.at[part]).wait()

    for copy in small[:6]:
        copy.start()
    for part in range(blocks):
        for n in range(parts):
            load(n, part, u_hbm, u_ref).start()
            load(n, part, kappa_hbm, k_ref).start()
    for copy in small[6:]:
        copy.start()

    far_in[...] = jnp.zeros(far_in.shape, F32)
    mort_in[...] = jnp.zeros(mort_in.shape, F32)

    barrier = pltpu.get_barrier_semaphore()

    def greet(step, carry):
        other = lax.rem(me + step, n_dom)
        pl.semaphore_signal(barrier, inc=1, device_id=(other, sub), device_id_type=MESH)
        return carry

    lax.fori_loop(1, n_dom, greet, 0, unroll=n_dom <= 8)

    @pl.when(sub > 0)
    def _():
        pl.semaphore_signal(barrier, inc=1, device_id=(me, sub - 1), device_id_type=MESH)

    @pl.when(sub < n_sub - 1)
    def _():
        pl.semaphore_signal(barrier, inc=1, device_id=(me, sub + 1), device_id_type=MESH)

    def clear(missing, slot):
        @pl.when(missing)
        def _():
            side_in[slot] = jnp.zeros(side_in.shape[1:], F32)

    clear(sub == 0, 0)
    clear(sub == n_sub - 1, 1)
    clear(me == 0, 2)
    clear(me == n_dom - 1, 3)

    pairs, rim, near = local_ref.shape[1], sub_ref.shape[1], near_ref.shape[1]
    far, groups = far_ref.shape[1], child_ref.shape[1]
    shifts = far // FAR
    farp, groupp, coarsep = up(far), up(groups), up(n_dom)
    coarse_at = 2 * farp
    kids_at = coarse_at + coarsep
    used = kids_at + 4 * groupp
    sources = up(used, 128)
    lane = lax.broadcasted_iota(I32, (8, sources), 1)
    row8 = lax.broadcasted_iota(I32, (8, sources), 0)
    on_low = (lane < farp) | (lane >= kids_at)
    reach = [
        jnp.where(on_low, float(WEIGHTS[c] * DERIV[c, 0]), float(WEIGHTS[c] * DERIV[c, last]))
        for c in range(NPTS)
    ]
    turn8 = []
    for r in range(NPTS):
        table = jnp.zeros((8, sources), F32)
        for b in range(NPTS):
            table = jnp.where(row8 == b, float(DERIV[b, (b + r) % NPTS]), table)
        turn8.append(table)
    quad8 = jnp.zeros((8, sources), F32)
    for k in range(NPTS):
        quad8 = jnp.where(row8 == k, float(WEIGHTS[k]), quad8)

    for copy in small[:6]:
        copy.wait()

    def held(first, ids, base):
        total = jnp.zeros((8, sources), I32)
        for slot, value in enumerate(ids):
            total = jnp.where(lane == first + slot, value + (1 - base * elems), total)
        return total

    ids = held(0, [far_ref[0, c] for c in range(far)], 4)
    ids += held(farp, [far_ref[1, c] for c in range(far)], 5)
    ids += held(coarse_at, [coarse_ref[c] for c in range(n_dom)], 5)
    for m in range(4):
        ids += held(kids_at + m * groupp, [child_ref[m, c] for c in range(groups)], 4)
    fold = []
    for rows_kind, tile_kind in ((0, 0), (1, 0), (0, 1)):
        tile = fold_ref[(2 + tile_kind) * NPTS : (3 + tile_kind) * NPTS, :]
        for i in range(NPTS):
            at = rows_kind * NPTS + i
            fold.append(fold_ref[at : at + 1, :] * tile)
    fold_high, fold_low = halves_of(jnp.concatenate(fold, axis=0))
    element = lax.broadcasted_iota(I32, (elems, sources), 0) + 1
    hot_src = jnp.where(element == ids[0:1], 1.0, 0.0).astype(BF16)
    scale = jnp.exp2(-level_ref[...].astype(F32))
    over = ((1,), (1,))

    def pick(ref, part):
        rows = []
        for k in range(NPTS):
            own = pl.ds(part * block + k, block // NPTS, NPTS)
            rows.append(jnp.concatenate([ref[n, own, :] for n in range(parts)], axis=1))
        high, low = halves_of(jnp.concatenate(rows, axis=0))
        both = dot(jnp.concatenate([high, low], axis=0), hot_src)
        return both[0:block] + both[block:]

    spot = jnp.bitwise_and(ids - 1, 127)
    piece = lax.shift_right_arithmetic(ids - 1, 7)
    lookup = lax.GatherDimensionNumbers(
        offset_dims=(),
        collapsed_slice_dims=(1,),
        start_index_map=(1,),
        operand_batching_dims=(0,),
        start_indices_batching_dims=(0,),
    )

    def fetch(ref, part):
        rows = []
        for k in range(NPTS):
            for at in range(0, block, NPTS * NPTS):
                own = pl.ds(part * block + at + k, NPTS, NPTS)
                tiles = []
                for first in range(0, sources, 128):
                    where = slice(first, first + 128)
                    found = jnp.zeros((8, 128), F32)
                    for n in range(parts):
                        taken = lax.gather(
                            ref[n, own, :],
                            spot[:, where][..., None],
                            lookup,
                            slice_sizes=(1, 1),
                            mode=lax.GatherScatterMode.PROMISE_IN_BOUNDS,
                        )
                        found = jnp.where(piece[:, where] == n, taken, found)
                    tiles.append(found)
                rows.append(tiles[0] if len(tiles) == 1 else jnp.concatenate(tiles, axis=1))
        return jnp.concatenate(rows, axis=0)

    edge = float(WEIGHTS[0])
    chosen = None
    along_k, along_j, plane_u, plane_g = [], [], [], []
    for part in range(blocks):
        loaded(part)
    for part in range(blocks):
        u_part, k_part = fetch(u_ref, part), pick(k_ref, part)
        if chosen is None:
            chosen = dot(jnp.broadcast_to(scale, (16, elems)).astype(BF16), hot_src)[0:8]
            chosen = chosen * quad8
        wide = block // NPTS
        for i in range(part * wide // NPTS, (part + 1) * wide // NPTS):
            at = i * NPTS - part * wide

            def strip(values, k):
                return values[k * wide + at : k * wide + at + NPTS]

            here = chosen * float(WEIGHTS[i])
            flat = jnp.where(on_low, strip(u_part, 0), strip(u_part, last))
            g = jnp.where(on_low, strip(k_part, 0), strip(k_part, last)) * (here * edge)
            plane_u.append(flat)
            plane_g.append(g)
            turned = turn8[0] * flat
            for r in range(1, NPTS):
                turned += turn8[r] * pltpu.roll(flat, NPTS - r, 0)
            along_j.append(turned * g)
            deep = line([strip(u_part, k) for k in range(NPTS)], DERIV)
            total = reach[0] * strip(k_part, 0) * deep[0]
            for c in range(1, NPTS):
                total += reach[c] * strip(k_part, c) * deep[c]
            along_k.append(total * here)
    across_i = line(plane_u, DERIV)
    along_i = [across_i[i] * plane_g[i] for i in range(NPTS)]
    flux = jnp.concatenate(along_k + along_i + along_j, axis=0)

    flux = flux.T

    def folded(rows, first, width):
        high, low = halves_of(rows)
        cols = slice(first, first + width)
        both = dot(jnp.concatenate([high, low], axis=0), fold_high[:, cols])
        return both[0 : rows.shape[0]] + both[rows.shape[0] :] + dot(high, fold_low[:, cols])

    raised = folded(flux[coarse_at : coarse_at + up(coarsep, 16)], 384, 256)
    kids = folded(flux[kids_at:used], 128, 256)
    own = folded(flux[0 : up(used, 16)], 0, 128)

    half = lax.broadcasted_iota(I32, (8, 128), 1) < square
    for side in range(2):
        for first in range(0, farp, 8):
            faces = own[side * farp + first : side * farp + first + 8]
            far_out[side, first : first + 8] = jnp.where(half, faces, pltpu.roll(faces, 6, 0))
    half_g = lax.broadcasted_iota(I32, (groupp, 128), 1) < square
    kid = [kids[m * groupp : (m + 1) * groupp] for m in range(4)]
    projected = jnp.where(half_g, kid[0][:, 0:128], kid[1][:, 0:128]) + jnp.where(
        half_g, kid[2][:, 128:256], kid[3][:, 128:256]
    )
    peer_row = lax.broadcasted_iota(I32, (n_dom, 128), 0)
    routed = jnp.zeros((n_dom, 128), F32)
    for slot in range(groups):
        routed = jnp.where(peer_row == peer_ref[slot], projected[slot : slot + 1], routed)
    mort_out[pl.ds(0, n_dom, 8), :] = routed
    mort_out[pl.ds(1, n_dom, 8), :] = raised[0:n_dom, 0:128]
    mort_out[pl.ds(2, n_dom, 8), :] = raised[0:n_dom, 128:256]

    greeted = n_dom - 1 + (sub > 0).astype(I32) + (sub < n_sub - 1).astype(I32)

    def mail(step, landing):
        other = lax.rem(me + step, n_dom)
        return pltpu.make_async_remote_copy(
            src_ref=mort_out.at[pl.ds(pl.multiple_of(other * 8, 8), 3)],
            dst_ref=mort_in.at[
                pl.ds(pl.multiple_of((other if landing else me) * 8, 8), 3)
            ],
            send_sem=mort_send.at[other],
            recv_sem=mort_recv.at[other if landing else me],
            device_id=(other, sub),
            device_id_type=MESH,
        )

    def far_copy(side, s, landing):
        other = me - s - 2 if side == 0 else me + s + 2
        rows = pl.ds(s * FAR, FAR // 2)
        there = side if landing else 1 - side
        return pltpu.make_async_remote_copy(
            src_ref=far_out.at[side, rows],
            dst_ref=far_in.at[there, rows],
            send_sem=far_send.at[side, s],
            recv_sem=far_recv.at[there, s],
            device_id=(other, sub),
            device_id_type=MESH,
        )

    def far_there(side, s):
        return me >= s + 2 if side == 0 else me + s + 2 < n_dom

    def send_messages():
        pl.semaphore_wait(barrier, greeted)

        def start_all(step, carry):
            mail(step, False).start()
            return carry

        lax.fori_loop(1, n_dom, start_all, 0, unroll=n_dom <= 8)
        for side in range(2):
            for s in range(shifts):
                @pl.when(far_there(side, s))
                def _():
                    far_copy(side, s, False).start()

    early = me < 3

    @pl.when(jnp.logical_not(early))
    def _():
        send_messages()

    for copy in small[6:]:
        copy.wait()

    hot0l = hot_rows([column(local_ref[1:2], up(pairs))], 0, elems)
    hot1l = hot_rows([column(local_ref[0:1], up(pairs))], elems, elems)
    hot0s = hot_rows([column(sub_ref[0:1], up(rim))], 0, elems)
    hot1s = hot_rows([column(sub_ref[1:2], up(rim))], elems, elems)
    hot2 = hot_rows([column(near_ref[0:1], up(near))], 2 * elems, elems)
    hot3 = hot_rows([column(near_ref[1:2], up(near))], 3 * elems, elems)

    sub8 = lax.broadcasted_iota(I32, (8, elems), 0)
    weight = jnp.zeros((8, elems), F32)
    for k in range(NPTS):
        weight = jnp.where(sub8 == k, float(WEIGHTS[k]), weight)
    weight = weight * scale

    def slab(i, j):
        return pl.ds((i * NPTS + j) * NPTS, NPTS)

    def across(ref, own):
        return jnp.concatenate([ref[n, own, :] for n in range(parts)], axis=1)

    def add_across(own, values):
        for n in range(parts):
            w_ref[n, own, :] += values[:, n * 128 : (n + 1) * 128]

    turns = [deriv_ref[128 * n : 128 * n + 128, :] for n in range(4)]

    def along(pair, values):
        high, low = halves_of(values)
        both = jnp.concatenate([high, low], axis=0)
        return dot(jnp.concatenate([pair[0], pair[0]], axis=1), both) + dot(pair[1], high)

    for n in range(parts):
        here = weight[:, n * 128 : (n + 1) * 128]
        for i in range(NPTS):
            for j in range(NPTS):
                g_ref[n, slab(i, j), :] = k_ref[n, slab(i, j), :] * (
                    here * float(WEIGHTS[i] * WEIGHTS[j])
                )
    for part in range(blocks):
        own_rows = pl.ds(part * block, block)
        turn = along(turns[0:2], across(u_ref, own_rows)) * across(g_ref, own_rows)
        turn = along(turns[2:4], turn)
        for n in range(parts):
            w_ref[n, own_rows, :] = turn[:, n * 128 : (n + 1) * 128]
    for n in range(parts):
        for j in range(NPTS):
            turn = line([u_ref[n, slab(i, j), :] for i in range(NPTS)], DERIV)
            turn = [turn[i] * g_ref[n, slab(i, j), :] for i in range(NPTS)]
            turn = line(turn, DERIV.T)
            for i in range(NPTS):
                w_ref[n, slab(i, j), :] += turn[i]
        for i in range(NPTS):
            turn = line([u_ref[n, slab(i, j), :] for j in range(NPTS)], DERIV)
            turn = [turn[j] * g_ref[n, slab(i, j), :] for j in range(NPTS)]
            turn = line(turn, DERIV.T)
            for j in range(NPTS):
                w_ref[n, slab(i, j), :] += turn[j]

    low_i, high_i = pl.ds(0, square), pl.ds(last * square, square)
    low_k, high_k = pl.ds(0, square, NPTS), pl.ds(last, square, NPTS)
    face0 = across(w_ref, low_i)
    face1 = across(w_ref, high_i)
    face2 = jnp.concatenate([across(w_ref, slab(i, 0)) for i in range(NPTS)], axis=0)
    face3 = jnp.concatenate([across(w_ref, slab(i, last)) for i in range(NPTS)], axis=0)
    side_out[0, 0:rim, 0:square] = take_rows(hot0s, face0)[0:rim]
    side_out[1, 0:rim, 0:square] = take_rows(hot1s, face1)[0:rim]
    side_out[2, 0:near, 0:square] = take_rows(hot2, face2)[0:near]
    side_out[3, 0:near, 0:square] = take_rows(hot3, face3)[0:near]

    @pl.when(early)
    def _():
        send_messages()

    sides = [
        (sub > 0, 0, 1, (me, sub - 1)),
        (sub < n_sub - 1, 1, 0, (me, sub + 1)),
        (me > 0, 2, 3, (me - 1, sub)),
        (me < n_dom - 1, 3, 2, (me + 1, sub)),
    ]

    def side_copy(mine, theirs, device):
        return pltpu.make_async_remote_copy(
            src_ref=side_out.at[mine],
            dst_ref=side_in.at[theirs],
            send_sem=side_send.at[mine],
            recv_sem=side_recv.at[theirs],
            device_id=device,
            device_id_type=MESH,
        )

    for there, mine, theirs, device in sides:
        @pl.when(there)
        def _():
            side_copy(mine, theirs, device).start()

    keyed = up(2 * farp + 8 * n_dom, 128)

    def landing_rows(keys):
        at = lax.broadcasted_iota(I32, (2 * keyed, sources), 0)
        hit = at == keys[0]
        for key in keys[1:]:
            hit = hit | (at == key)
        return dot(jnp.where(hit, 1.0, 0.0).astype(BF16), hot_src, over).astype(BF16)

    src = lax.broadcasted_iota(I32, (1, sources), 1)

    def far_key(first):
        f = src - first
        s, j = lax.shift_right_logical(f, 2), lax.bitwise_and(f, FAR - 1)
        key = lax.shift_right_logical(j, 1) * keyed + first + 4 * s + lax.bitwise_and(j, 1)
        return jnp.where((f >= 0) & (f < far), key, -1)

    key4 = far_key(0)
    for m in range(4):
        for slot in range(groups):
            key = (m & 1) * keyed + 2 * farp + peer_ref[slot] * 8 + 1 + (m >> 1)
            key4 = jnp.where(src == kids_at + m * groupp + slot, key, key4)
    key5 = far_key(farp)
    p = src - coarse_at
    holds = (p >= 0) & (p < n_dom)
    key5 = jnp.where(holds, 2 * farp + 8 * p, key5)
    land4 = landing_rows([key4])
    land5 = landing_rows([key5, jnp.where(holds, keyed + 2 * farp + 8 * p, -1)])

    joined = projected[:, 0:square] + projected[:, square:]
    lift = [mortar_ref[m * square : (m + 1) * square, :] for m in range(4)]
    share = []
    for m in range(4):
        first = kids_at + m * groupp
        share.append(product(joined, lift[m]) - own[first : first + groupp, 0:square])
    share = [jnp.zeros((kids_at, square), F32)] + share
    if sources > used:
        share.append(jnp.zeros((sources - used, square), F32))
    high, low = halves_of(jnp.concatenate(share, axis=0).T)
    add_across(low_k, dot(high, hot_src, over) + dot(low, hot_src, over))
    add_across(low_i, spread_rows(take_rows(hot1l, face1), hot0l))
    add_across(high_i, spread_rows(take_rows(hot0l, face0), hot1l))

    for there, mine, theirs, device in sides:
        @pl.when(there)
        def _():
            side_copy(mine, mine, device).wait()

    add_across(low_i, spread_rows(side_in[0, 0:rim, 0:square], hot0s))
    add_across(high_i, spread_rows(side_in[1, 0:rim, 0:square], hot1s))
    add2 = spread_rows(side_in[2, 0:near, 0:square], hot2)
    add3 = spread_rows(side_in[3, 0:near, 0:square], hot3)
    for i in range(NPTS):
        add_across(slab(i, 0), add2[i * NPTS : (i + 1) * NPTS])
        add_across(slab(i, last), add3[i * NPTS : (i + 1) * NPTS])

    def sent_all(step, carry):
        mail(step, True).wait_send()
        return carry

    lax.fori_loop(1, n_dom, sent_all, 0, unroll=n_dom <= 8)
    for side in range(2):
        for s in range(shifts):
            @pl.when(far_there(side, s))
            def _():
                far_copy(side, s, True).wait()

    def wait_all(step, carry):
        mail(step, True).wait_recv()
        return carry

    lax.fori_loop(1, n_dom, wait_all, 0, unroll=n_dom <= 8)

    received = [far_in[0], far_in[1], mort_in[...]]
    spare = keyed - 2 * farp - 8 * n_dom
    if spare:
        received.append(jnp.zeros((spare, 128), F32))
    received = jnp.concatenate(received, axis=0).T
    received = jnp.concatenate([received[0:square], received[square:]], axis=1)
    high, low = halves_of(received)
    add_across(low_k, dot(high, land4) + dot(low, land4))
    add_across(high_k, dot(high, land5) + dot(low, land5))
    for n in range(parts):
        out_ref[:, n * 128 : (n + 1) * 128] = w_ref[n]


def kernel(sizes, copies, *refs):
    n_dom, _ = sizes
    far_recv = refs[-2]
    pl.run_scoped(
        functools.partial(steps, sizes, *refs),
        pltpu.SemaphoreType.DMA((copies,)),
        pltpu.SemaphoreType.DMA((NPTS**3 // 128,)),
        pltpu.SemaphoreType.DMA((4,)),
        pltpu.SemaphoreType.DMA(far_recv.shape),
        pltpu.SemaphoreType.DMA((n_dom,)),
    )


def body(
    sizes,
    nodal_values,
    kappa,
    levels,
    local_faces,
    sub_faces,
    near_faces,
    far_faces,
    child_faces,
    child_peer,
    coarse_faces,
):
    n_dom, n_sub = sizes
    elems = nodal_values.shape[1]
    krons = [np.kron(HALVES[m // 2], HALVES[m % 2]) for m in range(4)]
    mortar = np.concatenate([m.T for m in krons], axis=0)
    far_rows = up(far_faces.shape[1])
    held = (elems // 128, NPTS**3, 128)
    side_rows = up(max(sub_faces.shape[1], near_faces.shape[1]))
    small = [
        levels.reshape(1, elems),
        local_faces,
        sub_faces,
        near_faces,
        jnp.asarray(folds(), F32),
        jnp.asarray(stencils(), BF16),
        jnp.asarray(mortar, F32),
    ]
    tables = [far_faces, child_faces, child_peer, coarse_faces]
    hbm = pl.BlockSpec(memory_space=pltpu.HBM)
    vmem = pl.BlockSpec(memory_space=pltpu.VMEM)
    return pl.pallas_call(
        functools.partial(kernel, sizes, len(small) + len(tables)),
        out_shape=pltpu.VMEM(nodal_values.shape, F32),
        in_specs=[hbm] * 13,
        out_specs=vmem,
        scratch_shapes=[pltpu.VMEM(item.shape, item.dtype) for item in small]
        + [pltpu.SMEM(item.shape, I32) for item in tables]
        + [
            pltpu.VMEM(held, F32),
            pltpu.VMEM((2, *held), F32),
            pltpu.VMEM(held, F32),
            pltpu.VMEM((4, side_rows, 128), F32),
            pltpu.VMEM((4, side_rows, 128), F32),
            pltpu.VMEM((2, far_rows, 128), F32),
            pltpu.VMEM((2, far_rows, 128), F32),
            pltpu.VMEM((n_dom * 8, 128), F32),
            pltpu.VMEM((n_dom * 8, 128), F32),
            pltpu.SemaphoreType.DMA((4,)),
            pltpu.SemaphoreType.DMA((2, far_faces.shape[1] // FAR)),
            pltpu.SemaphoreType.DMA((n_dom,)),
        ],
        compiler_params=pltpu.CompilerParams(
            collective_id=0, has_side_effects=True, vmem_limit_bytes=60 * 1024 * 1024
        ),
    )(
        nodal_values,
        kappa,
        *small,
        *tables,
    )


def solution(mesh):
    sizes = (mesh.shape["dom"], mesh.shape["sub"])
    wide = P(None, ("dom", "sub"))
    flat = P(("dom", "sub"))
    in_specs = (wide, wide, flat, wide, wide, wide, wide, wide, flat, flat)
    return jax.shard_map(
        functools.partial(body, sizes),
        mesh=mesh,
        in_specs=in_specs,
        out_specs=wide,
        check_vma=False,
    )
```

```python
import functools

import jax
import jax.numpy as jnp
import numpy as np
from jax import lax
from jax.experimental import pallas as pl
from jax.experimental.pallas import tpu as pltpu
from jax.sharding import PartitionSpec as P

NPTS = 8
FAR = 4
MESH = pl.DeviceIdType.MESH
F32, BF16, I32 = jnp.float32, jnp.bfloat16, jnp.int32


def legendre_table(points, degree):
    table = [np.ones(points.shape), points.copy()]
    for order in range(2, degree + 1):
        table.append(
            ((2 * order - 1) * points * table[order - 1] - (order - 1) * table[order - 2]) / order
        )
    return table


def lobatto_points(degree):
    points = np.cos(np.pi * np.arange(degree + 1) / degree)
    for sweep in range(100):
        table = legendre_table(points, degree)
        points = points - (points * table[degree] - table[degree - 1]) / (
            (degree + 1) * table[degree]
        )
    points = np.sort(points)
    return (points, legendre_table(points, degree)[degree])


def node_tables(count):
    degree = count - 1
    points, legendre = lobatto_points(degree)
    weights = 2.0 / (degree * (degree + 1) * legendre**2)
    spread = points[:, None] - points[None, :] + np.eye(count)
    derivative = legendre[:, None] / (legendre[None, :] * spread) * (1.0 - np.eye(count))
    derivative[0, 0] = -degree * (degree + 1) / 4.0
    derivative[degree, degree] = degree * (degree + 1) / 4.0
    halves = []
    for side in range(2):
        target = (points + 2.0 * side - 1.0) / 2.0
        matrix = np.ones((count, count))
        for column in range(count):
            for other in range(count):
                if other != column:
                    matrix[:, column] = (
                        matrix[:, column]
                        * (target - points[other])
                        / (points[column] - points[other])
                    )
        halves.append(matrix)
    return (points, weights, derivative, np.stack(halves))


POINTS, WEIGHTS, DERIV, HALVES = node_tables(NPTS)


def up(count, unit=8):
    return -(-count // unit) * unit


def halves_of(values):
    high = values.astype(BF16)
    return high, (values - high.astype(F32)).astype(BF16)


def numpy_halves(matrix):
    matrix = np.asarray(matrix, np.float32)
    high = matrix.astype(jnp.bfloat16)
    low = (matrix - high.astype(np.float32)).astype(jnp.bfloat16)
    return high, low


def dot(a, b, dims=((1,), (0,))):
    return lax.dot_general(a, b, (dims, ((), ())), preferred_element_type=F32)


def select(hot, values):
    high, low = halves_of(values)
    return dot(hot, high) + dot(hot, low)


def take_rows(hot, face):
    high, low = halves_of(face)
    dims = ((1,), (1,))
    return dot(hot, high, dims) + dot(hot, low, dims)


def spread_rows(rows, hot):
    high, low = halves_of(rows.T)
    return dot(high, hot) + dot(low, hot)


def product(a, matrix):
    high, low = halves_of(a)
    mhigh, mlow = halves_of(matrix)
    return dot(high, mhigh) + dot(low, mhigh) + dot(high, mlow)


def column(row, padded):
    count = row.shape[1]
    r = lax.broadcasted_iota(I32, (padded, count), 0)
    c = lax.broadcasted_iota(I32, (padded, count), 1)
    spread = jnp.where(r == c, jnp.broadcast_to(row.astype(F32), (padded, count)), 0.0)
    col = jnp.sum(spread, axis=1, keepdims=True)
    inside = lax.broadcasted_iota(I32, (padded, 1), 0) < count
    return jnp.where(inside, col, -1.0)


def hot_rows(columns, base, elems, kind=BF16):
    col = columns[0] if len(columns) == 1 else jnp.concatenate(columns, axis=0)
    lane = lax.broadcasted_iota(I32, (col.shape[0], elems), 1).astype(F32)
    return jnp.where(lane == col - float(base), 1.0, 0.0).astype(kind)


def line(values, matrix):
    half = NPTS // 2
    even = [values[i] + values[NPTS - 1 - i] for i in range(half)]
    odd = [values[i] - values[NPTS - 1 - i] for i in range(half)]
    out = [None] * NPTS
    for a in range(half):
        p = q = None
        for i in range(half):
            s = float((matrix[a, i] + matrix[a, NPTS - 1 - i]) / 2)
            t = float((matrix[a, i] - matrix[a, NPTS - 1 - i]) / 2)
            p = even[i] * s if p is None else p + even[i] * s
            q = odd[i] * t if q is None else q + odd[i] * t
        out[a] = q + p
        out[NPTS - 1 - a] = q - p
    return out


def stencils():
    forth, back = np.kron(np.eye(16), DERIV), np.kron(np.eye(16), DERIV.T)
    pieces = [piece for table in (forth, back) for piece in numpy_halves(table)]
    return np.concatenate(pieces, axis=0)


def folds():
    eye = np.eye(NPTS)
    heads = [(eye, eye)] * 2
    heads += [(HALVES[m // 2], HALVES[m % 2]) for m in range(4)]
    heads += [(HALVES[m // 2].T, HALVES[m % 2].T) for m in range(4)]
    rows, tiles = [], []
    for turn in (eye, DERIV):
        rows.append([np.repeat(turn @ first, NPTS, axis=1) for first, _ in heads])
        tiles.append([np.tile(turn @ second, (1, NPTS)) for _, second in heads])
    table = [np.concatenate(kind, axis=1) for kind in rows + tiles]
    return np.concatenate(table, axis=0).astype(np.float32)


def steps(
    sizes,
    u_hbm,
    kappa_hbm,
    level_hbm,
    local_hbm,
    sub_hbm,
    near_hbm,
    fold_hbm,
    deriv_hbm,
    mortar_hbm,
    far_hbm,
    child_hbm,
    peer_hbm,
    coarse_hbm,
    w_ref,
    level_ref,
    local_ref,
    sub_ref,
    near_ref,
    fold_ref,
    deriv_ref,
    mortar_ref,
    far_ref,
    child_ref,
    peer_ref,
    coarse_ref,
    uk_ref,
    g_ref,
    side_out,
    side_in,
    far_out,
    far_in,
    mort_out,
    mort_in,
    small_sem,
    load_sem,
    side_send,
    side_recv,
    far_send,
    far_recv,
    mort_send,
    mort_recv,
):
    n_dom, n_sub = sizes
    u_ref, k_ref = uk_ref.at[0], uk_ref.at[1]
    parts = u_ref.shape[0]
    elems = parts * 128
    square = NPTS * NPTS
    last = NPTS - 1
    me, sub = lax.axis_index("dom"), lax.axis_index("sub")

    urgent = [
        (fold_hbm, fold_ref),
        (far_hbm, far_ref),
        (child_hbm, child_ref),
        (coarse_hbm, coarse_ref),
        (level_hbm, level_ref),
        (peer_hbm, peer_ref),
    ]
    later = [
        (local_hbm, local_ref),
        (sub_hbm, sub_ref),
        (near_hbm, near_ref),
        (deriv_hbm, deriv_ref),
        (mortar_hbm, mortar_ref),
    ]
    small = [
        pltpu.make_async_copy(source, target, small_sem.at[slot])
        for slot, (source, target) in enumerate(urgent + later)
    ]
    block = 128
    blocks = NPTS**3 // block

    def load(n, part, source, target):
        own = pl.ds(part * block, block)
        return pltpu.make_async_copy(
            source.at[own, pl.ds(n * 128, 128)], target.at[n, own], load_sem.at[part]
        )

    def loaded(part):
        whole = uk_ref.at[0, :, pl.ds(0, 2 * block)]
        pltpu.make_async_copy(whole, whole, load_sem.at[part]).wait()

    for copy in small[:6]:
        copy.start()
    for part in range(blocks):
        for n in range(parts):
            load(n, part, u_hbm, u_ref).start()
            load(n, part, kappa_hbm, k_ref).start()
    for copy in small[6:]:
        copy.start()

    far_in[...] = jnp.zeros(far_in.shape, F32)
    mort_in[...] = jnp.zeros(mort_in.shape, F32)

    barrier = pltpu.get_barrier_semaphore()

    def greet(step, carry):
        other = lax.rem(me + step, n_dom)
        pl.semaphore_signal(barrier, inc=1, device_id=(other, sub), device_id_type=MESH)
        return carry

    lax.fori_loop(1, n_dom, greet, 0, unroll=n_dom <= 8)

    @pl.when(sub > 0)
    def _():
        pl.semaphore_signal(barrier, inc=1, device_id=(me, sub - 1), device_id_type=MESH)

    @pl.when(sub < n_sub - 1)
    def _():
        pl.semaphore_signal(barrier, inc=1, device_id=(me, sub + 1), device_id_type=MESH)

    def clear(missing, slot):
        @pl.when(missing)
        def _():
            side_in[slot] = jnp.zeros(side_in.shape[1:], F32)

    clear(sub == 0, 0)
    clear(sub == n_sub - 1, 1)
    clear(me == 0, 2)
    clear(me == n_dom - 1, 3)

    pairs, rim, near = local_ref.shape[1], sub_ref.shape[1], near_ref.shape[1]
    far, groups = far_ref.shape[1], child_ref.shape[1]
    shifts = far // FAR
    farp, groupp, coarsep = up(far), up(groups), up(n_dom)
    coarse_at = 2 * farp
    kids_at = coarse_at + coarsep
    used = kids_at + 4 * groupp
    sources = up(used, 128)
    lane = lax.broadcasted_iota(I32, (8, sources), 1)
    row8 = lax.broadcasted_iota(I32, (8, sources), 0)
    on_low = (lane < farp) | (lane >= kids_at)
    reach = [
        jnp.where(on_low, float(WEIGHTS[c] * DERIV[c, 0]), float(WEIGHTS[c] * DERIV[c, last]))
        for c in range(NPTS)
    ]
    turn8 = []
    for r in range(NPTS):
        table = jnp.zeros((8, sources), F32)
        for b in range(NPTS):
            table = jnp.where(row8 == b, float(DERIV[b, (b + r) % NPTS]), table)
        turn8.append(table)
    quad8 = jnp.zeros((8, sources), F32)
    for k in range(NPTS):
        quad8 = jnp.where(row8 == k, float(WEIGHTS[k]), quad8)

    for copy in small[:6]:
        copy.wait()

    def held(first, ids, base):
        total = jnp.zeros((8, sources), I32)
        for slot, value in enumerate(ids):
            total = jnp.where(lane == first + slot, value + (1 - base * elems), total)
        return total

    ids = held(0, [far_ref[0, c] for c in range(far)], 4)
    ids += held(farp, [far_ref[1, c] for c in range(far)], 5)
    ids += held(coarse_at, [coarse_ref[c] for c in range(n_dom)], 5)
    for m in range(4):
        ids += held(kids_at + m * groupp, [child_ref[m, c] for c in range(groups)], 4)
    fold = []
    for rows_kind, tile_kind in ((0, 0), (1, 0), (0, 1)):
        tile = fold_ref[(2 + tile_kind) * NPTS : (3 + tile_kind) * NPTS, :]
        for i in range(NPTS):
            at = rows_kind * NPTS + i
            fold.append(fold_ref[at : at + 1, :] * tile)
    fold_high, fold_low = halves_of(jnp.concatenate(fold, axis=0))
    element = lax.broadcasted_iota(I32, (elems, sources), 0) + 1
    hot_src = jnp.where(element == ids[0:1], 1.0, 0.0).astype(BF16)
    scale = jnp.exp2(-level_ref[...].astype(F32))
    over = ((1,), (1,))

    def pick(ref, part):
        rows = []
        for k in range(NPTS):
            own = pl.ds(part * block + k, block // NPTS, NPTS)
            rows.append(jnp.concatenate([ref[n, own, :] for n in range(parts)], axis=1))
        high, low = halves_of(jnp.concatenate(rows, axis=0))
        both = dot(jnp.concatenate([high, low], axis=0), hot_src)
        return both[0:block] + both[block:]

    spot = jnp.bitwise_and(ids - 1, 127)
    piece = lax.shift_right_arithmetic(ids - 1, 7)
    lookup = lax.GatherDimensionNumbers(
        offset_dims=(),
        collapsed_slice_dims=(1,),
        start_index_map=(1,),
        operand_batching_dims=(0,),
        start_indices_batching_dims=(0,),
    )

    def fetch(ref, part):
        rows = []
        for k in range(NPTS):
            for at in range(0, block, NPTS * NPTS):
                own = pl.ds(part * block + at + k, NPTS, NPTS)
                tiles = []
                for first in range(0, sources, 128):
                    where = slice(first, first + 128)
                    found = jnp.zeros((8, 128), F32)
                    for n in range(parts):
                        taken = lax.gather(
                            ref[n, own, :],
                            spot[:, where][..., None],
                            lookup,
                            slice_sizes=(1, 1),
                            mode=lax.GatherScatterMode.PROMISE_IN_BOUNDS,
                        )
                        found = jnp.where(piece[:, where] == n, taken, found)
                    tiles.append(found)
                rows.append(tiles[0] if len(tiles) == 1 else jnp.concatenate(tiles, axis=1))
        return jnp.concatenate(rows, axis=0)

    edge = float(WEIGHTS[0])
    chosen = None
    along_k, along_j, plane_u, plane_g = [], [], [], []
    for part in range(blocks):
        loaded(part)
    for part in range(blocks):
        u_part, k_part = fetch(u_ref, part), pick(k_ref, part)
        if chosen is None:
            chosen = dot(jnp.broadcast_to(scale, (16, elems)).astype(BF16), hot_src)[0:8]
            chosen = chosen * quad8
        wide = block // NPTS
        for i in range(part * wide // NPTS, (part + 1) * wide // NPTS):
            at = i * NPTS - part * wide

            def strip(values, k):
                return values[k * wide + at : k * wide + at + NPTS]

            here = chosen * float(WEIGHTS[i])
            flat = jnp.where(on_low, strip(u_part, 0), strip(u_part, last))
            g = jnp.where(on_low, strip(k_part, 0), strip(k_part, last)) * (here * edge)
            plane_u.append(flat)
            plane_g.append(g)
            turned = turn8[0] * flat
            for r in range(1, NPTS):
                turned += turn8[r] * pltpu.roll(flat, NPTS - r, 0)
            along_j.append(turned * g)
            deep = line([strip(u_part, k) for k in range(NPTS)], DERIV)
            total = reach[0] * strip(k_part, 0) * deep[0]
            for c in range(1, NPTS):
                total += reach[c] * strip(k_part, c) * deep[c]
            along_k.append(total * here)
    across_i = line(plane_u, DERIV)
    along_i = [across_i[i] * plane_g[i] for i in range(NPTS)]
    flux = jnp.concatenate(along_k + along_i + along_j, axis=0)

    flux = flux.T

    def folded(rows, first, width):
        high, low = halves_of(rows)
        cols = slice(first, first + width)
        both = dot(jnp.concatenate([high, low], axis=0), fold_high[:, cols])
        return both[0 : rows.shape[0]] + both[rows.shape[0] :] + dot(high, fold_low[:, cols])

    raised = folded(flux[coarse_at : coarse_at + up(coarsep, 16)], 384, 256)
    kids = folded(flux[kids_at:used], 128, 256)
    own = folded(flux[0 : up(used, 16)], 0, 128)

    half = lax.broadcasted_iota(I32, (8, 128), 1) < square
    for side in range(2):
        for first in range(0, farp, 8):
            faces = own[side * farp + first : side * farp + first + 8]
            far_out[side, first : first + 8] = jnp.where(half, faces, pltpu.roll(faces, 6, 0))
    half_g = lax.broadcasted_iota(I32, (groupp, 128), 1) < square
    kid = [kids[m * groupp : (m + 1) * groupp] for m in range(4)]
    projected = jnp.where(half_g, kid[0][:, 0:128], kid[1][:, 0:128]) + jnp.where(
        half_g, kid[2][:, 128:256], kid[3][:, 128:256]
    )
    peer_row = lax.broadcasted_iota(I32, (n_dom, 128), 0)
    routed = jnp.zeros((n_dom, 128), F32)
    for slot in range(groups):
        routed = jnp.where(peer_row == peer_ref[slot], projected[slot : slot + 1], routed)
    mort_out[pl.ds(0, n_dom, 8), :] = routed
    mort_out[pl.ds(1, n_dom, 8), :] = raised[0:n_dom, 0:128]
    mort_out[pl.ds(2, n_dom, 8), :] = raised[0:n_dom, 128:256]

    greeted = n_dom - 1 + (sub > 0).astype(I32) + (sub < n_sub - 1).astype(I32)

    def mail(step, landing):
        other = lax.rem(me + step, n_dom)
        return pltpu.make_async_remote_copy(
            src_ref=mort_out.at[pl.ds(pl.multiple_of(other * 8, 8), 3)],
            dst_ref=mort_in.at[
                pl.ds(pl.multiple_of((other if landing else me) * 8, 8), 3)
            ],
            send_sem=mort_send.at[other],
            recv_sem=mort_recv.at[other if landing else me],
            device_id=(other, sub),
            device_id_type=MESH,
        )

    def far_copy(side, s, landing):
        other = me - s - 2 if side == 0 else me + s + 2
        rows = pl.ds(s * FAR, FAR // 2)
        there = side if landing else 1 - side
        return pltpu.make_async_remote_copy(
            src_ref=far_out.at[side, rows],
            dst_ref=far_in.at[there, rows],
            send_sem=far_send.at[side, s],
            recv_sem=far_recv.at[there, s],
            device_id=(other, sub),
            device_id_type=MESH,
        )

    def far_there(side, s):
        return me >= s + 2 if side == 0 else me + s + 2 < n_dom

    def send_messages():
        pl.semaphore_wait(barrier, greeted)

        def start_all(step, carry):
            mail(step, False).start()
            return carry

        lax.fori_loop(1, n_dom, start_all, 0, unroll=n_dom <= 8)
        for side in range(2):
            for s in range(shifts):
                @pl.when(far_there(side, s))
                def _():
                    far_copy(side, s, False).start()

    early = me < 3

    @pl.when(jnp.logical_not(early))
    def _():
        send_messages()

    for copy in small[6:]:
        copy.wait()

    hot0l = hot_rows([column(local_ref[1:2], up(pairs))], 0, elems)
    hot1l = hot_rows([column(local_ref[0:1], up(pairs))], elems, elems)
    hot0s = hot_rows([column(sub_ref[0:1], up(rim))], 0, elems)
    hot1s = hot_rows([column(sub_ref[1:2], up(rim))], elems, elems)
    hot2 = hot_rows([column(near_ref[0:1], up(near))], 2 * elems, elems)
    hot3 = hot_rows([column(near_ref[1:2], up(near))], 3 * elems, elems)

    sub8 = lax.broadcasted_iota(I32, (8, elems), 0)
    weight = jnp.zeros((8, elems), F32)
    for k in range(NPTS):
        weight = jnp.where(sub8 == k, float(WEIGHTS[k]), weight)
    weight = weight * scale

    def slab(i, j):
        return pl.ds((i * NPTS + j) * NPTS, NPTS)

    def across(ref, own):
        return jnp.concatenate([ref[n, own, :] for n in range(parts)], axis=1)

    def spot_of(n, i, j):
        return pl.ds(((i * NPTS + j) * parts + n) * NPTS, NPTS)

    def face_of(tiles):
        return jnp.concatenate(
            [
                jnp.concatenate([w_ref[spot_of(n, i, j), :] for i, j in tiles], axis=0)
                for n in range(parts)
            ],
            axis=1,
        )

    def add_tiles(tiles, values):
        for t, (i, j) in enumerate(tiles):
            for n in range(parts):
                w_ref[spot_of(n, i, j), :] += values[
                    t * NPTS : (t + 1) * NPTS, n * 128 : (n + 1) * 128
                ]

    def add_level(k, values):
        for n in range(parts):
            own_rows = pl.ds(n * NPTS + k, square, parts * NPTS)
            w_ref[own_rows, :] += values[:, n * 128 : (n + 1) * 128]

    turns = [deriv_ref[128 * n : 128 * n + 128, :] for n in range(4)]

    def along(pair, values):
        high, low = halves_of(values)
        both = jnp.concatenate([high, low], axis=0)
        return dot(jnp.concatenate([pair[0], pair[0]], axis=1), both) + dot(pair[1], high)

    for n in range(parts):
        here = weight[:, n * 128 : (n + 1) * 128]
        for i in range(NPTS):
            for j in range(NPTS):
                g_ref[n, slab(i, j), :] = k_ref[n, slab(i, j), :] * (
                    here * float(WEIGHTS[i] * WEIGHTS[j])
                )
    for part in range(blocks):
        own_rows = pl.ds(part * block, block)
        turn = along(turns[0:2], across(u_ref, own_rows)) * across(g_ref, own_rows)
        turn = along(turns[2:4], turn)
        for t in range(block // NPTS):
            i, j = divmod(part * block // NPTS + t, NPTS)
            for n in range(parts):
                w_ref[spot_of(n, i, j), :] = turn[
                    t * NPTS : (t + 1) * NPTS, n * 128 : (n + 1) * 128
                ]
    for n in range(parts):
        for j in range(NPTS):
            turn = line([u_ref[n, slab(i, j), :] for i in range(NPTS)], DERIV)
            turn = [turn[i] * g_ref[n, slab(i, j), :] for i in range(NPTS)]
            turn = line(turn, DERIV.T)
            for i in range(NPTS):
                w_ref[spot_of(n, i, j), :] += turn[i]
        for i in range(NPTS):
            turn = line([u_ref[n, slab(i, j), :] for j in range(NPTS)], DERIV)
            turn = [turn[j] * g_ref[n, slab(i, j), :] for j in range(NPTS)]
            turn = line(turn, DERIV.T)
            for j in range(NPTS):
                w_ref[spot_of(n, i, j), :] += turn[j]

    low_i, high_i = ([(i, j) for j in range(NPTS)] for i in (0, last))
    low_j, high_j = ([(i, j) for i in range(NPTS)] for j in (0, last))
    face0, face1, face2, face3 = (face_of(tiles) for tiles in (low_i, high_i, low_j, high_j))
    side_out[0, 0:rim, 0:square] = take_rows(hot0s, face0)[0:rim]
    side_out[1, 0:rim, 0:square] = take_rows(hot1s, face1)[0:rim]
    side_out[2, 0:near, 0:square] = take_rows(hot2, face2)[0:near]
    side_out[3, 0:near, 0:square] = take_rows(hot3, face3)[0:near]

    @pl.when(early)
    def _():
        send_messages()

    sides = [
        (sub > 0, 0, 1, (me, sub - 1)),
        (sub < n_sub - 1, 1, 0, (me, sub + 1)),
        (me > 0, 2, 3, (me - 1, sub)),
        (me < n_dom - 1, 3, 2, (me + 1, sub)),
    ]

    def side_copy(mine, theirs, device):
        return pltpu.make_async_remote_copy(
            src_ref=side_out.at[mine],
            dst_ref=side_in.at[theirs],
            send_sem=side_send.at[mine],
            recv_sem=side_recv.at[theirs],
            device_id=device,
            device_id_type=MESH,
        )

    for there, mine, theirs, device in sides:
        @pl.when(there)
        def _():
            side_copy(mine, theirs, device).start()

    keyed = up(2 * farp + 8 * n_dom, 128)

    def landing_rows(keys):
        at = lax.broadcasted_iota(I32, (2 * keyed, sources), 0)
        hit = at == keys[0]
        for key in keys[1:]:
            hit = hit | (at == key)
        return dot(jnp.where(hit, 1.0, 0.0).astype(BF16), hot_src, over).astype(BF16)

    src = lax.broadcasted_iota(I32, (1, sources), 1)

    def far_key(first):
        f = src - first
        s, j = lax.shift_right_logical(f, 2), lax.bitwise_and(f, FAR - 1)
        key = lax.shift_right_logical(j, 1) * keyed + first + 4 * s + lax.bitwise_and(j, 1)
        return jnp.where((f >= 0) & (f < far), key, -1)

    key4 = far_key(0)
    for m in range(4):
        for slot in range(groups):
            key = (m & 1) * keyed + 2 * farp + peer_ref[slot] * 8 + 1 + (m >> 1)
            key4 = jnp.where(src == kids_at + m * groupp + slot, key, key4)
    key5 = far_key(farp)
    p = src - coarse_at
    holds = (p >= 0) & (p < n_dom)
    key5 = jnp.where(holds, 2 * farp + 8 * p, key5)
    land4 = landing_rows([key4])
    land5 = landing_rows([key5, jnp.where(holds, keyed + 2 * farp + 8 * p, -1)])

    joined = projected[:, 0:square] + projected[:, square:]
    lift = [mortar_ref[m * square : (m + 1) * square, :] for m in range(4)]
    share = []
    for m in range(4):
        first = kids_at + m * groupp
        share.append(product(joined, lift[m]) - own[first : first + groupp, 0:square])
    share = [jnp.zeros((kids_at, square), F32)] + share
    if sources > used:
        share.append(jnp.zeros((sources - used, square), F32))
    high, low = halves_of(jnp.concatenate(share, axis=0).T)
    add_level(0, dot(high, hot_src, over) + dot(low, hot_src, over))
    add_tiles(low_i, spread_rows(take_rows(hot1l, face1), hot0l))
    add_tiles(high_i, spread_rows(take_rows(hot0l, face0), hot1l))

    for there, mine, theirs, device in sides:
        @pl.when(there)
        def _():
            side_copy(mine, mine, device).wait()

    add_tiles(low_i, spread_rows(side_in[0, 0:rim, 0:square], hot0s))
    add_tiles(high_i, spread_rows(side_in[1, 0:rim, 0:square], hot1s))
    add2 = spread_rows(side_in[2, 0:near, 0:square], hot2)
    add3 = spread_rows(side_in[3, 0:near, 0:square], hot3)
    add_tiles(low_j, add2)
    add_tiles(high_j, add3)

    def sent_all(step, carry):
        mail(step, True).wait_send()
        return carry

    lax.fori_loop(1, n_dom, sent_all, 0, unroll=n_dom <= 8)
    for side in range(2):
        for s in range(shifts):
            @pl.when(far_there(side, s))
            def _():
                far_copy(side, s, True).wait()

    def wait_all(step, carry):
        mail(step, True).wait_recv()
        return carry

    lax.fori_loop(1, n_dom, wait_all, 0, unroll=n_dom <= 8)

    received = [far_in[0], far_in[1], mort_in[...]]
    spare = keyed - 2 * farp - 8 * n_dom
    if spare:
        received.append(jnp.zeros((spare, 128), F32))
    received = jnp.concatenate(received, axis=0).T
    received = jnp.concatenate([received[0:square], received[square:]], axis=1)
    both = jnp.concatenate(halves_of(received), axis=0)
    for k, land in ((0, land4), (last, land5)):
        added = dot(both, land)
        add_level(k, added[0:square] + added[square:])


def kernel(sizes, semaphores, *refs):
    pl.run_scoped(
        functools.partial(steps, sizes, *refs),
        *[pltpu.SemaphoreType.DMA(shape) for shape in semaphores],
    )


def body(
    sizes,
    nodal_values,
    kappa,
    levels,
    local_faces,
    sub_faces,
    near_faces,
    far_faces,
    child_faces,
    child_peer,
    coarse_faces,
):
    n_dom, n_sub = sizes
    elems = nodal_values.shape[1]
    krons = [np.kron(HALVES[m // 2], HALVES[m % 2]) for m in range(4)]
    mortar = np.concatenate([m.T for m in krons], axis=0)
    far_rows = up(far_faces.shape[1])
    held = (elems // 128, NPTS**3, 128)
    side_rows = up(max(sub_faces.shape[1], near_faces.shape[1]))
    small = [
        levels.reshape(1, elems),
        local_faces,
        sub_faces,
        near_faces,
        jnp.asarray(folds(), F32),
        jnp.asarray(stencils(), BF16),
        jnp.asarray(mortar, F32),
    ]
    tables = [far_faces, child_faces, child_peer, coarse_faces]
    far_slots = (2, far_faces.shape[1] // FAR)
    semaphores = [(len(small) + len(tables),), (NPTS**3 // 128,), (4,), (4,)]
    semaphores += [far_slots, far_slots, (n_dom,), (n_dom,)]
    hbm = pl.BlockSpec(memory_space=pltpu.HBM)
    vmem = pl.BlockSpec(memory_space=pltpu.VMEM)
    applied = pl.pallas_call(
        functools.partial(kernel, sizes, semaphores),
        out_shape=pltpu.VMEM((held[0] * held[1], 128), F32),
        in_specs=[hbm] * 13,
        out_specs=vmem,
        scratch_shapes=[pltpu.VMEM(item.shape, item.dtype) for item in small]
        + [pltpu.SMEM(item.shape, I32) for item in tables]
        + [
            pltpu.VMEM((2, *held), F32),
            pltpu.VMEM(held, F32),
            pltpu.VMEM((4, side_rows, 128), F32),
            pltpu.VMEM((4, side_rows, 128), F32),
            pltpu.VMEM((2, far_rows, 128), F32),
            pltpu.VMEM((2, far_rows, 128), F32),
            pltpu.VMEM((n_dom * 8, 128), F32),
            pltpu.VMEM((n_dom * 8, 128), F32),
        ],
        compiler_params=pltpu.CompilerParams(
            collective_id=0, has_side_effects=True, vmem_limit_bytes=60 * 1024 * 1024
        ),
    )(
        nodal_values,
        kappa,
        *small,
        *tables,
    )
    applied = applied.reshape(NPTS * NPTS, held[0], NPTS, 128).transpose(0, 2, 1, 3)
    return applied.reshape(nodal_values.shape)


def solution(mesh):
    sizes = (mesh.shape["dom"], mesh.shape["sub"])
    wide = P(None, ("dom", "sub"))
    flat = P(("dom", "sub"))
    in_specs = (wide, wide, flat, wide, wide, wide, wide, wide, flat, flat)
    return jax.shard_map(
        functools.partial(body, sizes),
        mesh=mesh,
        in_specs=in_specs,
        out_specs=wide,
        check_vma=False,
    )
```

```python
import functools

import jax
import jax.numpy as jnp
import numpy as np
from jax import lax
from jax.experimental import pallas as pl
from jax.experimental.pallas import tpu as pltpu
from jax.sharding import PartitionSpec as P

NPTS = 8
FAR = 4
MESH = pl.DeviceIdType.MESH
F32, BF16, I32 = jnp.float32, jnp.bfloat16, jnp.int32


def legendre_table(points, degree):
    table = [np.ones(points.shape), points.copy()]
    for order in range(2, degree + 1):
        table.append(
            ((2 * order - 1) * points * table[order - 1] - (order - 1) * table[order - 2]) / order
        )
    return table


def lobatto_points(degree):
    points = np.cos(np.pi * np.arange(degree + 1) / degree)
    for sweep in range(100):
        table = legendre_table(points, degree)
        points = points - (points * table[degree] - table[degree - 1]) / (
            (degree + 1) * table[degree]
        )
    points = np.sort(points)
    return (points, legendre_table(points, degree)[degree])


def node_tables(count):
    degree = count - 1
    points, legendre = lobatto_points(degree)
    weights = 2.0 / (degree * (degree + 1) * legendre**2)
    spread = points[:, None] - points[None, :] + np.eye(count)
    derivative = legendre[:, None] / (legendre[None, :] * spread) * (1.0 - np.eye(count))
    derivative[0, 0] = -degree * (degree + 1) / 4.0
    derivative[degree, degree] = degree * (degree + 1) / 4.0
    halves = []
    for side in range(2):
        target = (points + 2.0 * side - 1.0) / 2.0
        matrix = np.ones((count, count))
        for column in range(count):
            for other in range(count):
                if other != column:
                    matrix[:, column] = (
                        matrix[:, column]
                        * (target - points[other])
                        / (points[column] - points[other])
                    )
        halves.append(matrix)
    return (points, weights, derivative, np.stack(halves))


POINTS, WEIGHTS, DERIV, HALVES = node_tables(NPTS)


def up(count, unit=8):
    return -(-count // unit) * unit


def halves_of(values):
    high = values.astype(BF16)
    return high, (values - high.astype(F32)).astype(BF16)


def numpy_halves(matrix):
    matrix = np.asarray(matrix, np.float32)
    high = matrix.astype(jnp.bfloat16)
    low = (matrix - high.astype(np.float32)).astype(jnp.bfloat16)
    return high, low


def dot(a, b, dims=((1,), (0,))):
    return lax.dot_general(a, b, (dims, ((), ())), preferred_element_type=F32)


def select(hot, values):
    high, low = halves_of(values)
    return dot(hot, high) + dot(hot, low)


def take_rows(hot, face):
    high, low = halves_of(face)
    dims = ((1,), (1,))
    return dot(hot, high, dims) + dot(hot, low, dims)


def spread_rows(rows, hot):
    high, low = halves_of(rows.T)
    return dot(high, hot) + dot(low, hot)


def product(a, matrix):
    high, low = halves_of(a)
    mhigh, mlow = halves_of(matrix)
    return dot(high, mhigh) + dot(low, mhigh) + dot(high, mlow)


def column(row, padded):
    count = row.shape[1]
    r = lax.broadcasted_iota(I32, (padded, count), 0)
    c = lax.broadcasted_iota(I32, (padded, count), 1)
    spread = jnp.where(r == c, jnp.broadcast_to(row.astype(F32), (padded, count)), 0.0)
    col = jnp.sum(spread, axis=1, keepdims=True)
    inside = lax.broadcasted_iota(I32, (padded, 1), 0) < count
    return jnp.where(inside, col, -1.0)


def hot_rows(columns, base, elems, kind=BF16):
    col = columns[0] if len(columns) == 1 else jnp.concatenate(columns, axis=0)
    lane = lax.broadcasted_iota(I32, (col.shape[0], elems), 1).astype(F32)
    return jnp.where(lane == col - float(base), 1.0, 0.0).astype(kind)


def line(values, matrix):
    half = NPTS // 2
    even = [values[i] + values[NPTS - 1 - i] for i in range(half)]
    odd = [values[i] - values[NPTS - 1 - i] for i in range(half)]
    out = [None] * NPTS
    for a in range(half):
        p = q = None
        for i in range(half):
            s = float((matrix[a, i] + matrix[a, NPTS - 1 - i]) / 2)
            t = float((matrix[a, i] - matrix[a, NPTS - 1 - i]) / 2)
            p = even[i] * s if p is None else p + even[i] * s
            q = odd[i] * t if q is None else q + odd[i] * t
        out[a] = q + p
        out[NPTS - 1 - a] = q - p
    return out


def stencils():
    forth, back = np.kron(np.eye(16), DERIV), np.kron(np.eye(16), DERIV.T)
    pieces = [piece for table in (forth, back) for piece in numpy_halves(table)]
    return np.concatenate(pieces, axis=0)


def folds():
    heads = [(HALVES[m // 2], HALVES[m % 2]) for m in range(4)]
    heads += [(first.T, second.T) for first, second in heads]
    rows = np.concatenate([np.repeat(first, NPTS, axis=1) for first, _ in heads], axis=1)
    tiles = np.concatenate([np.tile(second, (1, NPTS)) for _, second in heads], axis=1)
    return np.concatenate([rows, tiles], axis=0).astype(np.float32)


def steps(
    sizes,
    u_hbm,
    kappa_hbm,
    level_hbm,
    local_hbm,
    sub_hbm,
    near_hbm,
    fold_hbm,
    deriv_hbm,
    mortar_hbm,
    far_hbm,
    child_hbm,
    peer_hbm,
    coarse_hbm,
    w_ref,
    level_ref,
    local_ref,
    sub_ref,
    near_ref,
    fold_ref,
    deriv_ref,
    mortar_ref,
    far_ref,
    child_ref,
    peer_ref,
    coarse_ref,
    uk_ref,
    g_ref,
    side_out,
    side_in,
    far_out,
    far_in,
    mort_out,
    mort_in,
    small_sem,
    load_sem,
    side_send,
    side_recv,
    far_send,
    far_recv,
    mort_send,
    mort_recv,
):
    n_dom, n_sub = sizes
    u_ref, k_ref = uk_ref.at[0], uk_ref.at[1]
    parts = u_ref.shape[0]
    elems = parts * 128
    square = NPTS * NPTS
    last = NPTS - 1
    me, sub = lax.axis_index("dom"), lax.axis_index("sub")

    urgent = [
        (fold_hbm, fold_ref),
        (far_hbm, far_ref),
        (child_hbm, child_ref),
        (coarse_hbm, coarse_ref),
        (level_hbm, level_ref),
        (peer_hbm, peer_ref),
    ]
    later = [
        (local_hbm, local_ref),
        (sub_hbm, sub_ref),
        (near_hbm, near_ref),
        (deriv_hbm, deriv_ref),
        (mortar_hbm, mortar_ref),
    ]
    small = [
        pltpu.make_async_copy(source, target, small_sem.at[slot])
        for slot, (source, target) in enumerate(urgent + later)
    ]
    block = 128
    blocks = NPTS**3 // block

    def load(n, part, source, target):
        own = pl.ds(part * block, block)
        return pltpu.make_async_copy(
            source.at[own, pl.ds(n * 128, 128)], target.at[n, own], load_sem.at[part]
        )

    def loaded(part):
        whole = uk_ref.at[0, :, pl.ds(0, 2 * block)]
        pltpu.make_async_copy(whole, whole, load_sem.at[part]).wait()

    for copy in small[:6]:
        copy.start()
    for part in range(blocks):
        for n in range(parts):
            load(n, part, u_hbm, u_ref).start()
            load(n, part, kappa_hbm, k_ref).start()
    for copy in small[6:]:
        copy.start()

    far_in[...] = jnp.zeros(far_in.shape, F32)
    mort_in[...] = jnp.zeros(mort_in.shape, F32)

    barrier = pltpu.get_barrier_semaphore()

    def greet(step, carry):
        other = lax.rem(me + step, n_dom)
        pl.semaphore_signal(barrier, inc=1, device_id=(other, sub), device_id_type=MESH)
        return carry

    lax.fori_loop(1, n_dom, greet, 0, unroll=n_dom <= 8)

    @pl.when(sub > 0)
    def _():
        pl.semaphore_signal(barrier, inc=1, device_id=(me, sub - 1), device_id_type=MESH)

    @pl.when(sub < n_sub - 1)
    def _():
        pl.semaphore_signal(barrier, inc=1, device_id=(me, sub + 1), device_id_type=MESH)

    def clear(missing, slot):
        @pl.when(missing)
        def _():
            side_in[slot] = jnp.zeros(side_in.shape[1:], F32)

    clear(sub == 0, 0)
    clear(sub == n_sub - 1, 1)
    clear(me == 0, 2)
    clear(me == n_dom - 1, 3)

    pairs, rim, near = local_ref.shape[1], sub_ref.shape[1], near_ref.shape[1]
    far, groups = far_ref.shape[1], child_ref.shape[1]
    shifts = far // FAR
    farp, groupp, coarsep = up(far), up(groups), up(n_dom)
    coarse_at = 2 * farp
    kids_at = coarse_at + coarsep
    used = kids_at + 4 * groupp
    sources = up(used, 128)
    lane = lax.broadcasted_iota(I32, (8, sources), 1)
    row8 = lax.broadcasted_iota(I32, (8, sources), 0)
    on_low = (lane < farp) | (lane >= kids_at)
    reach = [
        jnp.where(on_low, float(WEIGHTS[c] * DERIV[c, 0]), float(WEIGHTS[c] * DERIV[c, last]))
        for c in range(NPTS)
    ]

    def shifted(matrix):
        tables = []
        for r in range(NPTS):
            table = jnp.zeros((8, sources), F32)
            for b in range(NPTS):
                table = jnp.where(row8 == b, float(matrix[b, (b + r) % NPTS]), table)
            tables.append(table)
        return tables

    def turn(tables, values):
        total = tables[0] * values
        for r in range(1, NPTS):
            total += tables[r] * pltpu.roll(values, NPTS - r, 0)
        return total

    forth8, back8 = shifted(DERIV), shifted(DERIV.T)
    quad8 = jnp.zeros((8, sources), F32)
    for k in range(NPTS):
        quad8 = jnp.where(row8 == k, float(WEIGHTS[k]), quad8)

    for copy in small[:6]:
        copy.wait()

    def held(first, ids, base):
        total = jnp.zeros((8, sources), I32)
        for slot, value in enumerate(ids):
            total = jnp.where(lane == first + slot, value + (1 - base * elems), total)
        return total

    ids = held(0, [far_ref[0, c] for c in range(far)], 4)
    ids += held(farp, [far_ref[1, c] for c in range(far)], 5)
    ids += held(coarse_at, [coarse_ref[c] for c in range(n_dom)], 5)
    for m in range(4):
        ids += held(kids_at + m * groupp, [child_ref[m, c] for c in range(groups)], 4)
    element = lax.broadcasted_iota(I32, (elems, sources), 0) + 1
    hot_src = jnp.where(element == ids[0:1], 1.0, 0.0).astype(BF16)
    scale = jnp.exp2(-level_ref[...].astype(F32))
    over = ((1,), (1,))

    def pick(ref, part):
        rows = []
        for k in range(NPTS):
            own = pl.ds(part * block + k, block // NPTS, NPTS)
            rows.append(jnp.concatenate([ref[n, own, :] for n in range(parts)], axis=1))
        high, low = halves_of(jnp.concatenate(rows, axis=0))
        both = dot(jnp.concatenate([high, low], axis=0), hot_src)
        return both[0:block] + both[block:]

    spot = jnp.bitwise_and(ids - 1, 127)
    piece = lax.shift_right_arithmetic(ids - 1, 7)
    lookup = lax.GatherDimensionNumbers(
        offset_dims=(),
        collapsed_slice_dims=(1,),
        start_index_map=(1,),
        operand_batching_dims=(0,),
        start_indices_batching_dims=(0,),
    )

    def fetch(ref, part):
        rows = []
        for k in range(NPTS):
            for at in range(0, block, NPTS * NPTS):
                own = pl.ds(part * block + at + k, NPTS, NPTS)
                tiles = []
                for first in range(0, sources, 128):
                    where = slice(first, first + 128)
                    found = jnp.zeros((8, 128), F32)
                    for n in range(parts):
                        taken = lax.gather(
                            ref[n, own, :],
                            spot[:, where][..., None],
                            lookup,
                            slice_sizes=(1, 1),
                            mode=lax.GatherScatterMode.PROMISE_IN_BOUNDS,
                        )
                        found = jnp.where(piece[:, where] == n, taken, found)
                    tiles.append(found)
                rows.append(tiles[0] if len(tiles) == 1 else jnp.concatenate(tiles, axis=1))
        return jnp.concatenate(rows, axis=0)

    edge = float(WEIGHTS[0])
    chosen = None
    along_k, along_j, plane_u, plane_g = [], [], [], []
    for part in range(blocks):
        if part % 2 == 0:
            loaded(part)
            loaded(part + 1)
        u_part, k_part = fetch(u_ref, part), pick(k_ref, part)
        if chosen is None:
            chosen = dot(jnp.broadcast_to(scale, (16, elems)).astype(BF16), hot_src)[0:8]
            chosen = chosen * quad8
        wide = block // NPTS
        for i in range(part * wide // NPTS, (part + 1) * wide // NPTS):
            at = i * NPTS - part * wide

            def strip(values, k):
                return values[k * wide + at : k * wide + at + NPTS]

            here = chosen * float(WEIGHTS[i])
            flat = jnp.where(on_low, strip(u_part, 0), strip(u_part, last))
            g = jnp.where(on_low, strip(k_part, 0), strip(k_part, last)) * (here * edge)
            plane_u.append(flat)
            plane_g.append(g)
            along_j.append(turn(back8, turn(forth8, flat) * g))
            deep = line([strip(u_part, k) for k in range(NPTS)], DERIV)
            total = reach[0] * strip(k_part, 0) * deep[0]
            for c in range(1, NPTS):
                total += reach[c] * strip(k_part, c) * deep[c]
            along_k.append(total * here)
    fold = [
        fold_ref[i : i + 1, :] * fold_ref[NPTS : 2 * NPTS, :] for i in range(NPTS)
    ]
    fold_high, fold_low = halves_of(jnp.concatenate(fold, axis=0))
    across_i = line(plane_u, DERIV)
    along_i = line([across_i[i] * plane_g[i] for i in range(NPTS)], DERIV.T)
    summed = [along_i[i] + (along_j[i] + along_k[i]) for i in range(NPTS)]
    own = jnp.concatenate(summed + summed, axis=0).T

    def folded(rows, first, width):
        high, low = halves_of(rows)
        cols = slice(first, first + width)
        both = dot(jnp.concatenate([high, low], axis=0), fold_high[:, cols])
        return both[0 : rows.shape[0]] + both[rows.shape[0] :] + dot(high, fold_low[:, cols])

    raised = folded(own[coarse_at : coarse_at + up(coarsep, 16), 0:square], 256, 256)
    kids = folded(own[kids_at:used, 0:square], 0, 256)

    half = lax.broadcasted_iota(I32, (8, 128), 1) < square
    for side in range(2):
        for first in range(0, farp, 8):
            faces = own[side * farp + first : side * farp + first + 8]
            far_out[side, first : first + 8] = jnp.where(half, faces, pltpu.roll(faces, 6, 0))
    half_g = lax.broadcasted_iota(I32, (groupp, 128), 1) < square
    kid = [kids[m * groupp : (m + 1) * groupp] for m in range(4)]
    projected = jnp.where(half_g, kid[0][:, 0:128], kid[1][:, 0:128]) + jnp.where(
        half_g, kid[2][:, 128:256], kid[3][:, 128:256]
    )
    peer_row = lax.broadcasted_iota(I32, (n_dom, 128), 0)
    routed = jnp.zeros((n_dom, 128), F32)
    for slot in range(groups):
        routed = jnp.where(peer_row == peer_ref[slot], projected[slot : slot + 1], routed)
    mort_out[pl.ds(0, n_dom, 8), :] = routed
    mort_out[pl.ds(1, n_dom, 8), :] = raised[0:n_dom, 0:128]
    mort_out[pl.ds(2, n_dom, 8), :] = raised[0:n_dom, 128:256]

    greeted = n_dom - 1 + (sub > 0).astype(I32) + (sub < n_sub - 1).astype(I32)

    def mail(step, landing):
        other = lax.rem(me + step, n_dom)
        return pltpu.make_async_remote_copy(
            src_ref=mort_out.at[pl.ds(pl.multiple_of(other * 8, 8), 3)],
            dst_ref=mort_in.at[
                pl.ds(pl.multiple_of((other if landing else me) * 8, 8), 3)
            ],
            send_sem=mort_send.at[other],
            recv_sem=mort_recv.at[other if landing else me],
            device_id=(other, sub),
            device_id_type=MESH,
        )

    def far_copy(side, s, landing):
        other = me - s - 2 if side == 0 else me + s + 2
        rows = pl.ds(s * FAR, FAR // 2)
        there = side if landing else 1 - side
        return pltpu.make_async_remote_copy(
            src_ref=far_out.at[side, rows],
            dst_ref=far_in.at[there, rows],
            send_sem=far_send.at[side, s],
            recv_sem=far_recv.at[there, s],
            device_id=(other, sub),
            device_id_type=MESH,
        )

    def far_there(side, s):
        return me >= s + 2 if side == 0 else me + s + 2 < n_dom

    def send_messages():
        pl.semaphore_wait(barrier, greeted)

        def start_all(step, carry):
            mail(step, False).start()
            return carry

        lax.fori_loop(1, n_dom, start_all, 0, unroll=n_dom <= 8)
        for side in range(2):
            for s in range(shifts):
                @pl.when(far_there(side, s))
                def _():
                    far_copy(side, s, False).start()

    early = me < 3

    @pl.when(jnp.logical_not(early))
    def _():
        send_messages()

    for copy in small[6:]:
        copy.wait()

    hot0l = hot_rows([column(local_ref[1:2], up(pairs))], 0, elems)
    hot1l = hot_rows([column(local_ref[0:1], up(pairs))], elems, elems)
    hot0s = hot_rows([column(sub_ref[0:1], up(rim))], 0, elems)
    hot1s = hot_rows([column(sub_ref[1:2], up(rim))], elems, elems)
    hot2 = hot_rows([column(near_ref[0:1], up(near))], 2 * elems, elems)
    hot3 = hot_rows([column(near_ref[1:2], up(near))], 3 * elems, elems)

    sub8 = lax.broadcasted_iota(I32, (8, elems), 0)
    weight = jnp.zeros((8, elems), F32)
    for k in range(NPTS):
        weight = jnp.where(sub8 == k, float(WEIGHTS[k]), weight)
    weight = weight * scale

    def slab(i, j):
        return pl.ds((i * NPTS + j) * NPTS, NPTS)

    def across(ref, own):
        return jnp.concatenate([ref[n, own, :] for n in range(parts)], axis=1)

    def spot_of(n, i, j):
        return pl.ds(((i * NPTS + j) * parts + n) * NPTS, NPTS)

    def face_of(tiles):
        return jnp.concatenate(
            [
                jnp.concatenate([w_ref[spot_of(n, i, j), :] for i, j in tiles], axis=0)
                for n in range(parts)
            ],
            axis=1,
        )

    def add_tiles(tiles, values):
        for t, (i, j) in enumerate(tiles):
            for n in range(parts):
                w_ref[spot_of(n, i, j), :] += values[
                    t * NPTS : (t + 1) * NPTS, n * 128 : (n + 1) * 128
                ]

    def add_level(k, values):
        for n in range(parts):
            own_rows = pl.ds(n * NPTS + k, square, parts * NPTS)
            w_ref[own_rows, :] += values[:, n * 128 : (n + 1) * 128]

    turns = [deriv_ref[128 * n : 128 * n + 128, :] for n in range(4)]

    def along(pair, values):
        high, low = halves_of(values)
        both = jnp.concatenate([high, low], axis=0)
        return dot(jnp.concatenate([pair[0], pair[0]], axis=1), both) + dot(pair[1], high)

    for n in range(parts):
        here = weight[:, n * 128 : (n + 1) * 128]
        for i in range(NPTS):
            for j in range(NPTS):
                g_ref[n, slab(i, j), :] = k_ref[n, slab(i, j), :] * (
                    here * float(WEIGHTS[i] * WEIGHTS[j])
                )
    for part in range(blocks):
        own_rows = pl.ds(part * block, block)
        turn = along(turns[0:2], across(u_ref, own_rows)) * across(g_ref, own_rows)
        turn = along(turns[2:4], turn)
        for t in range(block // NPTS):
            i, j = divmod(part * block // NPTS + t, NPTS)
            for n in range(parts):
                w_ref[spot_of(n, i, j), :] = turn[
                    t * NPTS : (t + 1) * NPTS, n * 128 : (n + 1) * 128
                ]
    for n in range(parts):
        for j in range(NPTS):
            turn = line([u_ref[n, slab(i, j), :] for i in range(NPTS)], DERIV)
            turn = [turn[i] * g_ref[n, slab(i, j), :] for i in range(NPTS)]
            turn = line(turn, DERIV.T)
            for i in range(NPTS):
                w_ref[spot_of(n, i, j), :] += turn[i]
        for i in range(NPTS):
            turn = line([u_ref[n, slab(i, j), :] for j in range(NPTS)], DERIV)
            turn = [turn[j] * g_ref[n, slab(i, j), :] for j in range(NPTS)]
            turn = line(turn, DERIV.T)
            for j in range(NPTS):
                w_ref[spot_of(n, i, j), :] += turn[j]

    low_i, high_i = ([(i, j) for j in range(NPTS)] for i in (0, last))
    low_j, high_j = ([(i, j) for i in range(NPTS)] for j in (0, last))
    face0, face1, face2, face3 = (face_of(tiles) for tiles in (low_i, high_i, low_j, high_j))
    side_out[0, 0:rim, 0:square] = take_rows(hot0s, face0)[0:rim]
    side_out[1, 0:rim, 0:square] = take_rows(hot1s, face1)[0:rim]
    side_out[2, 0:near, 0:square] = take_rows(hot2, face2)[0:near]
    side_out[3, 0:near, 0:square] = take_rows(hot3, face3)[0:near]

    @pl.when(early)
    def _():
        send_messages()

    sides = [
        (sub > 0, 0, 1, (me, sub - 1)),
        (sub < n_sub - 1, 1, 0, (me, sub + 1)),
        (me > 0, 2, 3, (me - 1, sub)),
        (me < n_dom - 1, 3, 2, (me + 1, sub)),
    ]

    def side_copy(mine, theirs, device):
        return pltpu.make_async_remote_copy(
            src_ref=side_out.at[mine],
            dst_ref=side_in.at[theirs],
            send_sem=side_send.at[mine],
            recv_sem=side_recv.at[theirs],
            device_id=device,
            device_id_type=MESH,
        )

    for there, mine, theirs, device in sides:
        @pl.when(there)
        def _():
            side_copy(mine, theirs, device).start()

    keyed = up(2 * farp + 8 * n_dom, 128)

    def landing_rows(keys):
        at = lax.broadcasted_iota(I32, (2 * keyed, sources), 0)
        hit = at == keys[0]
        for key in keys[1:]:
            hit = hit | (at == key)
        return dot(jnp.where(hit, 1.0, 0.0).astype(BF16), hot_src, over).astype(BF16)

    src = lax.broadcasted_iota(I32, (1, sources), 1)

    def far_key(first):
        f = src - first
        s, j = lax.shift_right_logical(f, 2), lax.bitwise_and(f, FAR - 1)
        key = lax.shift_right_logical(j, 1) * keyed + first + 4 * s + lax.bitwise_and(j, 1)
        return jnp.where((f >= 0) & (f < far), key, -1)

    key4 = far_key(0)
    for m in range(4):
        for slot in range(groups):
            key = (m & 1) * keyed + 2 * farp + peer_ref[slot] * 8 + 1 + (m >> 1)
            key4 = jnp.where(src == kids_at + m * groupp + slot, key, key4)
    key5 = far_key(farp)
    p = src - coarse_at
    holds = (p >= 0) & (p < n_dom)
    key5 = jnp.where(holds, 2 * farp + 8 * p, key5)
    land4 = landing_rows([key4])
    land5 = landing_rows([key5, jnp.where(holds, keyed + 2 * farp + 8 * p, -1)])

    joined = projected[:, 0:square] + projected[:, square:]
    lift = [mortar_ref[m * square : (m + 1) * square, :] for m in range(4)]
    share = []
    for m in range(4):
        first = kids_at + m * groupp
        share.append(product(joined, lift[m]) - own[first : first + groupp, 0:square])
    share = [jnp.zeros((kids_at, square), F32)] + share
    if sources > used:
        share.append(jnp.zeros((sources - used, square), F32))
    high, low = halves_of(jnp.concatenate(share, axis=0).T)
    add_level(0, dot(high, hot_src, over) + dot(low, hot_src, over))
    add_tiles(low_i, spread_rows(take_rows(hot1l, face1), hot0l))
    add_tiles(high_i, spread_rows(take_rows(hot0l, face0), hot1l))

    for there, mine, theirs, device in sides:
        @pl.when(there)
        def _():
            side_copy(mine, mine, device).wait()

    add_tiles(low_i, spread_rows(side_in[0, 0:rim, 0:square], hot0s))
    add_tiles(high_i, spread_rows(side_in[1, 0:rim, 0:square], hot1s))
    add2 = spread_rows(side_in[2, 0:near, 0:square], hot2)
    add3 = spread_rows(side_in[3, 0:near, 0:square], hot3)
    add_tiles(low_j, add2)
    add_tiles(high_j, add3)

    def sent_all(step, carry):
        mail(step, True).wait_send()
        return carry

    lax.fori_loop(1, n_dom, sent_all, 0, unroll=n_dom <= 8)
    for side in range(2):
        for s in range(shifts):
            @pl.when(far_there(side, s))
            def _():
                far_copy(side, s, True).wait()

    def wait_all(step, carry):
        mail(step, True).wait_recv()
        return carry

    lax.fori_loop(1, n_dom, wait_all, 0, unroll=n_dom <= 8)

    received = [far_in[0], far_in[1], mort_in[...]]
    spare = keyed - 2 * farp - 8 * n_dom
    if spare:
        received.append(jnp.zeros((spare, 128), F32))
    received = jnp.concatenate(received, axis=0).T
    received = jnp.concatenate([received[0:square], received[square:]], axis=1)
    both = jnp.concatenate(halves_of(received), axis=0)
    for k, land in ((0, land4), (last, land5)):
        added = dot(both, land)
        add_level(k, added[0:square] + added[square:])


def kernel(sizes, semaphores, *refs):
    pl.run_scoped(
        functools.partial(steps, sizes, *refs),
        *[pltpu.SemaphoreType.DMA(shape) for shape in semaphores],
    )


def body(
    sizes,
    nodal_values,
    kappa,
    levels,
    local_faces,
    sub_faces,
    near_faces,
    far_faces,
    child_faces,
    child_peer,
    coarse_faces,
):
    n_dom, n_sub = sizes
    elems = nodal_values.shape[1]
    krons = [np.kron(HALVES[m // 2], HALVES[m % 2]) for m in range(4)]
    mortar = np.concatenate([m.T for m in krons], axis=0)
    far_rows = up(far_faces.shape[1])
    held = (elems // 128, NPTS**3, 128)
    side_rows = up(max(sub_faces.shape[1], near_faces.shape[1]))
    small = [
        levels.reshape(1, elems),
        local_faces,
        sub_faces,
        near_faces,
        jnp.asarray(folds(), F32),
        jnp.asarray(stencils(), BF16),
        jnp.asarray(mortar, F32),
    ]
    tables = [far_faces, child_faces, child_peer, coarse_faces]
    far_slots = (2, far_faces.shape[1] // FAR)
    semaphores = [(len(small) + len(tables),), (NPTS**3 // 128,), (4,), (4,)]
    semaphores += [far_slots, far_slots, (n_dom,), (n_dom,)]
    hbm = pl.BlockSpec(memory_space=pltpu.HBM)
    vmem = pl.BlockSpec(memory_space=pltpu.VMEM)
    applied = pl.pallas_call(
        functools.partial(kernel, sizes, semaphores),
        out_shape=pltpu.VMEM((held[0] * held[1], 128), F32),
        in_specs=[hbm] * 13,
        out_specs=vmem,
        scratch_shapes=[pltpu.VMEM(item.shape, item.dtype) for item in small]
        + [pltpu.SMEM(item.shape, I32) for item in tables]
        + [
            pltpu.VMEM((2, *held), F32),
            pltpu.VMEM(held, F32),
            pltpu.VMEM((4, side_rows, 128), F32),
            pltpu.VMEM((4, side_rows, 128), F32),
            pltpu.VMEM((2, far_rows, 128), F32),
            pltpu.VMEM((2, far_rows, 128), F32),
            pltpu.VMEM((n_dom * 8, 128), F32),
            pltpu.VMEM((n_dom * 8, 128), F32),
        ],
        compiler_params=pltpu.CompilerParams(
            collective_id=0, has_side_effects=True, vmem_limit_bytes=60 * 1024 * 1024
        ),
    )(
        nodal_values,
        kappa,
        *small,
        *tables,
    )
    applied = applied.reshape(NPTS * NPTS, held[0], NPTS, 128).transpose(0, 2, 1, 3)
    return applied.reshape(nodal_values.shape)


def solution(mesh):
    sizes = (mesh.shape["dom"], mesh.shape["sub"])
    wide = P(None, ("dom", "sub"))
    flat = P(("dom", "sub"))
    in_specs = (wide, wide, flat, wide, wide, wide, wide, wide, flat, flat)
    return jax.shard_map(
        functools.partial(body, sizes),
        mesh=mesh,
        in_specs=in_specs,
        out_specs=wide,
        check_vma=False,
    )
```

```python
import functools

import jax
import jax.numpy as jnp
import numpy as np
from jax import lax
from jax.experimental import pallas as pl
from jax.experimental.pallas import tpu as pltpu
from jax.sharding import PartitionSpec as P

NPTS = 8
FAR = 4
MESH = pl.DeviceIdType.MESH
F32, BF16, I32 = jnp.float32, jnp.bfloat16, jnp.int32


def legendre_table(points, degree):
    table = [np.ones(points.shape), points.copy()]
    for order in range(2, degree + 1):
        table.append(
            ((2 * order - 1) * points * table[order - 1] - (order - 1) * table[order - 2]) / order
        )
    return table


def lobatto_points(degree):
    points = np.cos(np.pi * np.arange(degree + 1) / degree)
    for sweep in range(100):
        table = legendre_table(points, degree)
        points = points - (points * table[degree] - table[degree - 1]) / (
            (degree + 1) * table[degree]
        )
    points = np.sort(points)
    return (points, legendre_table(points, degree)[degree])


def node_tables(count):
    degree = count - 1
    points, legendre = lobatto_points(degree)
    weights = 2.0 / (degree * (degree + 1) * legendre**2)
    spread = points[:, None] - points[None, :] + np.eye(count)
    derivative = legendre[:, None] / (legendre[None, :] * spread) * (1.0 - np.eye(count))
    derivative[0, 0] = -degree * (degree + 1) / 4.0
    derivative[degree, degree] = degree * (degree + 1) / 4.0
    halves = []
    for side in range(2):
        target = (points + 2.0 * side - 1.0) / 2.0
        matrix = np.ones((count, count))
        for column in range(count):
            for other in range(count):
                if other != column:
                    matrix[:, column] = (
                        matrix[:, column]
                        * (target - points[other])
                        / (points[column] - points[other])
                    )
        halves.append(matrix)
    return (points, weights, derivative, np.stack(halves))


POINTS, WEIGHTS, DERIV, HALVES = node_tables(NPTS)


def up(count, unit=8):
    return -(-count // unit) * unit


def halves_of(values):
    high = values.astype(BF16)
    return high, (values - high.astype(F32)).astype(BF16)


def numpy_halves(matrix):
    matrix = np.asarray(matrix, np.float32)
    high = matrix.astype(jnp.bfloat16)
    low = (matrix - high.astype(np.float32)).astype(jnp.bfloat16)
    return high, low


def dot(a, b, dims=((1,), (0,))):
    return lax.dot_general(a, b, (dims, ((), ())), preferred_element_type=F32)


def select(hot, values):
    high, low = halves_of(values)
    return dot(hot, high) + dot(hot, low)


def take_rows(hot, face):
    high, low = halves_of(face)
    dims = ((1,), (1,))
    return dot(hot, high, dims) + dot(hot, low, dims)


def spread_rows(rows, hot):
    high, low = halves_of(rows.T)
    return dot(high, hot) + dot(low, hot)


def product(a, matrix):
    high, low = halves_of(a)
    mhigh, mlow = halves_of(matrix)
    return dot(high, mhigh) + dot(low, mhigh) + dot(high, mlow)


def column(row, padded):
    count = row.shape[1]
    r = lax.broadcasted_iota(I32, (padded, count), 0)
    c = lax.broadcasted_iota(I32, (padded, count), 1)
    spread = jnp.where(r == c, jnp.broadcast_to(row.astype(F32), (padded, count)), 0.0)
    col = jnp.sum(spread, axis=1, keepdims=True)
    inside = lax.broadcasted_iota(I32, (padded, 1), 0) < count
    return jnp.where(inside, col, -1.0)


def hot_rows(columns, base, elems, kind=BF16):
    col = columns[0] if len(columns) == 1 else jnp.concatenate(columns, axis=0)
    lane = lax.broadcasted_iota(I32, (col.shape[0], elems), 1).astype(F32)
    return jnp.where(lane == col - float(base), 1.0, 0.0).astype(kind)


def line(values, matrix):
    half = NPTS // 2
    even = [values[i] + values[NPTS - 1 - i] for i in range(half)]
    odd = [values[i] - values[NPTS - 1 - i] for i in range(half)]
    out = [None] * NPTS
    for a in range(half):
        p = q = None
        for i in range(half):
            s = float((matrix[a, i] + matrix[a, NPTS - 1 - i]) / 2)
            t = float((matrix[a, i] - matrix[a, NPTS - 1 - i]) / 2)
            p = even[i] * s if p is None else p + even[i] * s
            q = odd[i] * t if q is None else q + odd[i] * t
        out[a] = q + p
        out[NPTS - 1 - a] = q - p
    return out


def stencils():
    forth, back = np.kron(np.eye(16), DERIV), np.kron(np.eye(16), DERIV.T)
    pieces = [piece for table in (forth, back) for piece in numpy_halves(table)]
    return np.concatenate(pieces, axis=0)


def folds():
    heads = [(HALVES[m // 2], HALVES[m % 2]) for m in range(4)]
    heads += [(first.T, second.T) for first, second in heads]
    rows = np.concatenate([np.repeat(first, NPTS, axis=1) for first, _ in heads], axis=1)
    tiles = np.concatenate([np.tile(second, (1, NPTS)) for _, second in heads], axis=1)
    return np.concatenate([rows, tiles], axis=0).astype(np.float32)


def steps(
    sizes,
    u_hbm,
    kappa_hbm,
    level_hbm,
    local_hbm,
    sub_hbm,
    near_hbm,
    fold_hbm,
    deriv_hbm,
    mortar_hbm,
    far_hbm,
    child_hbm,
    peer_hbm,
    coarse_hbm,
    w_ref,
    arrived_ref,
    land_ref,
    level_ref,
    local_ref,
    sub_ref,
    near_ref,
    fold_ref,
    deriv_ref,
    mortar_ref,
    far_ref,
    child_ref,
    peer_ref,
    coarse_ref,
    uk_ref,
    g_ref,
    side_out,
    side_in,
    far_out,
    far_in,
    mort_out,
    mort_in,
    small_sem,
    load_sem,
    side_send,
    side_recv,
    far_send,
    far_recv,
    mort_send,
    mort_recv,
):
    n_dom, n_sub = sizes
    u_ref, k_ref = uk_ref.at[0], uk_ref.at[1]
    parts = u_ref.shape[0]
    elems = parts * 128
    square = NPTS * NPTS
    last = NPTS - 1
    me, sub = lax.axis_index("dom"), lax.axis_index("sub")

    urgent = [
        (fold_hbm, fold_ref),
        (far_hbm, far_ref),
        (child_hbm, child_ref),
        (coarse_hbm, coarse_ref),
        (level_hbm, level_ref),
        (peer_hbm, peer_ref),
    ]
    later = [
        (local_hbm, local_ref),
        (sub_hbm, sub_ref),
        (near_hbm, near_ref),
        (deriv_hbm, deriv_ref),
        (mortar_hbm, mortar_ref),
    ]
    small = [
        pltpu.make_async_copy(source, target, small_sem.at[slot])
        for slot, (source, target) in enumerate(urgent + later)
    ]
    block = 128
    blocks = NPTS**3 // block

    def load(n, part, source, target):
        own = pl.ds(part * block, block)
        return pltpu.make_async_copy(
            source.at[own, pl.ds(n * 128, 128)], target.at[n, own], load_sem.at[part]
        )

    def loaded(part):
        whole = uk_ref.at[0, :, pl.ds(0, 2 * block)]
        pltpu.make_async_copy(whole, whole, load_sem.at[part]).wait()

    for copy in small[:6]:
        copy.start()
    for part in range(blocks):
        for n in range(parts):
            load(n, part, u_hbm, u_ref).start()
            load(n, part, kappa_hbm, k_ref).start()
    for copy in small[6:]:
        copy.start()

    far_in[...] = jnp.zeros(far_in.shape, F32)
    mort_in[...] = jnp.zeros(mort_in.shape, F32)

    barrier = pltpu.get_barrier_semaphore()

    def greet(step, carry):
        other = lax.rem(me + step, n_dom)
        pl.semaphore_signal(barrier, inc=1, device_id=(other, sub), device_id_type=MESH)
        return carry

    lax.fori_loop(1, n_dom, greet, 0, unroll=n_dom <= 8)

    @pl.when(sub > 0)
    def _():
        pl.semaphore_signal(barrier, inc=1, device_id=(me, sub - 1), device_id_type=MESH)

    @pl.when(sub < n_sub - 1)
    def _():
        pl.semaphore_signal(barrier, inc=1, device_id=(me, sub + 1), device_id_type=MESH)

    def clear(missing, slot):
        @pl.when(missing)
        def _():
            side_in[slot] = jnp.zeros(side_in.shape[1:], F32)

    clear(sub == 0, 0)
    clear(sub == n_sub - 1, 1)
    clear(me == 0, 2)
    clear(me == n_dom - 1, 3)

    pairs, rim, near = local_ref.shape[1], sub_ref.shape[1], near_ref.shape[1]
    far, groups = far_ref.shape[1], child_ref.shape[1]
    shifts = far // FAR
    farp, groupp, coarsep = up(far), up(groups), up(n_dom)
    coarse_at = 2 * farp
    kids_at = coarse_at + coarsep
    used = kids_at + 4 * groupp
    sources = up(used, 128)
    lane = lax.broadcasted_iota(I32, (8, sources), 1)
    row8 = lax.broadcasted_iota(I32, (8, sources), 0)
    on_low = (lane < farp) | (lane >= kids_at)
    reach = [
        jnp.where(on_low, float(WEIGHTS[c] * DERIV[c, 0]), float(WEIGHTS[c] * DERIV[c, last]))
        for c in range(NPTS)
    ]

    def shifted(matrix):
        tables = []
        for r in range(NPTS):
            table = jnp.zeros((8, sources), F32)
            for b in range(NPTS):
                table = jnp.where(row8 == b, float(matrix[b, (b + r) % NPTS]), table)
            tables.append(table)
        return tables

    def turn(tables, values):
        total = tables[0] * values
        for r in range(1, NPTS):
            total += tables[r] * pltpu.roll(values, NPTS - r, 0)
        return total

    forth8, back8 = shifted(DERIV), shifted(DERIV.T)
    quad8 = jnp.zeros((8, sources), F32)
    for k in range(NPTS):
        quad8 = jnp.where(row8 == k, float(WEIGHTS[k]), quad8)

    for copy in small[:6]:
        copy.wait()

    def held(first, ids, base):
        total = jnp.zeros((8, sources), I32)
        for slot, value in enumerate(ids):
            total = jnp.where(lane == first + slot, value + (1 - base * elems), total)
        return total

    ids = held(0, [far_ref[0, c] for c in range(far)], 4)
    ids += held(farp, [far_ref[1, c] for c in range(far)], 5)
    ids += held(coarse_at, [coarse_ref[c] for c in range(n_dom)], 5)
    for m in range(4):
        ids += held(kids_at + m * groupp, [child_ref[m, c] for c in range(groups)], 4)
    element = lax.broadcasted_iota(I32, (elems, sources), 0) + 1
    hot_src = jnp.where(element == ids[0:1], 1.0, 0.0).astype(BF16)
    scale = jnp.exp2(-level_ref[...].astype(F32))
    over = ((1,), (1,))

    def pick(ref, part):
        rows = []
        for k in range(NPTS):
            own = pl.ds(part * block + k, block // NPTS, NPTS)
            rows.append(jnp.concatenate([ref[n, own, :] for n in range(parts)], axis=1))
        high, low = halves_of(jnp.concatenate(rows, axis=0))
        both = dot(jnp.concatenate([high, low], axis=0), hot_src)
        return both[0:block] + both[block:]

    spot = jnp.bitwise_and(ids - 1, 127)
    piece = lax.shift_right_arithmetic(ids - 1, 7)
    lookup = lax.GatherDimensionNumbers(
        offset_dims=(),
        collapsed_slice_dims=(1,),
        start_index_map=(1,),
        operand_batching_dims=(0,),
        start_indices_batching_dims=(0,),
    )

    def fetch(ref, part):
        rows = []
        for k in range(NPTS):
            for at in range(0, block, NPTS * NPTS):
                own = pl.ds(part * block + at + k, NPTS, NPTS)
                tiles = []
                for first in range(0, sources, 128):
                    where = slice(first, first + 128)
                    found = jnp.zeros((8, 128), F32)
                    for n in range(parts):
                        taken = lax.gather(
                            ref[n, own, :],
                            spot[:, where][..., None],
                            lookup,
                            slice_sizes=(1, 1),
                            mode=lax.GatherScatterMode.PROMISE_IN_BOUNDS,
                        )
                        found = jnp.where(piece[:, where] == n, taken, found)
                    tiles.append(found)
                rows.append(tiles[0] if len(tiles) == 1 else jnp.concatenate(tiles, axis=1))
        return jnp.concatenate(rows, axis=0)

    edge = float(WEIGHTS[0])
    chosen = None
    along_k, along_j, plane_u, plane_g = [], [], [], []
    for part in range(blocks):
        if part % 2 == 0:
            loaded(part)
            loaded(part + 1)
        u_part, k_part = fetch(u_ref, part), pick(k_ref, part)
        if chosen is None:
            chosen = dot(jnp.broadcast_to(scale, (16, elems)).astype(BF16), hot_src)[0:8]
            chosen = chosen * quad8
        wide = block // NPTS
        for i in range(part * wide // NPTS, (part + 1) * wide // NPTS):
            at = i * NPTS - part * wide

            def strip(values, k):
                return values[k * wide + at : k * wide + at + NPTS]

            here = chosen * float(WEIGHTS[i])
            flat = jnp.where(on_low, strip(u_part, 0), strip(u_part, last))
            g = jnp.where(on_low, strip(k_part, 0), strip(k_part, last)) * (here * edge)
            plane_u.append(flat)
            plane_g.append(g)
            along_j.append(turn(back8, turn(forth8, flat) * g))
            deep = line([strip(u_part, k) for k in range(NPTS)], DERIV)
            total = reach[0] * strip(k_part, 0) * deep[0]
            for c in range(1, NPTS):
                total += reach[c] * strip(k_part, c) * deep[c]
            along_k.append(total * here)
    fold = [
        fold_ref[i : i + 1, :] * fold_ref[NPTS : 2 * NPTS, :] for i in range(NPTS)
    ]
    fold_high, fold_low = halves_of(jnp.concatenate(fold, axis=0))
    across_i = line(plane_u, DERIV)
    along_i = line([across_i[i] * plane_g[i] for i in range(NPTS)], DERIV.T)
    summed = [along_i[i] + (along_j[i] + along_k[i]) for i in range(NPTS)]
    own = jnp.concatenate(summed + summed, axis=0).T

    def folded(rows, first, width):
        high, low = halves_of(rows)
        cols = slice(first, first + width)
        both = dot(jnp.concatenate([high, low], axis=0), fold_high[:, cols])
        return both[0 : rows.shape[0]] + both[rows.shape[0] :] + dot(high, fold_low[:, cols])

    raised = folded(own[coarse_at : coarse_at + up(coarsep, 16), 0:square], 256, 256)
    kids = folded(own[kids_at:used, 0:square], 0, 256)

    half = lax.broadcasted_iota(I32, (8, 128), 1) < square
    for side in range(2):
        for first in range(0, farp, 8):
            faces = own[side * farp + first : side * farp + first + 8]
            far_out[side, first : first + 8] = jnp.where(half, faces, pltpu.roll(faces, 6, 0))
    half_g = lax.broadcasted_iota(I32, (groupp, 128), 1) < square
    kid = [kids[m * groupp : (m + 1) * groupp] for m in range(4)]
    projected = jnp.where(half_g, kid[0][:, 0:128], kid[1][:, 0:128]) + jnp.where(
        half_g, kid[2][:, 128:256], kid[3][:, 128:256]
    )
    peer_row = lax.broadcasted_iota(I32, (n_dom, 128), 0)
    routed = jnp.zeros((n_dom, 128), F32)
    for slot in range(groups):
        routed = jnp.where(peer_row == peer_ref[slot], projected[slot : slot + 1], routed)
    mort_out[pl.ds(0, n_dom, 8), :] = routed
    mort_out[pl.ds(1, n_dom, 8), :] = raised[0:n_dom, 0:128]
    mort_out[pl.ds(2, n_dom, 8), :] = raised[0:n_dom, 128:256]

    greeted = n_dom - 1 + (sub > 0).astype(I32) + (sub < n_sub - 1).astype(I32)

    def mail(step, landing):
        other = lax.rem(me + step, n_dom)
        return pltpu.make_async_remote_copy(
            src_ref=mort_out.at[pl.ds(pl.multiple_of(other * 8, 8), 3)],
            dst_ref=mort_in.at[
                pl.ds(pl.multiple_of((other if landing else me) * 8, 8), 3)
            ],
            send_sem=mort_send.at[other],
            recv_sem=mort_recv.at[other if landing else me],
            device_id=(other, sub),
            device_id_type=MESH,
        )

    def far_copy(side, s, landing):
        other = me - s - 2 if side == 0 else me + s + 2
        rows = pl.ds(s * FAR, FAR // 2)
        there = side if landing else 1 - side
        return pltpu.make_async_remote_copy(
            src_ref=far_out.at[side, rows],
            dst_ref=far_in.at[there, rows],
            send_sem=far_send.at[side, s],
            recv_sem=far_recv.at[there, s],
            device_id=(other, sub),
            device_id_type=MESH,
        )

    def far_there(side, s):
        return me >= s + 2 if side == 0 else me + s + 2 < n_dom

    def send_messages():
        pl.semaphore_wait(barrier, greeted)

        def start_all(step, carry):
            mail(step, False).start()
            return carry

        lax.fori_loop(1, n_dom, start_all, 0, unroll=n_dom <= 8)
        for side in range(2):
            for s in range(shifts):
                @pl.when(far_there(side, s))
                def _():
                    far_copy(side, s, False).start()

    early = me < 3

    @pl.when(jnp.logical_not(early))
    def _():
        send_messages()

    for copy in small[6:]:
        copy.wait()

    hot0l = hot_rows([column(local_ref[1:2], up(pairs))], 0, elems)
    hot1l = hot_rows([column(local_ref[0:1], up(pairs))], elems, elems)
    hot0s = hot_rows([column(sub_ref[0:1], up(rim))], 0, elems)
    hot1s = hot_rows([column(sub_ref[1:2], up(rim))], elems, elems)
    hot2 = hot_rows([column(near_ref[0:1], up(near))], 2 * elems, elems)
    hot3 = hot_rows([column(near_ref[1:2], up(near))], 3 * elems, elems)

    sub8 = lax.broadcasted_iota(I32, (8, elems), 0)
    weight = jnp.zeros((8, elems), F32)
    for k in range(NPTS):
        weight = jnp.where(sub8 == k, float(WEIGHTS[k]), weight)
    weight = weight * scale

    def slab(i, j):
        return pl.ds((i * NPTS + j) * NPTS, NPTS)

    def across(ref, own):
        return jnp.concatenate([ref[n, own, :] for n in range(parts)], axis=1)

    def spot_of(n, i, j):
        return pl.ds(((i * NPTS + j) * parts + n) * NPTS, NPTS)

    def face_of(tiles):
        return jnp.concatenate(
            [
                jnp.concatenate([w_ref[spot_of(n, i, j), :] for i, j in tiles], axis=0)
                for n in range(parts)
            ],
            axis=1,
        )

    def add_tiles(tiles, values):
        for t, (i, j) in enumerate(tiles):
            for n in range(parts):
                w_ref[spot_of(n, i, j), :] += values[
                    t * NPTS : (t + 1) * NPTS, n * 128 : (n + 1) * 128
                ]

    def add_level(k, values):
        for n in range(parts):
            own_rows = pl.ds(n * NPTS + k, square, parts * NPTS)
            w_ref[own_rows, :] += values[:, n * 128 : (n + 1) * 128]

    turns = [deriv_ref[128 * n : 128 * n + 128, :] for n in range(4)]

    def along(pair, values):
        high, low = halves_of(values)
        both = jnp.concatenate([high, low], axis=0)
        return dot(jnp.concatenate([pair[0], pair[0]], axis=1), both) + dot(pair[1], high)

    for n in range(parts):
        here = weight[:, n * 128 : (n + 1) * 128]
        for i in range(NPTS):
            for j in range(NPTS):
                g_ref[n, slab(i, j), :] = k_ref[n, slab(i, j), :] * (
                    here * float(WEIGHTS[i] * WEIGHTS[j])
                )
    for part in range(blocks):
        own_rows = pl.ds(part * block, block)
        turn = along(turns[0:2], across(u_ref, own_rows)) * across(g_ref, own_rows)
        turn = along(turns[2:4], turn)
        for t in range(block // NPTS):
            i, j = divmod(part * block // NPTS + t, NPTS)
            for n in range(parts):
                w_ref[spot_of(n, i, j), :] = turn[
                    t * NPTS : (t + 1) * NPTS, n * 128 : (n + 1) * 128
                ]
    for n in range(parts):
        for j in range(NPTS):
            turn = line([u_ref[n, slab(i, j), :] for i in range(NPTS)], DERIV)
            turn = [turn[i] * g_ref[n, slab(i, j), :] for i in range(NPTS)]
            turn = line(turn, DERIV.T)
            for i in range(NPTS):
                w_ref[spot_of(n, i, j), :] += turn[i]
        for i in range(NPTS):
            turn = line([u_ref[n, slab(i, j), :] for j in range(NPTS)], DERIV)
            turn = [turn[j] * g_ref[n, slab(i, j), :] for j in range(NPTS)]
            turn = line(turn, DERIV.T)
            for j in range(NPTS):
                w_ref[spot_of(n, i, j), :] += turn[j]

    low_i, high_i = ([(i, j) for j in range(NPTS)] for i in (0, last))
    low_j, high_j = ([(i, j) for i in range(NPTS)] for j in (0, last))
    face0, face1, face2, face3 = (face_of(tiles) for tiles in (low_i, high_i, low_j, high_j))
    side_out[0, 0:rim, 0:square] = take_rows(hot0s, face0)[0:rim]
    side_out[1, 0:rim, 0:square] = take_rows(hot1s, face1)[0:rim]
    side_out[2, 0:near, 0:square] = take_rows(hot2, face2)[0:near]
    side_out[3, 0:near, 0:square] = take_rows(hot3, face3)[0:near]

    @pl.when(early)
    def _():
        send_messages()

    sides = [
        (sub > 0, 0, 1, (me, sub - 1)),
        (sub < n_sub - 1, 1, 0, (me, sub + 1)),
        (me > 0, 2, 3, (me - 1, sub)),
        (me < n_dom - 1, 3, 2, (me + 1, sub)),
    ]

    def side_copy(mine, theirs, device):
        return pltpu.make_async_remote_copy(
            src_ref=side_out.at[mine],
            dst_ref=side_in.at[theirs],
            send_sem=side_send.at[mine],
            recv_sem=side_recv.at[theirs],
            device_id=device,
            device_id_type=MESH,
        )

    for there, mine, theirs, device in sides:
        @pl.when(there)
        def _():
            side_copy(mine, theirs, device).start()

    keyed = up(2 * farp + 8 * n_dom, 128)

    def landing_rows(keys):
        at = lax.broadcasted_iota(I32, (2 * keyed, sources), 0)
        hit = at == keys[0]
        for key in keys[1:]:
            hit = hit | (at == key)
        return dot(jnp.where(hit, 1.0, 0.0).astype(BF16), hot_src, over).astype(BF16)

    src = lax.broadcasted_iota(I32, (1, sources), 1)

    def far_key(first):
        f = src - first
        s, j = lax.shift_right_logical(f, 2), lax.bitwise_and(f, FAR - 1)
        key = lax.shift_right_logical(j, 1) * keyed + first + 4 * s + lax.bitwise_and(j, 1)
        return jnp.where((f >= 0) & (f < far), key, -1)

    key4 = far_key(0)
    for m in range(4):
        for slot in range(groups):
            key = (m & 1) * keyed + 2 * farp + peer_ref[slot] * 8 + 1 + (m >> 1)
            key4 = jnp.where(src == kids_at + m * groupp + slot, key, key4)
    key5 = far_key(farp)
    p = src - coarse_at
    holds = (p >= 0) & (p < n_dom)
    key5 = jnp.where(holds, 2 * farp + 8 * p, key5)
    land_ref[0] = landing_rows([key4])
    land_ref[1] = landing_rows([key5, jnp.where(holds, keyed + 2 * farp + 8 * p, -1)])

    joined = projected[:, 0:square] + projected[:, square:]
    lift = [mortar_ref[m * square : (m + 1) * square, :] for m in range(4)]
    share = []
    for m in range(4):
        first = kids_at + m * groupp
        share.append(product(joined, lift[m]) - own[first : first + groupp, 0:square])
    share = [jnp.zeros((kids_at, square), F32)] + share
    if sources > used:
        share.append(jnp.zeros((sources - used, square), F32))
    high, low = halves_of(jnp.concatenate(share, axis=0).T)
    add_level(0, dot(high, hot_src, over) + dot(low, hot_src, over))
    add_tiles(low_i, spread_rows(take_rows(hot1l, face1), hot0l))
    add_tiles(high_i, spread_rows(take_rows(hot0l, face0), hot1l))

    for there, mine, theirs, device in sides:
        @pl.when(there)
        def _():
            side_copy(mine, mine, device).wait()

    add_tiles(low_i, spread_rows(side_in[0, 0:rim, 0:square], hot0s))
    add_tiles(high_i, spread_rows(side_in[1, 0:rim, 0:square], hot1s))
    add2 = spread_rows(side_in[2, 0:near, 0:square], hot2)
    add3 = spread_rows(side_in[3, 0:near, 0:square], hot3)
    add_tiles(low_j, add2)
    add_tiles(high_j, add3)

    def sent_all(step, carry):
        mail(step, True).wait_send()
        return carry

    lax.fori_loop(1, n_dom, sent_all, 0, unroll=n_dom <= 8)
    for side in range(2):
        for s in range(shifts):
            @pl.when(far_there(side, s))
            def _():
                far_copy(side, s, True).wait()

    def wait_all(step, carry):
        mail(step, True).wait_recv()
        return carry

    lax.fori_loop(1, n_dom, wait_all, 0, unroll=n_dom <= 8)

    arrived_ref[0:farp] = far_in[0]
    arrived_ref[farp : 2 * farp] = far_in[1]
    arrived_ref[2 * farp :] = mort_in[...]


def kernel(sizes, semaphores, *refs):
    pl.run_scoped(
        functools.partial(steps, sizes, *refs),
        *[pltpu.SemaphoreType.DMA(shape) for shape in semaphores],
    )


def finish(w_ref, arrived_ref, land_ref, out_hbm, ends_ref):
    def run(sem):
        square = NPTS * NPTS
        tiles, parts = w_ref.shape[0] // NPTS, w_ref.shape[0] // NPTS // square
        inner = pltpu.make_async_copy(
            w_ref.reshape(tiles, NPTS, 128).at[:, 1 : NPTS - 1],
            out_hbm.reshape(tiles, NPTS, 128).at[:, 1 : NPTS - 1],
            sem.at[2 * parts],
        )
        inner.start()
        received = arrived_ref[...]
        spare = land_ref.shape[1] // 2 - received.shape[0]
        if spare:
            received = jnp.concatenate([received, jnp.zeros((spare, 128), F32)], axis=0)
        received = received.T
        received = jnp.concatenate([received[0:square], received[square:]], axis=1)
        both = jnp.concatenate(halves_of(received), axis=0)
        rim = out_hbm.reshape(square, parts, NPTS, 128)
        copies = [inner]
        for side, k in enumerate((0, NPTS - 1)):
            added = dot(both, land_ref[side])
            added = added[0:square] + added[square:]
            for n in range(parts):
                rows = w_ref[pl.ds(n * NPTS + k, square, parts * NPTS), :]
                ends_ref[side, n] = rows + added[:, n * 128 : (n + 1) * 128]
                copy = pltpu.make_async_copy(
                    ends_ref.at[side, n], rim.at[:, n, k], sem.at[side * parts + n]
                )
                copies.append(copy)
        for copy in copies[1:]:
            copy.start()
        for copy in copies:
            copy.wait()

    pl.run_scoped(run, pltpu.SemaphoreType.DMA((2 * w_ref.shape[0] // NPTS**3 + 1,)))


def body(
    sizes,
    nodal_values,
    kappa,
    levels,
    local_faces,
    sub_faces,
    near_faces,
    far_faces,
    child_faces,
    child_peer,
    coarse_faces,
):
    n_dom, n_sub = sizes
    elems = nodal_values.shape[1]
    krons = [np.kron(HALVES[m // 2], HALVES[m % 2]) for m in range(4)]
    mortar = np.concatenate([m.T for m in krons], axis=0)
    far_rows = up(far_faces.shape[1])
    held = (elems // 128, NPTS**3, 128)
    side_rows = up(max(sub_faces.shape[1], near_faces.shape[1]))
    small = [
        levels.reshape(1, elems),
        local_faces,
        sub_faces,
        near_faces,
        jnp.asarray(folds(), F32),
        jnp.asarray(stencils(), BF16),
        jnp.asarray(mortar, F32),
    ]
    tables = [far_faces, child_faces, child_peer, coarse_faces]
    far_slots = (2, far_faces.shape[1] // FAR)
    semaphores = [(len(small) + len(tables),), (NPTS**3 // 128,), (4,), (4,)]
    semaphores += [far_slots, far_slots, (n_dom,), (n_dom,)]
    hbm = pl.BlockSpec(memory_space=pltpu.HBM)
    vmem = pl.BlockSpec(memory_space=pltpu.VMEM)
    arrivals = 2 * far_rows + 8 * n_dom
    parts = pl.pallas_call(
        functools.partial(kernel, sizes, semaphores),
        out_shape=[
            pltpu.VMEM((held[0] * held[1], 128), F32),
            pltpu.VMEM((arrivals, 128), F32),
            pltpu.VMEM((2, 2 * up(arrivals, 128), elems), BF16),
        ],
        in_specs=[hbm] * 13,
        out_specs=[vmem] * 3,
        scratch_shapes=[pltpu.VMEM(item.shape, item.dtype) for item in small]
        + [pltpu.SMEM(item.shape, I32) for item in tables]
        + [
            pltpu.VMEM((2, *held), F32),
            pltpu.VMEM(held, F32),
            pltpu.VMEM((4, side_rows, 128), F32),
            pltpu.VMEM((4, side_rows, 128), F32),
            pltpu.VMEM((2, far_rows, 128), F32),
            pltpu.VMEM((2, far_rows, 128), F32),
            pltpu.VMEM((n_dom * 8, 128), F32),
            pltpu.VMEM((n_dom * 8, 128), F32),
        ],
        compiler_params=pltpu.CompilerParams(
            collective_id=0, has_side_effects=True, vmem_limit_bytes=60 * 1024 * 1024
        ),
    )(
        nodal_values,
        kappa,
        *small,
        *tables,
    )
    applied = pl.pallas_call(
        finish,
        out_shape=jax.ShapeDtypeStruct((held[0] * held[1], 128), F32),
        in_specs=[vmem] * 3,
        out_specs=hbm,
        scratch_shapes=[pltpu.VMEM((2, held[0], NPTS * NPTS, 128), F32)],
    )(*[pltpu.with_memory_space_constraint(item, pltpu.VMEM) for item in parts])
    applied = applied.reshape(NPTS * NPTS, held[0], NPTS, 128).transpose(0, 2, 1, 3)
    return applied.reshape(nodal_values.shape)


def solution(mesh):
    sizes = (mesh.shape["dom"], mesh.shape["sub"])
    wide = P(None, ("dom", "sub"))
    flat = P(("dom", "sub"))
    in_specs = (wide, wide, flat, wide, wide, wide, wide, wide, flat, flat)
    return jax.shard_map(
        functools.partial(body, sizes),
        mesh=mesh,
        in_specs=in_specs,
        out_specs=wide,
        check_vma=False,
    )
```

```python
import functools

import jax
import jax.numpy as jnp
import numpy as np
from jax import lax
from jax.experimental import pallas as pl
from jax.experimental.pallas import tpu as pltpu
from jax.sharding import PartitionSpec as P

NPTS = 8
FAR = 4
MESH = pl.DeviceIdType.MESH
F32, BF16, I32 = jnp.float32, jnp.bfloat16, jnp.int32


def legendre_table(points, degree):
    table = [np.ones(points.shape), points.copy()]
    for order in range(2, degree + 1):
        table.append(
            ((2 * order - 1) * points * table[order - 1] - (order - 1) * table[order - 2]) / order
        )
    return table


def lobatto_points(degree):
    points = np.cos(np.pi * np.arange(degree + 1) / degree)
    for sweep in range(100):
        table = legendre_table(points, degree)
        points = points - (points * table[degree] - table[degree - 1]) / (
            (degree + 1) * table[degree]
        )
    points = np.sort(points)
    return (points, legendre_table(points, degree)[degree])


def node_tables(count):
    degree = count - 1
    points, legendre = lobatto_points(degree)
    weights = 2.0 / (degree * (degree + 1) * legendre**2)
    spread = points[:, None] - points[None, :] + np.eye(count)
    derivative = legendre[:, None] / (legendre[None, :] * spread) * (1.0 - np.eye(count))
    derivative[0, 0] = -degree * (degree + 1) / 4.0
    derivative[degree, degree] = degree * (degree + 1) / 4.0
    halves = []
    for side in range(2):
        target = (points + 2.0 * side - 1.0) / 2.0
        matrix = np.ones((count, count))
        for column in range(count):
            for other in range(count):
                if other != column:
                    matrix[:, column] = (
                        matrix[:, column]
                        * (target - points[other])
                        / (points[column] - points[other])
                    )
        halves.append(matrix)
    return (points, weights, derivative, np.stack(halves))


POINTS, WEIGHTS, DERIV, HALVES = node_tables(NPTS)


def up(count, unit=8):
    return -(-count // unit) * unit


def halves_of(values):
    high = values.astype(BF16)
    return high, (values - high.astype(F32)).astype(BF16)


def numpy_halves(matrix):
    matrix = np.asarray(matrix, np.float32)
    high = matrix.astype(jnp.bfloat16)
    low = (matrix - high.astype(np.float32)).astype(jnp.bfloat16)
    return high, low


def dot(a, b, dims=((1,), (0,))):
    return lax.dot_general(a, b, (dims, ((), ())), preferred_element_type=F32)


def select(hot, values):
    high, low = halves_of(values)
    return dot(hot, high) + dot(hot, low)


def take_rows(hot, face):
    high, low = halves_of(face)
    dims = ((1,), (1,))
    return dot(hot, high, dims) + dot(hot, low, dims)


def spread_rows(rows, hot):
    high, low = halves_of(rows.T)
    return dot(high, hot) + dot(low, hot)


def product(a, matrix):
    high, low = halves_of(a)
    mhigh, mlow = halves_of(matrix)
    return dot(high, mhigh) + dot(low, mhigh) + dot(high, mlow)


def column(row, padded):
    count = row.shape[1]
    r = lax.broadcasted_iota(I32, (padded, count), 0)
    c = lax.broadcasted_iota(I32, (padded, count), 1)
    spread = jnp.where(r == c, jnp.broadcast_to(row.astype(F32), (padded, count)), 0.0)
    col = jnp.sum(spread, axis=1, keepdims=True)
    inside = lax.broadcasted_iota(I32, (padded, 1), 0) < count
    return jnp.where(inside, col, -1.0)


def hot_rows(columns, base, elems, kind=BF16):
    col = columns[0] if len(columns) == 1 else jnp.concatenate(columns, axis=0)
    lane = lax.broadcasted_iota(I32, (col.shape[0], elems), 1).astype(F32)
    return jnp.where(lane == col - float(base), 1.0, 0.0).astype(kind)


def line(values, matrix):
    half = NPTS // 2
    even = [values[i] + values[NPTS - 1 - i] for i in range(half)]
    odd = [values[i] - values[NPTS - 1 - i] for i in range(half)]
    out = [None] * NPTS
    for a in range(half):
        p = q = None
        for i in range(half):
            s = float((matrix[a, i] + matrix[a, NPTS - 1 - i]) / 2)
            t = float((matrix[a, i] - matrix[a, NPTS - 1 - i]) / 2)
            p = even[i] * s if p is None else p + even[i] * s
            q = odd[i] * t if q is None else q + odd[i] * t
        out[a] = q + p
        out[NPTS - 1 - a] = q - p
    return out


def stencils():
    forth, back = np.kron(np.eye(16), DERIV), np.kron(np.eye(16), DERIV.T)
    pieces = [piece for table in (forth, back) for piece in numpy_halves(table)]
    return np.concatenate(pieces, axis=0)


def places(n_dom, far, groups):
    farp, groupp, coarsep = up(far), up(groups), up(n_dom)
    coarse_at = 2 * farp
    kids_at = coarse_at + 4 * coarsep
    raw_at = kids_at + 4 * groupp
    return farp, groupp, coarsep, coarse_at, kids_at, raw_at, raw_at + 4 * groupp


def transforms(n_dom, far, groups):
    farp, groupp, coarsep, coarse_at, kids_at, raw_at, used = places(n_dom, far, groups)
    eye = np.eye(NPTS)[:, :, None]
    first = np.repeat(eye, up(used, 128), axis=2)
    second = first.copy()
    for m in range(4):
        own = slice(coarse_at + m * coarsep, coarse_at + (m + 1) * coarsep)
        first[:, :, own] = HALVES[m // 2][:, :, None]
        second[:, :, own] = HALVES[m % 2][:, :, None]
        own = slice(kids_at + m * groupp, kids_at + (m + 1) * groupp)
        first[:, :, own] = HALVES[m // 2].T[:, :, None]
        second[:, :, own] = HALVES[m % 2].T[:, :, None]
    rows = [first[o, i] for o in range(NPTS) for i in range(NPTS)]
    rows += [second[b, (b + r) % NPTS] for r in range(NPTS) for b in range(NPTS)]
    return np.stack(rows).astype(np.float32)


def steps(
    sizes,
    u_hbm,
    kappa_hbm,
    level_hbm,
    local_hbm,
    sub_hbm,
    near_hbm,
    fold_hbm,
    deriv_hbm,
    mortar_hbm,
    far_hbm,
    child_hbm,
    peer_hbm,
    coarse_hbm,
    w_ref,
    arrived_ref,
    land_ref,
    level_ref,
    local_ref,
    sub_ref,
    near_ref,
    fold_ref,
    deriv_ref,
    mortar_ref,
    far_ref,
    child_ref,
    peer_ref,
    coarse_ref,
    uk_ref,
    g_ref,
    side_out,
    side_in,
    far_out,
    far_in,
    mort_out,
    mort_in,
    small_sem,
    load_sem,
    side_send,
    side_recv,
    far_send,
    far_recv,
    mort_send,
    mort_recv,
):
    n_dom, n_sub = sizes
    u_ref, k_ref = uk_ref.at[0], uk_ref.at[1]
    parts = u_ref.shape[0]
    elems = parts * 128
    square = NPTS * NPTS
    last = NPTS - 1
    me, sub = lax.axis_index("dom"), lax.axis_index("sub")

    urgent = [
        (fold_hbm, fold_ref),
        (far_hbm, far_ref),
        (child_hbm, child_ref),
        (coarse_hbm, coarse_ref),
        (level_hbm, level_ref),
        (peer_hbm, peer_ref),
    ]
    later = [
        (local_hbm, local_ref),
        (sub_hbm, sub_ref),
        (near_hbm, near_ref),
        (deriv_hbm, deriv_ref),
        (mortar_hbm, mortar_ref),
    ]
    small = [
        pltpu.make_async_copy(source, target, small_sem.at[slot])
        for slot, (source, target) in enumerate(urgent + later)
    ]
    block = 128
    blocks = NPTS**3 // block

    def load(n, part, source, target):
        own = pl.ds(part * block, block)
        return pltpu.make_async_copy(
            source.at[own, pl.ds(n * 128, 128)], target.at[n, own], load_sem.at[part]
        )

    def loaded(part):
        whole = uk_ref.at[0, :, pl.ds(0, 2 * block)]
        pltpu.make_async_copy(whole, whole, load_sem.at[part]).wait()

    for copy in small[:6]:
        copy.start()
    for part in range(blocks):
        for n in range(parts):
            load(n, part, u_hbm, u_ref).start()
            load(n, part, kappa_hbm, k_ref).start()
    for copy in small[6:]:
        copy.start()

    far_in[...] = jnp.zeros(far_in.shape, F32)
    mort_in[...] = jnp.zeros(mort_in.shape, F32)

    barrier = pltpu.get_barrier_semaphore()

    def greet(step, carry):
        other = lax.rem(me + step, n_dom)
        pl.semaphore_signal(barrier, inc=1, device_id=(other, sub), device_id_type=MESH)
        return carry

    lax.fori_loop(1, n_dom, greet, 0, unroll=n_dom <= 8)

    @pl.when(sub > 0)
    def _():
        pl.semaphore_signal(barrier, inc=1, device_id=(me, sub - 1), device_id_type=MESH)

    @pl.when(sub < n_sub - 1)
    def _():
        pl.semaphore_signal(barrier, inc=1, device_id=(me, sub + 1), device_id_type=MESH)

    def clear(missing, slot):
        @pl.when(missing)
        def _():
            side_in[slot] = jnp.zeros(side_in.shape[1:], F32)

    clear(sub == 0, 0)
    clear(sub == n_sub - 1, 1)
    clear(me == 0, 2)
    clear(me == n_dom - 1, 3)

    pairs, rim, near = local_ref.shape[1], sub_ref.shape[1], near_ref.shape[1]
    far, groups = far_ref.shape[1], child_ref.shape[1]
    shifts = far // FAR
    farp, groupp, coarsep, coarse_at, kids_at, raw_at, used = places(n_dom, far, groups)
    sources = up(used, 128)
    lane = lax.broadcasted_iota(I32, (8, sources), 1)
    named = lane
    for m in range(1, 4):
        again = (lane >= coarse_at + m * coarsep) & (lane < coarse_at + (m + 1) * coarsep)
        named = jnp.where(again, lane - m * coarsep, named)
    named = jnp.where(lane >= raw_at, lane - (raw_at - kids_at), named)
    row8 = lax.broadcasted_iota(I32, (8, sources), 0)
    on_low = (lane < farp) | (lane >= kids_at)
    reach = [
        jnp.where(on_low, float(WEIGHTS[c] * DERIV[c, 0]), float(WEIGHTS[c] * DERIV[c, last]))
        for c in range(NPTS)
    ]

    def shifted(matrix):
        tables = []
        for r in range(NPTS):
            table = jnp.zeros((8, sources), F32)
            for b in range(NPTS):
                table = jnp.where(row8 == b, float(matrix[b, (b + r) % NPTS]), table)
            tables.append(table)
        return tables

    def turn(tables, values):
        total = tables[0] * values
        for r in range(1, NPTS):
            total += tables[r] * pltpu.roll(values, NPTS - r, 0)
        return total

    forth8, back8 = shifted(DERIV), shifted(DERIV.T)
    quad8 = jnp.zeros((8, sources), F32)
    for k in range(NPTS):
        quad8 = jnp.where(row8 == k, float(WEIGHTS[k]), quad8)

    for copy in small[:6]:
        copy.wait()

    def held(first, ids, base):
        total = jnp.zeros((8, sources), I32)
        for slot, value in enumerate(ids):
            total = jnp.where(named == first + slot, value + (1 - base * elems), total)
        return total

    ids = held(0, [far_ref[0, c] for c in range(far)], 4)
    ids += held(farp, [far_ref[1, c] for c in range(far)], 5)
    ids += held(coarse_at, [coarse_ref[c] for c in range(n_dom)], 5)
    for m in range(4):
        ids += held(kids_at + m * groupp, [child_ref[m, c] for c in range(groups)], 4)
    element = lax.broadcasted_iota(I32, (elems, sources), 0) + 1
    hot_src = jnp.where(element == ids[0:1], 1.0, 0.0).astype(BF16)
    scale = jnp.exp2(-level_ref[...].astype(F32))
    over = ((1,), (1,))

    def pick(ref, part):
        rows = []
        for k in range(NPTS):
            own = pl.ds(part * block + k, block // NPTS, NPTS)
            rows.append(jnp.concatenate([ref[n, own, :] for n in range(parts)], axis=1))
        high, low = halves_of(jnp.concatenate(rows, axis=0))
        both = dot(jnp.concatenate([high, low], axis=0), hot_src)
        return both[0:block] + both[block:]

    spot = jnp.bitwise_and(ids - 1, 127)
    piece = lax.shift_right_arithmetic(ids - 1, 7)
    lookup = lax.GatherDimensionNumbers(
        offset_dims=(),
        collapsed_slice_dims=(1,),
        start_index_map=(1,),
        operand_batching_dims=(0,),
        start_indices_batching_dims=(0,),
    )

    def fetch(ref, part):
        rows = []
        for k in range(NPTS):
            for at in range(0, block, NPTS * NPTS):
                own = pl.ds(part * block + at + k, NPTS, NPTS)
                tiles = []
                for first in range(0, sources, 128):
                    where = slice(first, first + 128)
                    found = jnp.zeros((8, 128), F32)
                    for n in range(parts):
                        taken = lax.gather(
                            ref[n, own, :],
                            spot[:, where][..., None],
                            lookup,
                            slice_sizes=(1, 1),
                            mode=lax.GatherScatterMode.PROMISE_IN_BOUNDS,
                        )
                        found = jnp.where(piece[:, where] == n, taken, found)
                    tiles.append(found)
                rows.append(tiles[0] if len(tiles) == 1 else jnp.concatenate(tiles, axis=1))
        return jnp.concatenate(rows, axis=0)

    edge = float(WEIGHTS[0])
    chosen = None
    along_k, along_j, plane_u, plane_g = [], [], [], []
    for part in range(blocks):
        if part % 2 == 0:
            loaded(part)
            loaded(part + 1)
        u_part, k_part = fetch(u_ref, part), pick(k_ref, part)
        if chosen is None:
            chosen = dot(jnp.broadcast_to(scale, (16, elems)).astype(BF16), hot_src)[0:8]
            chosen = chosen * quad8
        wide = block // NPTS
        for i in range(part * wide // NPTS, (part + 1) * wide // NPTS):
            at = i * NPTS - part * wide

            def strip(values, k):
                return values[k * wide + at : k * wide + at + NPTS]

            here = chosen * float(WEIGHTS[i])
            flat = jnp.where(on_low, strip(u_part, 0), strip(u_part, last))
            g = jnp.where(on_low, strip(k_part, 0), strip(k_part, last)) * (here * edge)
            plane_u.append(flat)
            plane_g.append(g)
            along_j.append(turn(back8, turn(forth8, flat) * g))
            deep = line([strip(u_part, k) for k in range(NPTS)], DERIV)
            total = reach[0] * strip(k_part, 0) * deep[0]
            for c in range(1, NPTS):
                total += reach[c] * strip(k_part, c) * deep[c]
            along_k.append(total * here)
    across_i = line(plane_u, DERIV)
    along_i = line([across_i[i] * plane_g[i] for i in range(NPTS)], DERIV.T)
    summed = [along_i[i] + (along_j[i] + along_k[i]) for i in range(NPTS)]
    cross8 = [fold_ref[square + r * NPTS : square + (r + 1) * NPTS, :] for r in range(NPTS)]
    moved = []
    for o in range(NPTS):
        total = fold_ref[o * NPTS : o * NPTS + 1, :] * summed[0]
        for i in range(1, NPTS):
            total += fold_ref[o * NPTS + i : o * NPTS + i + 1, :] * summed[i]
        moved.append(turn(cross8, total))
    summed = moved
    own = jnp.concatenate(summed + summed, axis=0).T

    half = lax.broadcasted_iota(I32, (8, 128), 1) < square
    for side in range(2):
        for first in range(0, farp, 8):
            faces = own[side * farp + first : side * farp + first + 8]
            far_out[side, first : first + 8] = jnp.where(half, faces, pltpu.roll(faces, 6, 0))
    half_g = lax.broadcasted_iota(I32, (groupp, 128), 1) < square
    kid = [own[kids_at + m * groupp : kids_at + (m + 1) * groupp] for m in range(4)]
    projected = jnp.where(half_g, kid[0], kid[1]) + jnp.where(half_g, kid[2], kid[3])
    half_c = lax.broadcasted_iota(I32, (coarsep, 128), 1) < square
    raised = [own[coarse_at + m * coarsep : coarse_at + (m + 1) * coarsep] for m in range(4)]
    raised = [jnp.where(half_c, raised[m], raised[m + 1]) for m in (0, 2)]
    peer_row = lax.broadcasted_iota(I32, (n_dom, 128), 0)
    routed = jnp.zeros((n_dom, 128), F32)
    for slot in range(groups):
        routed = jnp.where(peer_row == peer_ref[slot], projected[slot : slot + 1], routed)
    mort_out[pl.ds(0, n_dom, 8), :] = routed
    mort_out[pl.ds(1, n_dom, 8), :] = raised[0][0:n_dom]
    mort_out[pl.ds(2, n_dom, 8), :] = raised[1][0:n_dom]

    greeted = n_dom - 1 + (sub > 0).astype(I32) + (sub < n_sub - 1).astype(I32)

    def mail(step, landing):
        other = lax.rem(me + step, n_dom)
        return pltpu.make_async_remote_copy(
            src_ref=mort_out.at[pl.ds(pl.multiple_of(other * 8, 8), 3)],
            dst_ref=mort_in.at[
                pl.ds(pl.multiple_of((other if landing else me) * 8, 8), 3)
            ],
            send_sem=mort_send.at[other],
            recv_sem=mort_recv.at[other if landing else me],
            device_id=(other, sub),
            device_id_type=MESH,
        )

    def far_copy(side, s, landing):
        other = me - s - 2 if side == 0 else me + s + 2
        rows = pl.ds(s * FAR, FAR // 2)
        there = side if landing else 1 - side
        return pltpu.make_async_remote_copy(
            src_ref=far_out.at[side, rows],
            dst_ref=far_in.at[there, rows],
            send_sem=far_send.at[side, s],
            recv_sem=far_recv.at[there, s],
            device_id=(other, sub),
            device_id_type=MESH,
        )

    def far_there(side, s):
        return me >= s + 2 if side == 0 else me + s + 2 < n_dom

    def send_messages():
        pl.semaphore_wait(barrier, greeted)

        def start_all(step, carry):
            mail(step, False).start()
            return carry

        lax.fori_loop(1, n_dom, start_all, 0, unroll=n_dom <= 8)
        for side in range(2):
            for s in range(shifts):
                @pl.when(far_there(side, s))
                def _():
                    far_copy(side, s, False).start()

    early = me < 3

    @pl.when(jnp.logical_not(early))
    def _():
        send_messages()

    for copy in small[6:]:
        copy.wait()

    hot0l = hot_rows([column(local_ref[1:2], up(pairs))], 0, elems)
    hot1l = hot_rows([column(local_ref[0:1], up(pairs))], elems, elems)
    hot0s = hot_rows([column(sub_ref[0:1], up(rim))], 0, elems)
    hot1s = hot_rows([column(sub_ref[1:2], up(rim))], elems, elems)
    hot2 = hot_rows([column(near_ref[0:1], up(near))], 2 * elems, elems)
    hot3 = hot_rows([column(near_ref[1:2], up(near))], 3 * elems, elems)

    sub8 = lax.broadcasted_iota(I32, (8, elems), 0)
    weight = jnp.zeros((8, elems), F32)
    for k in range(NPTS):
        weight = jnp.where(sub8 == k, float(WEIGHTS[k]), weight)
    weight = weight * scale

    def slab(i, j):
        return pl.ds((i * NPTS + j) * NPTS, NPTS)

    def across(ref, own):
        return jnp.concatenate([ref[n, own, :] for n in range(parts)], axis=1)

    def spot_of(n, i, j):
        return pl.ds(((i * NPTS + j) * parts + n) * NPTS, NPTS)

    def face_of(tiles):
        return jnp.concatenate(
            [
                jnp.concatenate([w_ref[spot_of(n, i, j), :] for i, j in tiles], axis=0)
                for n in range(parts)
            ],
            axis=1,
        )

    def add_tiles(tiles, values):
        for t, (i, j) in enumerate(tiles):
            for n in range(parts):
                w_ref[spot_of(n, i, j), :] += values[
                    t * NPTS : (t + 1) * NPTS, n * 128 : (n + 1) * 128
                ]

    def add_level(k, values):
        for n in range(parts):
            own_rows = pl.ds(n * NPTS + k, square, parts * NPTS)
            w_ref[own_rows, :] += values[:, n * 128 : (n + 1) * 128]

    turns = [deriv_ref[128 * n : 128 * n + 128, :] for n in range(4)]

    def along(pair, values):
        high, low = halves_of(values)
        both = jnp.concatenate([high, low], axis=0)
        return dot(jnp.concatenate([pair[0], pair[0]], axis=1), both) + dot(pair[1], high)

    for n in range(parts):
        here = weight[:, n * 128 : (n + 1) * 128]
        for i in range(NPTS):
            for j in range(NPTS):
                g_ref[n, slab(i, j), :] = k_ref[n, slab(i, j), :] * (
                    here * float(WEIGHTS[i] * WEIGHTS[j])
                )
    for part in range(blocks):
        own_rows = pl.ds(part * block, block)
        turn = along(turns[0:2], across(u_ref, own_rows)) * across(g_ref, own_rows)
        turn = along(turns[2:4], turn)
        for t in range(block // NPTS):
            i, j = divmod(part * block // NPTS + t, NPTS)
            for n in range(parts):
                w_ref[spot_of(n, i, j), :] = turn[
                    t * NPTS : (t + 1) * NPTS, n * 128 : (n + 1) * 128
                ]
    for n in range(parts):
        for j in range(NPTS):
            turn = line([u_ref[n, slab(i, j), :] for i in range(NPTS)], DERIV)
            turn = [turn[i] * g_ref[n, slab(i, j), :] for i in range(NPTS)]
            turn = line(turn, DERIV.T)
            for i in range(NPTS):
                w_ref[spot_of(n, i, j), :] += turn[i]
        for i in range(NPTS):
            turn = line([u_ref[n, slab(i, j), :] for j in range(NPTS)], DERIV)
            turn = [turn[j] * g_ref[n, slab(i, j), :] for j in range(NPTS)]
            turn = line(turn, DERIV.T)
            for j in range(NPTS):
                w_ref[spot_of(n, i, j), :] += turn[j]

    low_i, high_i = ([(i, j) for j in range(NPTS)] for i in (0, last))
    low_j, high_j = ([(i, j) for i in range(NPTS)] for j in (0, last))
    face0, face1, face2, face3 = (face_of(tiles) for tiles in (low_i, high_i, low_j, high_j))
    side_out[0, 0:rim, 0:square] = take_rows(hot0s, face0)[0:rim]
    side_out[1, 0:rim, 0:square] = take_rows(hot1s, face1)[0:rim]
    side_out[2, 0:near, 0:square] = take_rows(hot2, face2)[0:near]
    side_out[3, 0:near, 0:square] = take_rows(hot3, face3)[0:near]

    @pl.when(early)
    def _():
        send_messages()

    sides = [
        (sub > 0, 0, 1, (me, sub - 1)),
        (sub < n_sub - 1, 1, 0, (me, sub + 1)),
        (me > 0, 2, 3, (me - 1, sub)),
        (me < n_dom - 1, 3, 2, (me + 1, sub)),
    ]

    def side_copy(mine, theirs, device):
        return pltpu.make_async_remote_copy(
            src_ref=side_out.at[mine],
            dst_ref=side_in.at[theirs],
            send_sem=side_send.at[mine],
            recv_sem=side_recv.at[theirs],
            device_id=device,
            device_id_type=MESH,
        )

    for there, mine, theirs, device in sides:
        @pl.when(there)
        def _():
            side_copy(mine, theirs, device).start()

    keyed = up(2 * farp + 8 * n_dom, 128)

    def landing_rows(keys):
        at = lax.broadcasted_iota(I32, (2 * keyed, sources), 0)
        hit = at == keys[0]
        for key in keys[1:]:
            hit = hit | (at == key)
        return dot(jnp.where(hit, 1.0, 0.0).astype(BF16), hot_src, over).astype(BF16)

    src = lax.broadcasted_iota(I32, (1, sources), 1)

    def far_key(first):
        f = src - first
        s, j = lax.shift_right_logical(f, 2), lax.bitwise_and(f, FAR - 1)
        key = lax.shift_right_logical(j, 1) * keyed + first + 4 * s + lax.bitwise_and(j, 1)
        return jnp.where((f >= 0) & (f < far), key, -1)

    key4 = far_key(0)
    for m in range(4):
        for slot in range(groups):
            key = (m & 1) * keyed + 2 * farp + peer_ref[slot] * 8 + 1 + (m >> 1)
            key4 = jnp.where(src == kids_at + m * groupp + slot, key, key4)
    key5 = far_key(farp)
    p = src - coarse_at
    holds = (p >= 0) & (p < n_dom)
    key5 = jnp.where(holds, 2 * farp + 8 * p, key5)
    land_ref[0] = landing_rows([key4])
    land_ref[1] = landing_rows([key5, jnp.where(holds, keyed + 2 * farp + 8 * p, -1)])

    joined = projected[:, 0:square] + projected[:, square:]
    lift = [mortar_ref[m * square : (m + 1) * square, :] for m in range(4)]
    share = []
    for m in range(4):
        first = raw_at + m * groupp
        share.append(product(joined, lift[m]) - own[first : first + groupp, 0:square])
    share = [jnp.zeros((kids_at, square), F32)] + share
    share.append(jnp.zeros((sources - raw_at, square), F32))
    high, low = halves_of(jnp.concatenate(share, axis=0).T)
    add_level(0, dot(high, hot_src, over) + dot(low, hot_src, over))
    add_tiles(low_i, spread_rows(take_rows(hot1l, face1), hot0l))
    add_tiles(high_i, spread_rows(take_rows(hot0l, face0), hot1l))

    for there, mine, theirs, device in sides:
        @pl.when(there)
        def _():
            side_copy(mine, mine, device).wait()

    add_tiles(low_i, spread_rows(side_in[0, 0:rim, 0:square], hot0s))
    add_tiles(high_i, spread_rows(side_in[1, 0:rim, 0:square], hot1s))
    add2 = spread_rows(side_in[2, 0:near, 0:square], hot2)
    add3 = spread_rows(side_in[3, 0:near, 0:square], hot3)
    add_tiles(low_j, add2)
    add_tiles(high_j, add3)

    def sent_all(step, carry):
        mail(step, True).wait_send()
        return carry

    lax.fori_loop(1, n_dom, sent_all, 0, unroll=n_dom <= 8)
    for side in range(2):
        for s in range(shifts):
            @pl.when(far_there(side, s))
            def _():
                far_copy(side, s, True).wait()

    def wait_all(step, carry):
        mail(step, True).wait_recv()
        return carry

    lax.fori_loop(1, n_dom, wait_all, 0, unroll=n_dom <= 8)

    arrived_ref[0:farp] = far_in[0]
    arrived_ref[farp : 2 * farp] = far_in[1]
    arrived_ref[2 * farp :] = mort_in[...]


def kernel(sizes, semaphores, *refs):
    pl.run_scoped(
        functools.partial(steps, sizes, *refs),
        *[pltpu.SemaphoreType.DMA(shape) for shape in semaphores],
    )


def finish(w_ref, arrived_ref, land_ref, out_hbm, ends_ref):
    def run(sem):
        square = NPTS * NPTS
        tiles, parts = w_ref.shape[0] // NPTS, w_ref.shape[0] // NPTS // square
        inner = pltpu.make_async_copy(
            w_ref.reshape(tiles, NPTS, 128).at[:, 1 : NPTS - 1],
            out_hbm.reshape(tiles, NPTS, 128).at[:, 1 : NPTS - 1],
            sem.at[2 * parts],
        )
        inner.start()
        received = arrived_ref[...]
        spare = land_ref.shape[1] // 2 - received.shape[0]
        if spare:
            received = jnp.concatenate([received, jnp.zeros((spare, 128), F32)], axis=0)
        received = received.T
        received = jnp.concatenate([received[0:square], received[square:]], axis=1)
        both = jnp.concatenate(halves_of(received), axis=0)
        rim = out_hbm.reshape(square, parts, NPTS, 128)
        copies = [inner]
        for side, k in enumerate((0, NPTS - 1)):
            added = dot(both, land_ref[side])
            added = added[0:square] + added[square:]
            for n in range(parts):
                rows = w_ref[pl.ds(n * NPTS + k, square, parts * NPTS), :]
                ends_ref[side, n] = rows + added[:, n * 128 : (n + 1) * 128]
                copy = pltpu.make_async_copy(
                    ends_ref.at[side, n], rim.at[:, n, k], sem.at[side * parts + n]
                )
                copies.append(copy)
        for copy in copies[1:]:
            copy.start()
        for copy in copies:
            copy.wait()

    pl.run_scoped(run, pltpu.SemaphoreType.DMA((2 * w_ref.shape[0] // NPTS**3 + 1,)))


def body(
    sizes,
    nodal_values,
    kappa,
    levels,
    local_faces,
    sub_faces,
    near_faces,
    far_faces,
    child_faces,
    child_peer,
    coarse_faces,
):
    n_dom, n_sub = sizes
    elems = nodal_values.shape[1]
    krons = [np.kron(HALVES[m // 2], HALVES[m % 2]) for m in range(4)]
    mortar = np.concatenate([m.T for m in krons], axis=0)
    far_rows = up(far_faces.shape[1])
    held = (elems // 128, NPTS**3, 128)
    side_rows = up(max(sub_faces.shape[1], near_faces.shape[1]))
    small = [
        levels.reshape(1, elems),
        local_faces,
        sub_faces,
        near_faces,
        jnp.asarray(transforms(n_dom, far_faces.shape[1], child_faces.shape[1]), F32),
        jnp.asarray(stencils(), BF16),
        jnp.asarray(mortar, F32),
    ]
    tables = [far_faces, child_faces, child_peer, coarse_faces]
    far_slots = (2, far_faces.shape[1] // FAR)
    semaphores = [(len(small) + len(tables),), (NPTS**3 // 128,), (4,), (4,)]
    semaphores += [far_slots, far_slots, (n_dom,), (n_dom,)]
    hbm = pl.BlockSpec(memory_space=pltpu.HBM)
    vmem = pl.BlockSpec(memory_space=pltpu.VMEM)
    arrivals = 2 * far_rows + 8 * n_dom
    parts = pl.pallas_call(
        functools.partial(kernel, sizes, semaphores),
        out_shape=[
            pltpu.VMEM((held[0] * held[1], 128), F32),
            pltpu.VMEM((arrivals, 128), F32),
            pltpu.VMEM((2, 2 * up(arrivals, 128), elems), BF16),
        ],
        in_specs=[hbm] * 13,
        out_specs=[vmem] * 3,
        scratch_shapes=[pltpu.VMEM(item.shape, item.dtype) for item in small]
        + [pltpu.SMEM(item.shape, I32) for item in tables]
        + [
            pltpu.VMEM((2, *held), F32),
            pltpu.VMEM(held, F32),
            pltpu.VMEM((4, side_rows, 128), F32),
            pltpu.VMEM((4, side_rows, 128), F32),
            pltpu.VMEM((2, far_rows, 128), F32),
            pltpu.VMEM((2, far_rows, 128), F32),
            pltpu.VMEM((n_dom * 8, 128), F32),
            pltpu.VMEM((n_dom * 8, 128), F32),
        ],
        compiler_params=pltpu.CompilerParams(
            collective_id=0, has_side_effects=True, vmem_limit_bytes=60 * 1024 * 1024
        ),
    )(
        nodal_values,
        kappa,
        *small,
        *tables,
    )
    applied = pl.pallas_call(
        finish,
        out_shape=jax.ShapeDtypeStruct((held[0] * held[1], 128), F32),
        in_specs=[vmem] * 3,
        out_specs=hbm,
        scratch_shapes=[pltpu.VMEM((2, held[0], NPTS * NPTS, 128), F32)],
    )(*[pltpu.with_memory_space_constraint(item, pltpu.VMEM) for item in parts])
    applied = applied.reshape(NPTS * NPTS, held[0], NPTS, 128).transpose(0, 2, 1, 3)
    return applied.reshape(nodal_values.shape)


def solution(mesh):
    sizes = (mesh.shape["dom"], mesh.shape["sub"])
    wide = P(None, ("dom", "sub"))
    flat = P(("dom", "sub"))
    in_specs = (wide, wide, flat, wide, wide, wide, wide, wide, flat, flat)
    return jax.shard_map(
        functools.partial(body, sizes),
        mesh=mesh,
        in_specs=in_specs,
        out_specs=wide,
        check_vma=False,
    )
```

```python
import functools

import jax
import jax.numpy as jnp
import numpy as np
from jax import lax
from jax.experimental import pallas as pl
from jax.experimental.pallas import tpu as pltpu
from jax.sharding import PartitionSpec as P

NPTS = 8
FAR = 4
MESH = pl.DeviceIdType.MESH
F32, BF16, I32 = jnp.float32, jnp.bfloat16, jnp.int32


def legendre_table(points, degree):
    table = [np.ones(points.shape), points.copy()]
    for order in range(2, degree + 1):
        table.append(
            ((2 * order - 1) * points * table[order - 1] - (order - 1) * table[order - 2]) / order
        )
    return table


def lobatto_points(degree):
    points = np.cos(np.pi * np.arange(degree + 1) / degree)
    for sweep in range(100):
        table = legendre_table(points, degree)
        points = points - (points * table[degree] - table[degree - 1]) / (
            (degree + 1) * table[degree]
        )
    points = np.sort(points)
    return (points, legendre_table(points, degree)[degree])


def node_tables(count):
    degree = count - 1
    points, legendre = lobatto_points(degree)
    weights = 2.0 / (degree * (degree + 1) * legendre**2)
    spread = points[:, None] - points[None, :] + np.eye(count)
    derivative = legendre[:, None] / (legendre[None, :] * spread) * (1.0 - np.eye(count))
    derivative[0, 0] = -degree * (degree + 1) / 4.0
    derivative[degree, degree] = degree * (degree + 1) / 4.0
    halves = []
    for side in range(2):
        target = (points + 2.0 * side - 1.0) / 2.0
        matrix = np.ones((count, count))
        for column in range(count):
            for other in range(count):
                if other != column:
                    matrix[:, column] = (
                        matrix[:, column]
                        * (target - points[other])
                        / (points[column] - points[other])
                    )
        halves.append(matrix)
    return (points, weights, derivative, np.stack(halves))


POINTS, WEIGHTS, DERIV, HALVES = node_tables(NPTS)


def up(count, unit=8):
    return -(-count // unit) * unit


def halves_of(values):
    high = values.astype(BF16)
    return high, (values - high.astype(F32)).astype(BF16)


def numpy_halves(matrix):
    matrix = np.asarray(matrix, np.float32)
    high = matrix.astype(jnp.bfloat16)
    low = (matrix - high.astype(np.float32)).astype(jnp.bfloat16)
    return high, low


def dot(a, b, dims=((1,), (0,))):
    return lax.dot_general(a, b, (dims, ((), ())), preferred_element_type=F32)


def select(hot, values):
    high, low = halves_of(values)
    return dot(hot, high) + dot(hot, low)


def take_rows(hot, face):
    high, low = halves_of(face)
    dims = ((1,), (1,))
    return dot(hot, high, dims) + dot(hot, low, dims)


def spread_rows(rows, hot):
    high, low = halves_of(rows.T)
    return dot(high, hot) + dot(low, hot)


def product(a, matrix):
    high, low = halves_of(a)
    mhigh, mlow = halves_of(matrix)
    return dot(high, mhigh) + dot(low, mhigh) + dot(high, mlow)


def column(row, padded):
    count = row.shape[1]
    r = lax.broadcasted_iota(I32, (padded, count), 0)
    c = lax.broadcasted_iota(I32, (padded, count), 1)
    spread = jnp.where(r == c, jnp.broadcast_to(row.astype(F32), (padded, count)), 0.0)
    col = jnp.sum(spread, axis=1, keepdims=True)
    inside = lax.broadcasted_iota(I32, (padded, 1), 0) < count
    return jnp.where(inside, col, -1.0)


def hot_rows(columns, base, elems, kind=BF16):
    col = columns[0] if len(columns) == 1 else jnp.concatenate(columns, axis=0)
    lane = lax.broadcasted_iota(I32, (col.shape[0], elems), 1).astype(F32)
    return jnp.where(lane == col - float(base), 1.0, 0.0).astype(kind)


def line(values, matrix):
    half = NPTS // 2
    even = [values[i] + values[NPTS - 1 - i] for i in range(half)]
    odd = [values[i] - values[NPTS - 1 - i] for i in range(half)]
    out = [None] * NPTS
    for a in range(half):
        p = q = None
        for i in range(half):
            s = float((matrix[a, i] + matrix[a, NPTS - 1 - i]) / 2)
            t = float((matrix[a, i] - matrix[a, NPTS - 1 - i]) / 2)
            p = even[i] * s if p is None else p + even[i] * s
            q = odd[i] * t if q is None else q + odd[i] * t
        out[a] = q + p
        out[NPTS - 1 - a] = q - p
    return out


def stencils():
    forth, back = np.kron(np.eye(16), DERIV), np.kron(np.eye(16), DERIV.T)
    pieces = [piece for table in (forth, back) for piece in numpy_halves(table)]
    return np.concatenate(pieces, axis=0)


def places(n_dom, far, groups):
    farp, groupp, coarsep = up(far), up(groups), up(n_dom)
    coarse_at = 2 * farp
    kids_at = coarse_at + 4 * coarsep
    raw_at = kids_at + 4 * groupp
    return farp, groupp, coarsep, coarse_at, kids_at, raw_at, raw_at + 4 * groupp


def transforms(n_dom, far, groups):
    farp, groupp, coarsep, coarse_at, kids_at, raw_at, used = places(n_dom, far, groups)
    eye = np.eye(NPTS)[:, :, None]
    first = np.repeat(eye, up(used, 128), axis=2)
    second = first.copy()
    for m in range(4):
        own = slice(coarse_at + m * coarsep, coarse_at + (m + 1) * coarsep)
        first[:, :, own] = HALVES[m // 2][:, :, None]
        second[:, :, own] = HALVES[m % 2][:, :, None]
        own = slice(kids_at + m * groupp, kids_at + (m + 1) * groupp)
        first[:, :, own] = HALVES[m // 2].T[:, :, None]
        second[:, :, own] = HALVES[m % 2].T[:, :, None]
    rows = [first[o, i] for o in range(NPTS) for i in range(NPTS)]
    rows += [second[b, (b + r) % NPTS] for r in range(NPTS) for b in range(NPTS)]
    return np.stack(rows).astype(np.float32)


def steps(
    sizes,
    u_hbm,
    kappa_hbm,
    level_hbm,
    local_hbm,
    sub_hbm,
    near_hbm,
    fold_hbm,
    deriv_hbm,
    mortar_hbm,
    far_hbm,
    child_hbm,
    peer_hbm,
    coarse_hbm,
    w_ref,
    arrived_ref,
    land_ref,
    level_ref,
    local_ref,
    sub_ref,
    near_ref,
    fold_ref,
    deriv_ref,
    mortar_ref,
    far_ref,
    child_ref,
    peer_ref,
    coarse_ref,
    uk_ref,
    g_ref,
    side_out,
    side_in,
    far_out,
    far_in,
    mort_out,
    mort_in,
    small_sem,
    load_sem,
    side_send,
    side_recv,
    far_send,
    far_recv,
    mort_send,
    mort_recv,
):
    n_dom, n_sub = sizes
    u_ref, k_ref = uk_ref.at[0], uk_ref.at[1]
    parts = u_ref.shape[0]
    elems = parts * 128
    square = NPTS * NPTS
    last = NPTS - 1
    me, sub = lax.axis_index("dom"), lax.axis_index("sub")

    urgent = [
        (fold_hbm, fold_ref),
        (far_hbm, far_ref),
        (child_hbm, child_ref),
        (coarse_hbm, coarse_ref),
        (level_hbm, level_ref),
        (peer_hbm, peer_ref),
    ]
    later = [
        (local_hbm, local_ref),
        (sub_hbm, sub_ref),
        (near_hbm, near_ref),
        (deriv_hbm, deriv_ref),
        (mortar_hbm, mortar_ref),
    ]
    small = [
        pltpu.make_async_copy(source, target, small_sem.at[slot])
        for slot, (source, target) in enumerate(urgent + later)
    ]
    block = 128
    blocks = NPTS**3 // block

    def load(n, part, source, target):
        own = pl.ds(part * block, block)
        return pltpu.make_async_copy(
            source.at[own, pl.ds(n * 128, 128)], target.at[n, own], load_sem.at[part]
        )

    def loaded(part):
        whole = uk_ref.at[0, :, pl.ds(0, 2 * block)]
        pltpu.make_async_copy(whole, whole, load_sem.at[part]).wait()

    for copy in small[:6]:
        copy.start()
    for part in range(blocks):
        for n in range(parts):
            load(n, part, u_hbm, u_ref).start()
            load(n, part, kappa_hbm, k_ref).start()
    for copy in small[6:]:
        copy.start()

    far_in[...] = jnp.zeros(far_in.shape, F32)
    mort_in[...] = jnp.zeros(mort_in.shape, F32)

    barrier = pltpu.get_barrier_semaphore()

    def greet(step, carry):
        other = lax.rem(me + step, n_dom)
        pl.semaphore_signal(barrier, inc=1, device_id=(other, sub), device_id_type=MESH)
        return carry

    lax.fori_loop(1, n_dom, greet, 0, unroll=n_dom <= 8)

    @pl.when(sub > 0)
    def _():
        pl.semaphore_signal(barrier, inc=1, device_id=(me, sub - 1), device_id_type=MESH)

    @pl.when(sub < n_sub - 1)
    def _():
        pl.semaphore_signal(barrier, inc=1, device_id=(me, sub + 1), device_id_type=MESH)

    def clear(missing, slot):
        @pl.when(missing)
        def _():
            side_in[slot] = jnp.zeros(side_in.shape[1:], F32)

    clear(sub == 0, 0)
    clear(sub == n_sub - 1, 1)
    clear(me == 0, 2)
    clear(me == n_dom - 1, 3)

    pairs, rim, near = local_ref.shape[1], sub_ref.shape[1], near_ref.shape[1]
    far, groups = far_ref.shape[1], child_ref.shape[1]
    shifts = far // FAR
    farp, groupp, coarsep, coarse_at, kids_at, raw_at, used = places(n_dom, far, groups)
    sources = up(used, 128)
    lane = lax.broadcasted_iota(I32, (8, sources), 1)
    named = lane
    for m in range(1, 4):
        again = (lane >= coarse_at + m * coarsep) & (lane < coarse_at + (m + 1) * coarsep)
        named = jnp.where(again, lane - m * coarsep, named)
    named = jnp.where(lane >= raw_at, lane - (raw_at - kids_at), named)
    row8 = lax.broadcasted_iota(I32, (8, sources), 0)
    on_low = (lane < farp) | (lane >= kids_at)
    reach = [
        jnp.where(on_low, float(WEIGHTS[c] * DERIV[c, 0]), float(WEIGHTS[c] * DERIV[c, last]))
        for c in range(NPTS)
    ]

    def shifted(matrix):
        tables = []
        for r in range(NPTS):
            table = jnp.zeros((8, sources), F32)
            for b in range(NPTS):
                table = jnp.where(row8 == b, float(matrix[b, (b + r) % NPTS]), table)
            tables.append(table)
        return tables

    def turn(tables, values):
        total = tables[0] * values
        for r in range(1, NPTS):
            total += tables[r] * pltpu.roll(values, NPTS - r, 0)
        return total

    forth8, back8 = shifted(DERIV), shifted(DERIV.T)
    quad8 = jnp.zeros((8, sources), F32)
    for k in range(NPTS):
        quad8 = jnp.where(row8 == k, float(WEIGHTS[k]), quad8)

    for copy in small[:6]:
        copy.wait()

    def held(first, ids, base):
        total = jnp.zeros((8, sources), I32)
        for slot, value in enumerate(ids):
            total = jnp.where(named == first + slot, value + (1 - base * elems), total)
        return total

    ids = held(0, [far_ref[0, c] for c in range(far)], 4)
    ids += held(farp, [far_ref[1, c] for c in range(far)], 5)
    ids += held(coarse_at, [coarse_ref[c] for c in range(n_dom)], 5)
    for m in range(4):
        ids += held(kids_at + m * groupp, [child_ref[m, c] for c in range(groups)], 4)
    element = lax.broadcasted_iota(I32, (elems, sources), 0) + 1
    hot_src = jnp.where(element == ids[0:1], 1.0, 0.0).astype(BF16)
    scale = jnp.exp2(-level_ref[...].astype(F32))
    over = ((1,), (1,))

    def pick(ref, part):
        rows = []
        for k in range(NPTS):
            own = pl.ds(part * block + k, block // NPTS, NPTS)
            rows.append(jnp.concatenate([ref[n, own, :] for n in range(parts)], axis=1))
        high, low = halves_of(jnp.concatenate(rows, axis=0))
        both = dot(jnp.concatenate([high, low], axis=0), hot_src)
        return both[0:block] + both[block:]

    spot = jnp.bitwise_and(ids - 1, 127)
    piece = lax.shift_right_arithmetic(ids - 1, 7)
    lookup = lax.GatherDimensionNumbers(
        offset_dims=(),
        collapsed_slice_dims=(1,),
        start_index_map=(1,),
        operand_batching_dims=(0,),
        start_indices_batching_dims=(0,),
    )

    def fetch(ref, part):
        rows = []
        for k in range(NPTS):
            for at in range(0, block, NPTS * NPTS):
                own = pl.ds(part * block + at + k, NPTS, NPTS)
                tiles = []
                for first in range(0, sources, 128):
                    where = slice(first, first + 128)
                    found = jnp.zeros((8, 128), F32)
                    for n in range(parts):
                        taken = lax.gather(
                            ref[n, own, :],
                            spot[:, where][..., None],
                            lookup,
                            slice_sizes=(1, 1),
                            mode=lax.GatherScatterMode.PROMISE_IN_BOUNDS,
                        )
                        found = jnp.where(piece[:, where] == n, taken, found)
                    tiles.append(found)
                rows.append(tiles[0] if len(tiles) == 1 else jnp.concatenate(tiles, axis=1))
        return jnp.concatenate(rows, axis=0)

    edge = float(WEIGHTS[0])
    chosen = None
    along_k, along_j, plane_u, plane_g = [], [], [], []
    for part in range(blocks):
        if part % 2 == 0:
            loaded(part)
            loaded(part + 1)
        u_part, k_part = fetch(u_ref, part), pick(k_ref, part)
        if chosen is None:
            chosen = dot(jnp.broadcast_to(scale, (16, elems)).astype(BF16), hot_src)[0:8]
            chosen = chosen * quad8
        wide = block // NPTS
        for i in range(part * wide // NPTS, (part + 1) * wide // NPTS):
            at = i * NPTS - part * wide

            def strip(values, k):
                return values[k * wide + at : k * wide + at + NPTS]

            here = chosen * float(WEIGHTS[i])
            flat = jnp.where(on_low, strip(u_part, 0), strip(u_part, last))
            g = jnp.where(on_low, strip(k_part, 0), strip(k_part, last)) * (here * edge)
            plane_u.append(flat)
            plane_g.append(g)
            along_j.append(turn(back8, turn(forth8, flat) * g))
            deep = line([strip(u_part, k) for k in range(NPTS)], DERIV)
            total = reach[0] * strip(k_part, 0) * deep[0]
            for c in range(1, NPTS):
                total += reach[c] * strip(k_part, c) * deep[c]
            along_k.append(total * here)
    across_i = line(plane_u, DERIV)
    along_i = line([across_i[i] * plane_g[i] for i in range(NPTS)], DERIV.T)
    summed = [along_i[i] + (along_j[i] + along_k[i]) for i in range(NPTS)]
    cross8 = [fold_ref[square + r * NPTS : square + (r + 1) * NPTS, :] for r in range(NPTS)]
    moved = []
    for o in range(NPTS):
        total = fold_ref[o * NPTS : o * NPTS + 1, :] * summed[0]
        for i in range(1, NPTS):
            total += fold_ref[o * NPTS + i : o * NPTS + i + 1, :] * summed[i]
        moved.append(turn(cross8, total))
    summed = moved
    own = jnp.concatenate(summed + summed, axis=0).T

    half = lax.broadcasted_iota(I32, (8, 128), 1) < square
    for side in range(2):
        for first in range(0, farp, 8):
            faces = own[side * farp + first : side * farp + first + 8]
            far_out[side, first : first + 8] = jnp.where(half, faces, pltpu.roll(faces, 6, 0))
    half_g = lax.broadcasted_iota(I32, (groupp, 128), 1) < square
    kid = [own[kids_at + m * groupp : kids_at + (m + 1) * groupp] for m in range(4)]
    projected = jnp.where(half_g, kid[0], kid[1]) + jnp.where(half_g, kid[2], kid[3])
    half_c = lax.broadcasted_iota(I32, (coarsep, 128), 1) < square
    raised = [own[coarse_at + m * coarsep : coarse_at + (m + 1) * coarsep] for m in range(4)]
    raised = [jnp.where(half_c, raised[m], raised[m + 1]) for m in (0, 2)]
    peer_row = lax.broadcasted_iota(I32, (n_dom, 128), 0)
    routed = jnp.zeros((n_dom, 128), F32)
    for slot in range(groups):
        routed = jnp.where(peer_row == peer_ref[slot], projected[slot : slot + 1], routed)
    mort_out[pl.ds(0, n_dom, 8), :] = routed
    mort_out[pl.ds(1, n_dom, 8), :] = raised[0][0:n_dom]
    mort_out[pl.ds(2, n_dom, 8), :] = raised[1][0:n_dom]

    greeted = n_dom - 1 + (sub > 0).astype(I32) + (sub < n_sub - 1).astype(I32)

    def mail(step, landing):
        other = lax.rem(me + step, n_dom)
        return pltpu.make_async_remote_copy(
            src_ref=mort_out.at[pl.ds(pl.multiple_of(other * 8, 8), 3)],
            dst_ref=mort_in.at[
                pl.ds(pl.multiple_of((other if landing else me) * 8, 8), 3)
            ],
            send_sem=mort_send.at[other],
            recv_sem=mort_recv.at[other if landing else me],
            device_id=(other, sub),
            device_id_type=MESH,
        )

    def far_copy(side, s, landing):
        other = me - s - 2 if side == 0 else me + s + 2
        rows = pl.ds(s * FAR, FAR // 2)
        there = side if landing else 1 - side
        return pltpu.make_async_remote_copy(
            src_ref=far_out.at[side, rows],
            dst_ref=far_in.at[there, rows],
            send_sem=far_send.at[side, s],
            recv_sem=far_recv.at[there, s],
            device_id=(other, sub),
            device_id_type=MESH,
        )

    def far_there(side, s):
        return me >= s + 2 if side == 0 else me + s + 2 < n_dom

    sides = [
        (sub > 0, 0, 1, (me, sub - 1)),
        (sub < n_sub - 1, 1, 0, (me, sub + 1)),
        (me > 0, 2, 3, (me - 1, sub)),
        (me < n_dom - 1, 3, 2, (me + 1, sub)),
    ]

    def side_copy(mine, theirs, device):
        return pltpu.make_async_remote_copy(
            src_ref=side_out.at[mine],
            dst_ref=side_in.at[theirs],
            send_sem=side_send.at[mine],
            recv_sem=side_recv.at[theirs],
            device_id=device,
            device_id_type=MESH,
        )

    def send_sides():
        for there, mine, theirs, device in sides:
            @pl.when(there)
            def _():
                side_copy(mine, theirs, device).start()

    def meet():
        pl.semaphore_wait(barrier, greeted)

    def send_messages():
        def start_all(step, carry):
            mail(step, False).start()
            return carry

        lax.fori_loop(1, n_dom, start_all, 0, unroll=n_dom <= 8)
        for side in range(2):
            for s in range(shifts):
                @pl.when(far_there(side, s))
                def _():
                    far_copy(side, s, False).start()

    early = me < 3

    @pl.when(jnp.logical_not(early))
    def _():
        meet()
        send_messages()

    for copy in small[6:]:
        copy.wait()

    hot0l = hot_rows([column(local_ref[1:2], up(pairs))], 0, elems)
    hot1l = hot_rows([column(local_ref[0:1], up(pairs))], elems, elems)
    folded = side_out.shape[1]
    hot0s = hot_rows([column(sub_ref[0:1], 2 * folded)], 0, elems)
    hot1s = hot_rows([column(sub_ref[1:2], 2 * folded)], elems, elems)
    hot2 = hot_rows([column(near_ref[0:1], 2 * folded)], 2 * elems, elems)
    hot3 = hot_rows([column(near_ref[1:2], 2 * folded)], 3 * elems, elems)

    sub8 = lax.broadcasted_iota(I32, (8, elems), 0)
    weight = jnp.zeros((8, elems), F32)
    for k in range(NPTS):
        weight = jnp.where(sub8 == k, float(WEIGHTS[k]), weight)
    weight = weight * scale

    def slab(i, j):
        return pl.ds((i * NPTS + j) * NPTS, NPTS)

    def across(ref, own):
        return jnp.concatenate([ref[n, own, :] for n in range(parts)], axis=1)

    def spot_of(n, i, j):
        return pl.ds(((i * NPTS + j) * parts + n) * NPTS, NPTS)

    def face_of(tiles):
        return jnp.concatenate(
            [
                jnp.concatenate([w_ref[spot_of(n, i, j), :] for i, j in tiles], axis=0)
                for n in range(parts)
            ],
            axis=1,
        )

    def add_tiles(tiles, values):
        for t, (i, j) in enumerate(tiles):
            for n in range(parts):
                w_ref[spot_of(n, i, j), :] += values[
                    t * NPTS : (t + 1) * NPTS, n * 128 : (n + 1) * 128
                ]

    def add_level(k, values):
        for n in range(parts):
            own_rows = pl.ds(n * NPTS + k, square, parts * NPTS)
            w_ref[own_rows, :] += values[:, n * 128 : (n + 1) * 128]

    turns = [deriv_ref[128 * n : 128 * n + 128, :] for n in range(4)]

    def along(pair, values):
        high, low = halves_of(values)
        both = jnp.concatenate([high, low], axis=0)
        return dot(jnp.concatenate([pair[0], pair[0]], axis=1), both) + dot(pair[1], high)

    for n in range(parts):
        here = weight[:, n * 128 : (n + 1) * 128]
        for i in range(NPTS):
            for j in range(NPTS):
                g_ref[n, slab(i, j), :] = k_ref[n, slab(i, j), :] * (
                    here * float(WEIGHTS[i] * WEIGHTS[j])
                )
    for part in range(blocks):
        own_rows = pl.ds(part * block, block)
        turn = along(turns[0:2], across(u_ref, own_rows)) * across(g_ref, own_rows)
        turn = along(turns[2:4], turn)
        for t in range(block // NPTS):
            i, j = divmod(part * block // NPTS + t, NPTS)
            for n in range(parts):
                w_ref[spot_of(n, i, j), :] = turn[
                    t * NPTS : (t + 1) * NPTS, n * 128 : (n + 1) * 128
                ]
    for n in range(parts):
        for j in range(NPTS):
            turn = line([u_ref[n, slab(i, j), :] for i in range(NPTS)], DERIV)
            turn = [turn[i] * g_ref[n, slab(i, j), :] for i in range(NPTS)]
            turn = line(turn, DERIV.T)
            for i in range(NPTS):
                w_ref[spot_of(n, i, j), :] += turn[i]
        for i in range(NPTS):
            turn = line([u_ref[n, slab(i, j), :] for j in range(NPTS)], DERIV)
            turn = [turn[j] * g_ref[n, slab(i, j), :] for j in range(NPTS)]
            turn = line(turn, DERIV.T)
            for j in range(NPTS):
                w_ref[spot_of(n, i, j), :] += turn[j]

    low_i, high_i = ([(i, j) for j in range(NPTS)] for i in (0, last))
    low_j, high_j = ([(i, j) for i in range(NPTS)] for j in (0, last))
    face0, face1, face2, face3 = (face_of(tiles) for tiles in (low_i, high_i, low_j, high_j))
    faces = ((hot0s, face0), (hot1s, face1), (hot2, face2), (hot3, face3))
    for slot, (spots, face) in enumerate(faces):
        taken = take_rows(spots, face)
        side_out[slot] = jnp.concatenate([taken[0:folded], taken[folded:]], axis=1)

    @pl.when(early)
    def _():
        meet()
        send_sides()
        send_messages()

    @pl.when(jnp.logical_not(early))
    def _():
        send_sides()

    keyed = up(2 * farp + 8 * n_dom, 128)

    def landing_rows(keys):
        at = lax.broadcasted_iota(I32, (2 * keyed, sources), 0)
        hit = at == keys[0]
        for key in keys[1:]:
            hit = hit | (at == key)
        return dot(jnp.where(hit, 1.0, 0.0).astype(BF16), hot_src, over).astype(BF16)

    src = lax.broadcasted_iota(I32, (1, sources), 1)

    def far_key(first):
        f = src - first
        s, j = lax.shift_right_logical(f, 2), lax.bitwise_and(f, FAR - 1)
        key = lax.shift_right_logical(j, 1) * keyed + first + 4 * s + lax.bitwise_and(j, 1)
        return jnp.where((f >= 0) & (f < far), key, -1)

    key4 = far_key(0)
    for m in range(4):
        for slot in range(groups):
            key = (m & 1) * keyed + 2 * farp + peer_ref[slot] * 8 + 1 + (m >> 1)
            key4 = jnp.where(src == kids_at + m * groupp + slot, key, key4)
    key5 = far_key(farp)
    p = src - coarse_at
    holds = (p >= 0) & (p < n_dom)
    key5 = jnp.where(holds, 2 * farp + 8 * p, key5)
    land_ref[0] = landing_rows([key4])
    land_ref[1] = landing_rows([key5, jnp.where(holds, keyed + 2 * farp + 8 * p, -1)])

    joined = projected[:, 0:square] + projected[:, square:]
    lift = [mortar_ref[m * square : (m + 1) * square, :] for m in range(4)]
    share = []
    for m in range(4):
        first = raw_at + m * groupp
        share.append(product(joined, lift[m]) - own[first : first + groupp, 0:square])
    share = [jnp.zeros((kids_at, square), F32)] + share
    share.append(jnp.zeros((sources - raw_at, square), F32))
    high, low = halves_of(jnp.concatenate(share, axis=0).T)
    add_level(0, dot(high, hot_src, over) + dot(low, hot_src, over))
    add_tiles(low_i, spread_rows(take_rows(hot1l, face1), hot0l))
    add_tiles(high_i, spread_rows(take_rows(hot0l, face0), hot1l))

    targets = ((hot0s, low_i), (hot1s, high_i), (hot2, low_j), (hot3, high_j))
    for group in ((0, 2, 3), (1,)):
        for slot in group:
            there, mine, _, device = sides[slot]

            @pl.when(there)
            def _():
                side_copy(mine, mine, device).wait()

        for slot in group:
            spots, tiles = targets[slot]
            both = side_in[slot].T
            pieces = [both[0:square], both[square:]]
            rows = [jnp.concatenate(halves_of(piece), axis=0) for piece in pieces]
            added = dot(rows[0], spots[0:folded]) + dot(rows[1], spots[folded:])
            add_tiles(tiles, added[0:square] + added[square:])

    def sent_all(step, carry):
        mail(step, True).wait_send()
        return carry

    lax.fori_loop(1, n_dom, sent_all, 0, unroll=n_dom <= 8)
    for side in range(2):
        for s in range(shifts):
            @pl.when(far_there(side, s))
            def _():
                far_copy(side, s, True).wait()

    def wait_all(step, carry):
        mail(step, True).wait_recv()
        return carry

    lax.fori_loop(1, n_dom, wait_all, 0, unroll=n_dom <= 8)

    arrived_ref[0:farp] = far_in[0]
    arrived_ref[farp : 2 * farp] = far_in[1]
    arrived_ref[2 * farp :] = mort_in[...]


def kernel(sizes, semaphores, *refs):
    pl.run_scoped(
        functools.partial(steps, sizes, *refs),
        *[pltpu.SemaphoreType.DMA(shape) for shape in semaphores],
    )


def finish(w_ref, arrived_ref, land_ref, out_hbm, ends_ref):
    def run(sem):
        square = NPTS * NPTS
        tiles, parts = w_ref.shape[0] // NPTS, w_ref.shape[0] // NPTS // square
        inner = pltpu.make_async_copy(
            w_ref.reshape(tiles, NPTS, 128).at[:, 1 : NPTS - 1],
            out_hbm.reshape(tiles, NPTS, 128).at[:, 1 : NPTS - 1],
            sem.at[2 * parts],
        )
        inner.start()
        received = arrived_ref[...]
        spare = land_ref.shape[1] // 2 - received.shape[0]
        if spare:
            received = jnp.concatenate([received, jnp.zeros((spare, 128), F32)], axis=0)
        received = received.T
        received = jnp.concatenate([received[0:square], received[square:]], axis=1)
        both = jnp.concatenate(halves_of(received), axis=0)
        rim = out_hbm.reshape(square, parts, NPTS, 128)
        copies = [inner]
        for side, k in enumerate((0, NPTS - 1)):
            added = dot(both, land_ref[side])
            added = added[0:square] + added[square:]
            for n in range(parts):
                rows = w_ref[pl.ds(n * NPTS + k, square, parts * NPTS), :]
                ends_ref[side, n] = rows + added[:, n * 128 : (n + 1) * 128]
                copy = pltpu.make_async_copy(
                    ends_ref.at[side, n], rim.at[:, n, k], sem.at[side * parts + n]
                )
                copies.append(copy)
        for copy in copies[1:]:
            copy.start()
        for copy in copies:
            copy.wait()

    pl.run_scoped(run, pltpu.SemaphoreType.DMA((2 * w_ref.shape[0] // NPTS**3 + 1,)))


def body(
    sizes,
    nodal_values,
    kappa,
    levels,
    local_faces,
    sub_faces,
    near_faces,
    far_faces,
    child_faces,
    child_peer,
    coarse_faces,
):
    n_dom, n_sub = sizes
    elems = nodal_values.shape[1]
    krons = [np.kron(HALVES[m // 2], HALVES[m % 2]) for m in range(4)]
    mortar = np.concatenate([m.T for m in krons], axis=0)
    far_rows = up(far_faces.shape[1])
    held = (elems // 128, NPTS**3, 128)
    side_rows = up(max(sub_faces.shape[1], near_faces.shape[1]), 32) // 2
    small = [
        levels.reshape(1, elems),
        local_faces,
        sub_faces,
        near_faces,
        jnp.asarray(transforms(n_dom, far_faces.shape[1], child_faces.shape[1]), F32),
        jnp.asarray(stencils(), BF16),
        jnp.asarray(mortar, F32),
    ]
    tables = [far_faces, child_faces, child_peer, coarse_faces]
    far_slots = (2, far_faces.shape[1] // FAR)
    semaphores = [(len(small) + len(tables),), (NPTS**3 // 128,), (4,), (4,)]
    semaphores += [far_slots, far_slots, (n_dom,), (n_dom,)]
    hbm = pl.BlockSpec(memory_space=pltpu.HBM)
    vmem = pl.BlockSpec(memory_space=pltpu.VMEM)
    arrivals = 2 * far_rows + 8 * n_dom
    parts = pl.pallas_call(
        functools.partial(kernel, sizes, semaphores),
        out_shape=[
            pltpu.VMEM((held[0] * held[1], 128), F32),
            pltpu.VMEM((arrivals, 128), F32),
            pltpu.VMEM((2, 2 * up(arrivals, 128), elems), BF16),
        ],
        in_specs=[hbm] * 13,
        out_specs=[vmem] * 3,
        scratch_shapes=[pltpu.VMEM(item.shape, item.dtype) for item in small]
        + [pltpu.SMEM(item.shape, I32) for item in tables]
        + [
            pltpu.VMEM((2, *held), F32),
            pltpu.VMEM(held, F32),
            pltpu.VMEM((4, side_rows, 128), F32),
            pltpu.VMEM((4, side_rows, 128), F32),
            pltpu.VMEM((2, far_rows, 128), F32),
            pltpu.VMEM((2, far_rows, 128), F32),
            pltpu.VMEM((n_dom * 8, 128), F32),
            pltpu.VMEM((n_dom * 8, 128), F32),
        ],
        compiler_params=pltpu.CompilerParams(
            collective_id=0, has_side_effects=True, vmem_limit_bytes=60 * 1024 * 1024
        ),
    )(
        nodal_values,
        kappa,
        *small,
        *tables,
    )
    applied = pl.pallas_call(
        finish,
        out_shape=jax.ShapeDtypeStruct((held[0] * held[1], 128), F32),
        in_specs=[vmem] * 3,
        out_specs=hbm,
        scratch_shapes=[pltpu.VMEM((2, held[0], NPTS * NPTS, 128), F32)],
    )(*[pltpu.with_memory_space_constraint(item, pltpu.VMEM) for item in parts])
    applied = applied.reshape(NPTS * NPTS, held[0], NPTS, 128).transpose(0, 2, 1, 3)
    return applied.reshape(nodal_values.shape)


def solution(mesh):
    sizes = (mesh.shape["dom"], mesh.shape["sub"])
    wide = P(None, ("dom", "sub"))
    flat = P(("dom", "sub"))
    in_specs = (wide, wide, flat, wide, wide, wide, wide, wide, flat, flat)
    return jax.shard_map(
        functools.partial(body, sizes),
        mesh=mesh,
        in_specs=in_specs,
        out_specs=wide,
        check_vma=False,
    )
```
